32 devices in a mesh: bank: 8 (over y, x, core), lane: 4 (over z).
Axes of the slice: x: 2, y: 2, z: 4, core: 2. Of those that a mesh axis runs over, the one named last changes fastest.
Arguments:
- amplitudes: float32 [2, 128, 128, 128], P(None, ('bank', 'lane')), may hold values from -6 to 6
- energies: float32 [128, 128, 128], P(('bank', 'lane')), may hold values from -2 to 2
- phase_angles: float32 [2, 128], replicated, may hold values from 0.3 to 1.2
- mix_angles: float32 [2, 4], replicated, may hold values from 0.3 to 1.2
Outputs:
- final_parts: float32 [2, 128, 128, 128], P(None, ('bank', 'lane'))
- marginal: float32 [16, 128, 128], P('lane', 'bank')
The draws below stay inside these ranges and needn't reach their ends.
All inputs are finite; a program needn't handle non-finite values.
Results may differ from the reference program's by a relative error of at most 0.0003.
Values sent between devices are 32-bit elements; how exact they have to be, the bound alone decides.
A program may use at most 64 MiB of HBM per device.

```python
import jax
import jax.numpy as jnp
from jax import lax

BLOCKS_DEV = 4
ROWS = 128
LANES = 128
BLOCKS = 128
LAYERS = 2
N_BANK = 8
N_LANE = 4


def steps_of(stream_key, dims, pieces, low, top_value):
    def one(axis_at, shards_of):
        heights = jax.random.uniform(jax.random.fold_in(jax.random.fold_in(stream_key, 6), axis_at), (shards_of,), jnp.float32, low / len(pieces), top_value / len(pieces))
        return jnp.repeat(jnp.exp(heights), dims[axis_at] // shards_of).reshape((-1,) + (1,) * (len(dims) - axis_at - 1))

    loudness = one(*pieces[0])
    for cut in pieces[1:]:
        loudness = loudness * one(*cut)
    return loudness


def noise(key, dims, spread, bound, shards=(), kind=jnp.bfloat16):
    entries = jax.random.normal(key, dims, jnp.float32) * spread
    if len(shards) > 0:
        entries = steps_of(key, dims, shards, -0.22, 0.18) * entries
    return jnp.clip(entries, min=-bound, max=bound).astype(kind)


def setup_inputs(seed: int = 0) -> dict:
    key_list = jax.random.split(jax.random.key(seed), 5)
    return {
        "amplitudes": noise(key_list[0], (2, BLOCKS, ROWS, LANES), 1.0, 6.0, ((1, 32),), jnp.float32),
        "energies": jnp.clip(jax.random.uniform(key_list[1], (BLOCKS, ROWS, LANES), jnp.float32, -2.0, 2.0) * steps_of(key_list[1], (BLOCKS, ROWS, LANES), ((0, 32),), -0.4, 0.0), -2.0, 2.0),
        "phase_angles": jnp.clip(jax.random.uniform(key_list[2], (LAYERS, LANES), jnp.float32, 0.3, 1.2), 0.3, 1.2),
        "mix_angles": jnp.clip(jax.random.uniform(key_list[3], (LAYERS, 4), jnp.float32, 0.3, 1.2), 0.3, 1.2),
    }


def count_bits(values, count):
    places = jnp.arange(count.bit_length() - 1, dtype=jnp.int32)
    return jnp.sum((values[..., None] >> places) & 1, axis=-1)


def turn_table(count, angle):
    rank = jnp.arange(count, dtype=jnp.int32)
    apart = count_bits(rank[:, None] ^ rank[None, :], count)
    bits = count.bit_length() - 1
    size = jnp.cos(angle) ** (bits - apart).astype(jnp.float32) * jnp.sin(angle) ** apart.astype(jnp.float32)
    real_sign = jnp.where(apart % 4 == 0, 1.0, jnp.where(apart % 4 == 2, -1.0, 0.0)).astype(jnp.float32)
    imag_sign = jnp.where(apart % 4 == 1, -1.0, jnp.where(apart % 4 == 3, 1.0, 0.0)).astype(jnp.float32)
    return size * real_sign, size * imag_sign


def apply_along(values, dim, angle):
    real_part, imag_part = turn_table(values.shape[dim], angle)
    def times(table):
        moved = jnp.tensordot(values, table, axes=([dim], [0]), precision=lax.Precision.HIGHEST)
        return jnp.moveaxis(moved, -1, dim)
    by_real = times(real_part)
    by_imag = times(imag_part)
    return jnp.stack([by_real[0] - by_imag[1], by_real[1] + by_imag[0]])


def diagonal_step(values, levels, angle):
    turn = angle * levels
    return jnp.stack([values[0] * jnp.cos(turn) + values[1] * jnp.sin(turn), values[1] * jnp.cos(turn) - values[0] * jnp.sin(turn)])


def reference(amplitudes, energies, phase_angles, mix_angles):
    values = amplitudes
    for layer in range(LAYERS):
        values = diagonal_step(values, energies, phase_angles[layer])
        values = apply_along(values, 3, mix_angles[layer, 0])
        values = apply_along(values, 2, mix_angles[layer, 1])
        parts = values.reshape(2, N_BANK, N_LANE, BLOCKS_DEV, ROWS, LANES)
        parts = apply_along(parts, 1, mix_angles[layer, 2])
        parts = apply_along(parts, 2, mix_angles[layer, 3])
        parts = apply_along(parts, 3, mix_angles[layer, 2])
        values = parts.reshape(values.shape)
    chance = values[0] * values[0] + values[1] * values[1]
    marginal = jnp.mean(chance.reshape(N_BANK, -1, ROWS, LANES), axis=0)
    return values, marginal
```

```python
import functools

import jax
import jax.numpy as jnp
from jax import lax
from jax.experimental import pallas as pl
from jax.experimental.pallas import tpu as pltpu
from jax.sharding import PartitionSpec as P

MESH = pl.DeviceIdType.MESH
SIN = (1.0, -1 / 6, 1 / 120, -1 / 5040, 1 / 362880, -1 / 39916800, 1 / 6227020800, -1 / 1307674368000)
COS = (1.0, -1 / 2, 1 / 24, -1 / 720, 1 / 40320, -1 / 3628800, 1 / 479001600, -1 / 87178291200, 1 / 20922789888000)


def series(square, terms):
    total = jnp.full_like(square, terms[-1])
    for term in terms[-2::-1]:
        total = total * square + term
    return total


def sin_cos(turn):
    square = turn * turn
    return turn * series(square, SIN), series(square, COS)


def split(x):
    high = x.astype(jnp.bfloat16)
    return high, (x - high.astype(jnp.float32)).astype(jnp.bfloat16)


def dot3(a, b):
    def one(x, y):
        return lax.dot_general(x, y, (((1,), (0,)), ((), ())), preferred_element_type=jnp.float32)

    return one(a[0], b[0]) + (one(a[1], b[0]) + one(a[0], b[1]))


def turn_table(count, cosine, sine):
    row = lax.broadcasted_iota(jnp.int32, (count, count), 0)
    col = lax.broadcasted_iota(jnp.int32, (count, count), 1)
    apart = row ^ col
    size = jnp.ones((count, count), jnp.float32)
    ones = jnp.zeros((count, count), jnp.int32)
    for place in range(count.bit_length() - 1):
        bit = (apart >> place) & 1
        size = size * jnp.where(bit == 1, sine, cosine)
        ones = ones + bit
    phase = ones & 3
    real = jnp.where(phase == 0, size, jnp.where(phase == 2, -size, 0.0))
    imag = jnp.where(phase == 1, -size, jnp.where(phase == 3, size, 0.0))
    return real, imag


def butterfly(re, im, stride, cosine, sine):
    count, rest = re.shape[0], re.shape[1:]
    parts = (count // (2 * stride), 2, stride) + rest
    re, im = re.reshape(parts), im.reshape(parts)
    ur, vr, ui, vi = re[:, 0], re[:, 1], im[:, 0], im[:, 1]
    new_re = jnp.stack([cosine * ur + sine * vi, cosine * vr + sine * ui], axis=1)
    new_im = jnp.stack([cosine * ui - sine * vr, cosine * vi - sine * ur], axis=1)
    return new_re.reshape((count,) + rest), new_im.reshape((count,) + rest)


def kernel(
    nb, nl, halves, amp_hbm, en_hbm, ph_hbm, mix_hbm, out, marg,
    ph, mix, amp, en, e_l, tmp, s_a, e_b, b_b, o_b, r_a, cs_b, sn_b, part_done, ch, m_in, load, send, recv, line_in, lines_in, all_in,
):
    n = nb * nl
    depth, rows, lanes = amp.shape[1:]
    per = en.shape[2]
    step = per // halves
    tiled = per % 8 == 0
    units = rows // per
    piece = rows // nb
    last = 2 * halves + 2
    hub = nl // 2 - 1
    bank, lane = lax.axis_index("bank"), lax.axis_index("lane")
    me = bank * nl + lane

    load_en = pltpu.make_async_copy(en_hbm, en, load.at[0])
    load_amp = pltpu.make_async_copy(amp_hbm, amp, load.at[1])
    load_ph = pltpu.make_async_copy(ph_hbm, ph, load.at[2])
    load_mix = pltpu.make_async_copy(mix_hbm, mix, load.at[3])
    barrier = pltpu.get_barrier_semaphore()

    def partner(k):
        return lax.rem(bank + nb - lax.rem(k, nb), nb), lax.rem(lane + k // nb, nl)

    def greet_line(k, carry):
        to = lax.rem(lane + k, nl)

        @pl.when(to != hub)
        def _():
            pl.semaphore_signal(barrier, 1, device_id=(bank, to), device_id_type=MESH)

        return carry

    def signal_hubs(sem):
        def one(k, carry):
            pl.semaphore_signal(sem, 1, device_id=(lax.rem(bank + k, nb), hub), device_id_type=MESH)
            return carry

        lax.fori_loop(1, nb, one, 0)

    @pl.when(lane == hub)
    def _():
        signal_hubs(barrier)

    lax.fori_loop(1, nl, greet_line, 0)
    load_en.start()
    load_mix.start()
    load_amp.start()
    load_ph.start()

    def exchange(src, dst, which):
        def one(k, carry):
            to_bank, to_lane = partner(k)
            pltpu.make_async_remote_copy(
                src_ref=src.at[to_bank * nl + to_lane],
                dst_ref=dst.at[me],
                send_sem=send.at[which],
                recv_sem=recv.at[which],
                device_id=(to_bank, to_lane),
                device_id_type=MESH,
            ).start()
            return carry

        lax.fori_loop(1, n, one, 0)
        dst[me] = src[me]

    def arrived(dst, count, sems, which):
        most = dst.at[pl.ds(0, count - 1)]
        pltpu.make_async_copy(most, most, sems.at[which]).wait()

    load_en.wait()
    pl.semaphore_wait(barrier, jnp.where(lane == hub, nb - 1, nl - 1))

    @pl.when(lane == hub + 1)
    def _():
        pl.semaphore_signal(line_in, 1, device_id=(bank, hub), device_id_type=MESH)

    @pl.when(lane == hub)
    def _():
        pl.semaphore_wait(line_in, 1)
        signal_hubs(lines_in)

    def along_line(k, carry):
        to = lax.rem(lane + k, nl)
        pltpu.make_async_remote_copy(
            src_ref=en.at[:, to],
            dst_ref=e_l.at[lane],
            send_sem=send.at[0],
            recv_sem=recv.at[0],
            device_id=(bank, to),
            device_id_type=MESH,
        ).start()
        return carry

    lax.fori_loop(1, nl, along_line, 0)
    e_l[lane] = en[:, lane]
    load_mix.wait()
    cosines, sines = jnp.cos(mix[...]), jnp.sin(mix[...])

    def angle(layer, group):
        return cosines[layer : layer + 1, group : group + 1], sines[layer : layer + 1, group : group + 1]

    def tables(layer, count):
        real, imag = turn_table(lanes, *angle(layer, 0))
        by_lane = split(jnp.concatenate([jnp.concatenate([real, imag], 1), jnp.concatenate([-imag, real], 1)], 0))
        real, imag = turn_table(count, *angle(layer, 1))
        by_row = split(jnp.concatenate([jnp.concatenate([real, -imag], 1), jnp.concatenate([imag, real], 1)], 0))
        return by_lane, by_row

    def local_mix(layer, by_lane, by_row, count, read, write):
        pairs = [read(d) for d in range(depth)]
        stride = 1
        cosine, sine = (jnp.broadcast_to(x, (8, lanes))[None] for x in angle(layer, 2))
        re = jnp.stack([p[0] for p in pairs]).reshape(depth, count // 8, 8, lanes)
        im = jnp.stack([p[1] for p in pairs]).reshape(depth, count // 8, 8, lanes)
        while stride < depth:
            re, im = butterfly(re, im, stride, cosine, sine)
            stride *= 2
        re, im = re.reshape(depth, count, lanes), im.reshape(depth, count, lanes)
        for d in range(depth):
            both = dot3(split(jnp.concatenate([re[d], im[d]], 1)), by_lane)
            both = dot3(by_row, split(jnp.concatenate([both[:, :lanes], both[:, lanes:]], 0)))
            write(d, both[:count], both[count:])

    first_tables = tables(0, rows)
    second_tables = tables(1, rows // halves)

    load_amp.wait()
    load_ph.wait()

    def first(d):
        if tiled:
            e = en[pl.ds(d * units // nl, units // nl)].reshape(rows, lanes)
        else:
            e = tmp[0, d]
        sine, cosine = sin_cos(ph[0:1] * e)
        return amp[0, d] * cosine + amp[1, d] * sine, amp[1, d] * cosine - amp[0, d] * sine

    def to_units(d, re, im):
        if tiled:
            for part, x in enumerate((re, im)):
                x = x.reshape(units, halves, step, lanes)
                for h in range(halves):
                    s_a[h, pl.ds(d * units, units), part] = x[:, h]
        else:
            tmp[0, d] = re
            tmp[1, d] = im

    if not tiled:
        for d in range(depth):

            def spread(u, carry):
                tmp[0, d, pl.ds(u * per, per)] = en[(d * units + u) // nl, lax.rem(d * units + u, nl)]
                return carry

            lax.fori_loop(0, units, spread, 0)
    local_mix(0, *first_tables, rows, first, to_units)
    if not tiled:
        for d in range(depth):

            def gather(u, carry):
                for part in range(2):
                    s_a[0, d * units + u, part] = tmp[part, d, pl.ds(u * per, per)]
                return carry

            lax.fori_loop(0, units, gather, 0)

    @pl.when(lane == hub)
    def _():
        pl.semaphore_wait(lines_in, nb - 1)

        def tell(k, carry):
            pl.semaphore_signal(all_in, 1, device_id=(bank, lax.rem(lane + k, nl)), device_id_type=MESH)
            return carry

        lax.fori_loop(1, nl, tell, 0)

    @pl.when(lane != hub)
    def _():
        pl.semaphore_wait(all_in, 1)

    exchange(s_a.at[0], b_b.at[0], 1)
    arrived(e_l, nl, recv, 0)

    def across(k, carry):
        to = lax.rem(bank + k, nb)
        pltpu.make_async_remote_copy(
            src_ref=e_l.at[:, to],
            dst_ref=e_b.at[bank],
            send_sem=send.at[last - 1],
            recv_sem=recv.at[last - 1],
            device_id=(to, lane),
            device_id_type=MESH,
        ).start()
        return carry

    lax.fori_loop(1, nb, across, 0)
    e_b[bank] = e_l[:, bank]
    for h in range(1, halves):
        exchange(s_a.at[h], b_b.at[h], 1 + h)
    arrived(e_b, nb, recv, last - 1)
    sine, cosine = sin_cos(ph[1:2][None] * e_b[...].reshape(n, per, lanes))
    sn_b[...] = sine
    cs_b[...] = cosine

    for h in range(halves):
        arrived(b_b.at[h], n, recv, 1 + h)
        span = pl.ds(h * step, step)
        re, im = b_b[h, :, 0], b_b[h, :, 1]
        for layer in range(2):
            stride = 1
            while stride < n:
                cosine, sine = (
                    jnp.broadcast_to(x, (step, lanes))[None, None] for x in angle(layer, 3 if stride < nl else 2)
                )
                re, im = butterfly(re, im, stride, cosine, sine)
                stride *= 2
            if layer == 0:
                cosine, sine = cs_b[:, span], sn_b[:, span]
                re, im = re * cosine + im * sine, im * cosine - re * sine
        o_b[h, :, 0] = re
        o_b[h, :, 1] = im
        exchange(o_b.at[h], r_a.at[h], 1 + halves + h)

    def second(h, d):
        if tiled:
            return tuple(
                r_a[h, pl.ds(d * units, units), part].reshape(rows // halves, lanes) for part in range(2)
            )
        return tmp[0, d], tmp[1, d]

    def keep(d, re, im):
        part_done[0, d] = re
        part_done[1, d] = im

    def pass_on(d):
        def one(k, carry):
            to_bank = lax.rem(bank + k, nb)
            pltpu.make_async_remote_copy(
                src_ref=ch.at[d, to_bank],
                dst_ref=m_in.at[bank, d],
                send_sem=send.at[last],
                recv_sem=recv.at[last],
                device_id=(to_bank, lane),
                device_id_type=MESH,
            ).start()
            return carry

        lax.fori_loop(1, nb, one, 0)
        m_in[bank, d] = ch[d, bank]

    def finish(d, re, im):
        if halves == 2:
            cosine, sine = angle(1, 1)
            ur, ui, vr, vi = part_done[0, d], part_done[1, d], re, im
            shape = (units, 1, step, lanes)
            re = [cosine * ur + sine * vi, cosine * vr + sine * ui]
            im = [cosine * ui - sine * vr, cosine * vi - sine * ur]
            re = jnp.concatenate([x.reshape(shape) for x in re], 1).reshape(rows, lanes)
            im = jnp.concatenate([x.reshape(shape) for x in im], 1).reshape(rows, lanes)
        chance = re * re + im * im
        for g in range(nb):
            ch[d, g] = chance[g * piece : (g + 1) * piece]
        out[0, d] = re
        out[1, d] = im
        pass_on(d)

    for h in range(halves):
        arrived(r_a.at[h], n, recv, 1 + halves + h)
        if not tiled:
            for d in range(depth):

                def place(u, carry):
                    for part in range(2):
                        tmp[part, d, pl.ds(u * per, per)] = r_a[h, d * units + u, part]
                    return carry

                lax.fori_loop(0, units, place, 0)
        write = finish if h == halves - 1 else keep
        local_mix(1, *second_tables, rows // halves, functools.partial(second, h), write)

    arrived(m_in, nb, recv, last)
    total = m_in[0]
    for g in range(1, nb):
        total = total + m_in[g]
    marg[...] = total * (1.0 / nb)
    arrived(e_l, nl, send, 0)
    arrived(e_b, nb, send, last - 1)
    for h in range(halves):
        arrived(b_b.at[h], n, send, 1 + h)
        arrived(r_a.at[h], n, send, 1 + halves + h)
    arrived(m_in, nb, send, last)


def on_device(nb, nl, amplitudes, energies, phase_angles, mix_angles):
    _, depth, rows, lanes = amplitudes.shape
    n = nb * nl
    per = depth * rows // n
    halves = 2 if per % 16 == 0 else 1
    piece = rows // nb
    f32 = jnp.float32
    state = pltpu.VMEM((halves, n, 2, per // halves, lanes), f32)
    level = pltpu.VMEM((n, per, lanes), f32)
    spread = pltpu.VMEM((nb, nl, per, lanes), f32)
    vmem = pl.BlockSpec(memory_space=pltpu.VMEM)
    anywhere = pl.BlockSpec(memory_space=pl.ANY)
    whole = pltpu.VMEM((2, depth, rows, lanes), f32)
    return pl.pallas_call(
        functools.partial(kernel, nb, nl, halves),
        name="register",
        out_shape=(pltpu.VMEM(amplitudes.shape, f32), pltpu.VMEM((depth, piece, lanes), f32)),
        in_specs=[anywhere] * 4,
        out_specs=(vmem, vmem),
        scratch_shapes=[
            pltpu.VMEM(phase_angles.shape, f32),
            pltpu.VMEM(mix_angles.shape, f32),
            whole,
            spread,
            pltpu.VMEM((nl, nb, per, lanes), f32),
            whole if per % 8 else pltpu.VMEM((1, 1, 8, 128), f32),
            state,
            spread,
            state,
            state,
            state,
            level,
            level,
            pltpu.VMEM((2, depth, rows // halves, lanes), f32),
            pltpu.VMEM((depth, nb, piece, lanes), f32),
            pltpu.VMEM((nb, depth, piece, lanes), f32),
            pltpu.SemaphoreType.DMA((4,)),
            pltpu.SemaphoreType.DMA((2 * halves + 3,)),
            pltpu.SemaphoreType.DMA((2 * halves + 3,)),
            pltpu.SemaphoreType.REGULAR,
            pltpu.SemaphoreType.REGULAR,
            pltpu.SemaphoreType.REGULAR,
        ],
        compiler_params=pltpu.CompilerParams(collective_id=0, has_side_effects=True),
    )(amplitudes, energies.reshape(nb, nl, per, lanes), phase_angles, mix_angles)


def solution(mesh):
    placed = (P(None, ("bank", "lane"), None, None), P(("bank", "lane"), None, None), P(), P())
    return jax.shard_map(
        functools.partial(on_device, mesh.shape["bank"], mesh.shape["lane"]),
        mesh=mesh,
        in_specs=placed,
        out_specs=(P(None, ("bank", "lane"), None, None), P("lane", "bank", None)),
        check_vma=False,
    )
```

```python
import functools

import jax
import jax.numpy as jnp
from jax import lax
from jax.experimental import pallas as pl
from jax.experimental.pallas import tpu as pltpu
from jax.sharding import PartitionSpec as P

MESH = pl.DeviceIdType.MESH
SIN = (1.0, -1 / 6, 1 / 120, -1 / 5040, 1 / 362880, -1 / 39916800, 1 / 6227020800, -1 / 1307674368000)
COS = (1.0, -1 / 2, 1 / 24, -1 / 720, 1 / 40320, -1 / 3628800, 1 / 479001600, -1 / 87178291200, 1 / 20922789888000)


def series(square, terms):
    total = jnp.full_like(square, terms[-1])
    for term in terms[-2::-1]:
        total = total * square + term
    return total


def sin_cos(turn):
    square = turn * turn
    return turn * series(square, SIN), series(square, COS)


def split(x):
    high = x.astype(jnp.bfloat16)
    return high, (x - high.astype(jnp.float32)).astype(jnp.bfloat16)


def dot3(a, b):
    def one(x, y):
        return lax.dot_general(x, y, (((1,), (0,)), ((), ())), preferred_element_type=jnp.float32)

    return one(a[0], b[0]) + (one(a[1], b[0]) + one(a[0], b[1]))


def turn_table(count, cosine, sine, places=None):
    places = count.bit_length() - 1 if places is None else places
    row = lax.broadcasted_iota(jnp.int32, (count, count), 0)
    col = lax.broadcasted_iota(jnp.int32, (count, count), 1)
    apart = row ^ col
    size = jnp.ones((count, count), jnp.float32)
    ones = jnp.zeros((count, count), jnp.int32)
    for place in range(places):
        bit = (apart >> place) & 1
        size = size * jnp.where(bit == 1, sine, cosine)
        ones = ones + bit
    size = jnp.where(apart >> places == 0, size, 0.0)
    phase = ones & 3
    real = jnp.where(phase == 0, size, jnp.where(phase == 2, -size, 0.0))
    imag = jnp.where(phase == 1, -size, jnp.where(phase == 3, size, 0.0))
    return real, imag


def butterfly(re, im, stride, cosine, sine):
    count, rest = re.shape[0], re.shape[1:]
    parts = (count // (2 * stride), 2, stride) + rest
    re, im = re.reshape(parts), im.reshape(parts)
    ur, vr, ui, vi = re[:, 0], re[:, 1], im[:, 0], im[:, 1]
    new_re = jnp.stack([cosine * ur + sine * vi, cosine * vr + sine * ui], axis=1)
    new_im = jnp.stack([cosine * ui - sine * vr, cosine * vi - sine * ur], axis=1)
    return new_re.reshape((count,) + rest), new_im.reshape((count,) + rest)


def kernel(
    nb, nl, halves, amp_hbm, en_hbm, ph_hbm, mix_hbm, out, marg,
    ph, mix, amp, en, e_l, tmp, s_a, e_b, b_b, o_b, r_a, cs_b, sn_b, part_done, ch, m_in, load, send, recv, line_in, lines_in, all_in,
):
    n = nb * nl
    depth, rows, lanes = amp.shape[1:]
    per = en.shape[2]
    step = per // halves
    tiled = per % 8 == 0
    units = rows // per
    piece = rows // nb
    last = 2 * halves + 2
    hub = nl // 2 - 1
    bank, lane = lax.axis_index("bank"), lax.axis_index("lane")
    me = bank * nl + lane

    load_en = pltpu.make_async_copy(en_hbm, en, load.at[0])
    load_amp = pltpu.make_async_copy(amp_hbm, amp, load.at[1])
    load_ph = pltpu.make_async_copy(ph_hbm, ph, load.at[2])
    load_mix = pltpu.make_async_copy(mix_hbm, mix, load.at[3])
    barrier = pltpu.get_barrier_semaphore()

    def partner(k):
        return lax.rem(bank + nb - lax.rem(k, nb), nb), lax.rem(lane + k // nb, nl)

    def greet_line(k, carry):
        to = lax.rem(lane + k, nl)

        @pl.when(to != hub)
        def _():
            pl.semaphore_signal(barrier, 1, device_id=(bank, to), device_id_type=MESH)

        return carry

    def signal_hubs(sem):
        def one(k, carry):
            pl.semaphore_signal(sem, 1, device_id=(lax.rem(bank + k, nb), hub), device_id_type=MESH)
            return carry

        lax.fori_loop(1, nb, one, 0)

    @pl.when(lane == hub)
    def _():
        signal_hubs(barrier)

    lax.fori_loop(1, nl, greet_line, 0)
    load_en.start()
    load_mix.start()
    load_amp.start()
    load_ph.start()

    def exchange(src, dst, which):
        def one(k, carry):
            to_bank, to_lane = partner(k)
            pltpu.make_async_remote_copy(
                src_ref=src.at[to_bank * nl + to_lane],
                dst_ref=dst.at[me],
                send_sem=send.at[which],
                recv_sem=recv.at[which],
                device_id=(to_bank, to_lane),
                device_id_type=MESH,
            ).start()
            return carry

        lax.fori_loop(1, n, one, 0)
        dst[me] = src[me]

    def arrived(dst, count, sems, which):
        most = dst.at[pl.ds(0, count - 1)]
        pltpu.make_async_copy(most, most, sems.at[which]).wait()

    load_en.wait()
    pl.semaphore_wait(barrier, jnp.where(lane == hub, nb - 1, nl - 1))

    @pl.when(lane == hub + 1)
    def _():
        pl.semaphore_signal(line_in, 1, device_id=(bank, hub), device_id_type=MESH)

    @pl.when(lane == hub)
    def _():
        pl.semaphore_wait(line_in, 1)
        signal_hubs(lines_in)

    def along_line(k, carry):
        to = lax.rem(lane + k, nl)
        pltpu.make_async_remote_copy(
            src_ref=en.at[:, to],
            dst_ref=e_l.at[lane],
            send_sem=send.at[0],
            recv_sem=recv.at[0],
            device_id=(bank, to),
            device_id_type=MESH,
        ).start()
        return carry

    lax.fori_loop(1, nl, along_line, 0)
    e_l[lane] = en[:, lane]
    load_mix.wait()
    cosines, sines = jnp.cos(mix[...]), jnp.sin(mix[...])

    def angle(layer, group):
        return cosines[layer : layer + 1, group : group + 1], sines[layer : layer + 1, group : group + 1]

    def tables(layer, count):
        real, imag = turn_table(lanes, *angle(layer, 0))
        by_lane = split(jnp.concatenate([jnp.concatenate([real, imag], 1), jnp.concatenate([-imag, real], 1)], 0))
        real, imag = turn_table(count, *angle(layer, 1))
        by_row = split(jnp.concatenate([jnp.concatenate([real, -imag], 1), jnp.concatenate([imag, real], 1)], 0))
        return by_lane, by_row

    def local_mix(layer, by_lane, by_row, count, read, write):
        pairs = [read(d) for d in range(depth)]
        stride = 1
        cosine, sine = (jnp.broadcast_to(x, (8, lanes))[None] for x in angle(layer, 2))
        re = jnp.stack([p[0] for p in pairs]).reshape(depth, count // 8, 8, lanes)
        im = jnp.stack([p[1] for p in pairs]).reshape(depth, count // 8, 8, lanes)
        while stride < depth:
            re, im = butterfly(re, im, stride, cosine, sine)
            stride *= 2
        re, im = re.reshape(depth, count, lanes), im.reshape(depth, count, lanes)
        for d in range(depth):
            both = dot3(split(jnp.concatenate([re[d], im[d]], 1)), by_lane)
            both = dot3(by_row, split(jnp.concatenate([both[:, :lanes], both[:, lanes:]], 0)))
            write(d, both[:count], both[count:])

    first_tables = tables(0, rows)
    second_tables = tables(1, rows // halves)

    load_amp.wait()
    load_ph.wait()

    def first(d):
        if tiled:
            e = en[pl.ds(d * units // nl, units // nl)].reshape(rows, lanes)
        else:
            e = tmp[0, d]
        sine, cosine = sin_cos(ph[0:1] * e)
        return amp[0, d] * cosine + amp[1, d] * sine, amp[1, d] * cosine - amp[0, d] * sine

    def to_units(d, re, im):
        if tiled:
            for part, x in enumerate((re, im)):
                x = x.reshape(units, halves, step, lanes)
                for h in range(halves):
                    s_a[h, pl.ds(d * units, units), part] = x[:, h]
        else:
            tmp[0, d] = re
            tmp[1, d] = im

    if not tiled:
        for d in range(depth):

            def spread(u, carry):
                tmp[0, d, pl.ds(u * per, per)] = en[(d * units + u) // nl, lax.rem(d * units + u, nl)]
                return carry

            lax.fori_loop(0, units, spread, 0)
    local_mix(0, *first_tables, rows, first, to_units)
    if not tiled:
        for d in range(depth):

            def gather(u, carry):
                for part in range(2):
                    s_a[0, d * units + u, part] = tmp[part, d, pl.ds(u * per, per)]
                return carry

            lax.fori_loop(0, units, gather, 0)

    @pl.when(lane == hub)
    def _():
        pl.semaphore_wait(lines_in, nb - 1)

        def tell(k, carry):
            pl.semaphore_signal(all_in, 1, device_id=(bank, lax.rem(lane + k, nl)), device_id_type=MESH)
            return carry

        lax.fori_loop(1, nl, tell, 0)

    @pl.when(lane != hub)
    def _():
        pl.semaphore_wait(all_in, 1)

    exchange(s_a.at[0], b_b.at[0], 1)
    arrived(e_l, nl, recv, 0)

    def across(k, carry):
        to = lax.rem(bank + k, nb)
        pltpu.make_async_remote_copy(
            src_ref=e_l.at[:, to],
            dst_ref=e_b.at[bank],
            send_sem=send.at[last - 1],
            recv_sem=recv.at[last - 1],
            device_id=(to, lane),
            device_id_type=MESH,
        ).start()
        return carry

    lax.fori_loop(1, nb, across, 0)
    e_b[bank] = e_l[:, bank]
    for h in range(1, halves):
        exchange(s_a.at[h], b_b.at[h], 1 + h)
    arrived(e_b, nb, recv, last - 1)
    sine, cosine = sin_cos(ph[1:2][None] * e_b[...].reshape(n, per, lanes))
    sn_b[...] = sine
    cs_b[...] = cosine

    for h in range(halves):
        arrived(b_b.at[h], n, recv, 1 + h)
        span = pl.ds(h * step, step)
        re, im = b_b[h, :, 0], b_b[h, :, 1]
        for layer in range(2):
            stride = 1
            while stride < n:
                cosine, sine = (
                    jnp.broadcast_to(x, (step, lanes))[None, None] for x in angle(layer, 3 if stride < nl else 2)
                )
                re, im = butterfly(re, im, stride, cosine, sine)
                stride *= 2
            if layer == 0:
                cosine, sine = cs_b[:, span], sn_b[:, span]
                re, im = re * cosine + im * sine, im * cosine - re * sine
        o_b[h, :, 0] = re
        o_b[h, :, 1] = im
        exchange(o_b.at[h], r_a.at[h], 1 + halves + h)

    def second(h, d):
        if tiled:
            return tuple(
                r_a[h, pl.ds(d * units, units), part].reshape(rows // halves, lanes) for part in range(2)
            )
        return tmp[0, d], tmp[1, d]

    def keep(d, re, im):
        part_done[0, d] = re
        part_done[1, d] = im

    def pass_on(d):
        def one(k, carry):
            to_bank = lax.rem(bank + k, nb)
            pltpu.make_async_remote_copy(
                src_ref=ch.at[d, to_bank],
                dst_ref=m_in.at[bank, d],
                send_sem=send.at[last],
                recv_sem=recv.at[last],
                device_id=(to_bank, lane),
                device_id_type=MESH,
            ).start()
            return carry

        lax.fori_loop(1, nb, one, 0)
        m_in[bank, d] = ch[d, bank]

    def finish(d, re, im):
        if halves == 2:
            cosine, sine = angle(1, 1)
            ur, ui, vr, vi = part_done[0, d], part_done[1, d], re, im
            shape = (units, 1, step, lanes)
            re = [cosine * ur + sine * vi, cosine * vr + sine * ui]
            im = [cosine * ui - sine * vr, cosine * vi - sine * ur]
            re = jnp.concatenate([x.reshape(shape) for x in re], 1).reshape(rows, lanes)
            im = jnp.concatenate([x.reshape(shape) for x in im], 1).reshape(rows, lanes)
        chance = re * re + im * im
        for g in range(nb):
            ch[d, g] = chance[g * piece : (g + 1) * piece]
        out[0, d] = re
        out[1, d] = im
        pass_on(d)

    for h in range(halves):
        arrived(r_a.at[h], n, recv, 1 + halves + h)
        if not tiled:
            for d in range(depth):

                def place(u, carry):
                    for part in range(2):
                        tmp[part, d, pl.ds(u * per, per)] = r_a[h, d * units + u, part]
                    return carry

                lax.fori_loop(0, units, place, 0)
        write = finish if h == halves - 1 else keep
        local_mix(1, *second_tables, rows // halves, functools.partial(second, h), write)

    arrived(m_in, nb, recv, last)
    total = m_in[0]
    for g in range(1, nb):
        total = total + m_in[g]
    marg[...] = total * (1.0 / nb)
    arrived(e_l, nl, send, 0)
    arrived(e_b, nb, send, last - 1)
    for h in range(halves):
        arrived(b_b.at[h], n, send, 1 + h)
        arrived(r_a.at[h], n, send, 1 + halves + h)
    arrived(m_in, nb, send, last)


def contact(nb, nl, bank, lane, line_in, lines_in, all_in):
    barrier = pltpu.get_barrier_semaphore()
    hub = nl // 2 - 1

    def signal_hubs(sem):
        def one(k, carry):
            pl.semaphore_signal(sem, 1, device_id=(lax.rem(bank + k, nb), hub), device_id_type=MESH)
            return carry

        lax.fori_loop(1, nb, one, 0)

    def greet():
        def one(k, carry):
            to = lax.rem(lane + k, nl)

            @pl.when(to != hub)
            def _():
                pl.semaphore_signal(barrier, 1, device_id=(bank, to), device_id_type=MESH)

            return carry

        @pl.when(lane == hub)
        def _():
            signal_hubs(barrier)

        lax.fori_loop(1, nl, one, 0)

    def line():
        pl.semaphore_wait(barrier, jnp.where(lane == hub, nb - 1, nl - 1))

        @pl.when(lane == hub + 1)
        def _():
            pl.semaphore_signal(line_in, 1, device_id=(bank, hub), device_id_type=MESH)

        @pl.when(lane == hub)
        def _():
            pl.semaphore_wait(line_in, 1)
            signal_hubs(lines_in)

    def everyone():
        @pl.when(lane == hub)
        def _():
            pl.semaphore_wait(lines_in, nb - 1)

            def tell(k, carry):
                pl.semaphore_signal(all_in, 1, device_id=(bank, lax.rem(lane + k, nl)), device_id_type=MESH)
                return carry

            lax.fori_loop(1, nl, tell, 0)

        @pl.when(lane != hub)
        def _():
            pl.semaphore_wait(all_in, 1)

    return greet, line, everyone


def pieces(
    nb, nl, amp_hbm, en_hbm, ph_hbm, mix_hbm, out, marg,
    ph, mix, amp, en, e_l, s_a, e_b, b_b, o_a, o_b, r_a, r_b, cs_b, sn_b, part, ch, m_in,
    load, send, recv, line_in, lines_in, all_in,
):
    n = nb * nl
    depth, rows, lanes = amp.shape[1:]
    step = s_a.shape[3]
    half = step // 2
    units = rows // (2 * step)
    bank, lane = lax.axis_index("bank"), lax.axis_index("lane")
    me = bank * nl + lane
    greet, line, everyone = contact(nb, nl, bank, lane, line_in, lines_in, all_in)
    loads = [
        pltpu.make_async_copy(x, y, load.at[i])
        for i, (x, y) in enumerate([(en_hbm, en), (mix_hbm, mix), (amp_hbm, amp), (ph_hbm, ph)])
    ]
    greet()
    for copy in loads:
        copy.start()

    def remote(src, dst, which, to):
        pltpu.make_async_remote_copy(
            src_ref=src,
            dst_ref=dst,
            send_sem=send.at[which],
            recv_sem=recv.at[which],
            device_id=to,
            device_id_type=MESH,
        ).start()

    def exchange(src, dst, which, ahead=False):
        def one(k, carry):
            to_bank, apart = lax.rem(bank + nb - lax.rem(k, nb), nb), k // nb
            if ahead:
                to_lane = apart
            else:
                to_lane = apart

            @pl.when(to_bank * nl + to_lane != me)
            def _():
                remote(src.at[to_bank * nl + to_lane], dst.at[me], which, (to_bank, to_lane))

            return carry

        lax.fori_loop(0, n, one, 0)
        dst[me] = src[me]

    def along_line(src, dst, which):
        def one(k, carry):
            to = lane ^ (nl - k)
            remote(src.at[:, to], dst.at[lane], which, (bank, to))
            return carry

        lax.fori_loop(1, nl, one, 0)
        dst[lane] = src[:, lane]

    def across(pick, dst, which):
        def one(to, carry):
            @pl.when(to != bank)
            def _():
                remote(pick(to), dst.at[bank], which, (to, lane))

            return carry

        lax.fori_loop(0, nb, one, 0)

    def arrived(dst, count, sems, which):
        most = dst.at[pl.ds(0, count - 1)]
        pltpu.make_async_copy(most, most, sems.at[which]).wait()

    def angle(layer, group):
        return cosines[layer : layer + 1, group : group + 1], sines[layer : layer + 1, group : group + 1]

    def mixed(layer, re, im, stride, stop, group):
        cosine, sine = (jnp.broadcast_to(x, re.shape[1:])[None, None] for x in angle(layer, group))
        while stride < stop:
            re, im = butterfly(re, im, stride, cosine, sine)
            stride *= 2
        return re, im

    def lane_table(layer):
        real, imag = turn_table(lanes, *angle(layer, 0))
        return split(jnp.concatenate([jnp.concatenate([real, imag], 1), jnp.concatenate([-imag, real], 1)], 0))

    def row_table(layer, count, places=None):
        real, imag = turn_table(count, *angle(layer, 1), places)
        return split(jnp.concatenate([jnp.concatenate([real, -imag], 1), jnp.concatenate([imag, real], 1)], 0))

    loads[0].wait()
    line()
    along_line(en, e_l, 0)
    loads[1].wait()
    cosines, sines = jnp.cos(mix[...]), jnp.sin(mix[...])
    lane_first, row_first = lane_table(0), row_table(0, rows)
    lane_second, row_second = lane_table(1), row_table(1, lanes, step.bit_length() - 1)
    loads[2].wait()
    loads[3].wait()

    pairs = []
    for d in range(depth):
        e = en[pl.ds(d * units // nl, units // nl)].reshape(rows, lanes)
        sine, cosine = sin_cos(ph[0:1] * e)
        pairs.append((amp[0, d] * cosine + amp[1, d] * sine, amp[1, d] * cosine - amp[0, d] * sine))
    re = jnp.stack([p[0] for p in pairs]).reshape(depth, rows // 8, 8, lanes)
    im = jnp.stack([p[1] for p in pairs]).reshape(depth, rows // 8, 8, lanes)
    cosine, sine = (jnp.broadcast_to(x, (8, lanes))[None] for x in angle(0, 2))
    stride = 1
    while stride < depth:
        re, im = butterfly(re, im, stride, cosine, sine)
        stride *= 2
    re, im = re.reshape(depth, rows, lanes), im.reshape(depth, rows, lanes)
    for d in range(depth):
        both = dot3(split(jnp.concatenate([re[d], im[d]], 1)), lane_first)
        both = dot3(row_first, split(jnp.concatenate([both[:, :lanes], both[:, lanes:]], 0)))
        for i in range(2):
            x = both[i * rows : (i + 1) * rows].reshape(units, 2, step, lanes)
            for h in range(2):
                s_a[h, pl.ds(d * units, units), i] = x[:, h]

    everyone()
    exchange(s_a.at[0], b_b.at[0], 2)
    arrived(e_l, nl, recv, 0)
    across(lambda to: e_l.at[:, to], e_b, 1)
    e_b[bank] = e_l[:, bank]
    exchange(s_a.at[1], b_b.at[1], 3)
    arrived(e_b, nb, recv, 1)
    sine, cosine = sin_cos(ph[1:2][None] * e_b[...].reshape(n, 2 * step, lanes))
    sn_b[...] = sine
    cs_b[...] = cosine

    for h in range(2):
        arrived(b_b.at[h], n, recv, 2 + h)
        span = pl.ds(h * step, step)
        re, im = b_b[h, :, 0], b_b[h, :, 1]
        re, im = mixed(0, re, im, 1, nl, 3)
        re, im = mixed(0, re, im, nl, n, 2)
        cosine, sine = cs_b[:, span], sn_b[:, span]
        re, im = re * cosine + im * sine, im * cosine - re * sine
        re, im = mixed(1, re, im, 1, nl, 3)
        re, im = mixed(1, re, im, nl, n, 2)
        re, im = re.reshape(n * step, lanes), im.reshape(n * step, lanes)
        both = dot3(split(jnp.concatenate([re, im], 1)), lane_second)
        groups = range(0, n * step, lanes)
        wide = [jnp.concatenate([both[g : g + lanes, i * lanes : (i + 1) * lanes] for g in groups], 1) for i in range(2)]
        both = dot3(row_second, split(jnp.concatenate(wide, 0)))
        for i in range(2):
            x = [both[i * lanes : (i + 1) * lanes, g : g + lanes] for g in groups]
            x = jnp.concatenate(x, 0).reshape(n, step, lanes)
            if h == 0:
                o_a[:, i] = x
            else:
                for s in range(2):
                    o_b[s, :, i] = x[:, s * half : (s + 1) * half]
        if h == 0:
            exchange(o_a, r_a, 4, True)
        else:
            for s in range(2):
                exchange(o_b.at[s], r_b.at[s], 5 + s, True)

    arrived(r_a, n, recv, 4)
    re, im = mixed(1, r_a[:, 0], r_a[:, 1], 1, units, 1)
    re, im = mixed(1, re, im, units, n, 2)
    for s in range(2):
        part[s, 0] = re[:, s * half : (s + 1) * half]
        part[s, 1] = im[:, s * half : (s + 1) * half]

    for s in range(2):
        arrived(r_b.at[s], n, recv, 5 + s)
        vr, vi = mixed(1, r_b[s, :, 0], r_b[s, :, 1], 1, units, 1)
        vr, vi = mixed(1, vr, vi, units, n, 2)
        ur, ui = part[s, 0], part[s, 1]
        cosine, sine = (jnp.broadcast_to(x, (half, lanes))[None] for x in angle(1, 1))
        re = (cosine * ur + sine * vi, cosine * vr + sine * ui)
        im = (cosine * ui - sine * vr, cosine * vi - sine * ur)
        for h in range(2):
            chance = re[h] * re[h] + im[h] * im[h]
            for d in range(depth):
                ch[s, :, d, h] = chance[d * units : (d + 1) * units]
        across(lambda to: ch.at[s, to], m_in.at[s], 7 + s)
        m_in[s, bank] = ch[s, bank]
        for h in range(2):
            for i, x in enumerate((re[h], im[h])):
                out[i, :, :, h, s * half : (s + 1) * half] = x.reshape(depth, units, half, lanes)

    for s in range(2):
        arrived(m_in.at[s], nb, recv, 7 + s)
        total = m_in[s, 0]
        for g in range(1, nb):
            total = total + m_in[s, g]
        marg[:, :, s * half : (s + 1) * half] = total * (1.0 / nb)
    arrived(e_l, nl, send, 0)
    arrived(e_b, nb, send, 1)
    for h in range(2):
        arrived(b_b.at[h], n, send, 2 + h)
        arrived(r_b.at[h], n, send, 5 + h)
        arrived(m_in.at[h], nb, send, 7 + h)
    arrived(r_a, n, send, 4)


def keep(a, b, a_hbm, b_hbm, sems):
    copies = [pltpu.make_async_copy(a, a_hbm, sems.at[0]), pltpu.make_async_copy(b, b_hbm, sems.at[1])]
    for copy in copies:
        copy.start()
    for copy in copies:
        copy.wait()


def in_pieces(nb, nl, amplitudes, energies, phase_angles, mix_angles):
    _, depth, rows, lanes = amplitudes.shape
    n = nb * nl
    per = depth * rows // n
    step, half = per // 2, per // 4
    f32 = jnp.float32
    vmem = pl.BlockSpec(memory_space=pltpu.VMEM)
    anywhere = pl.BlockSpec(memory_space=pl.ANY)
    state = pltpu.VMEM((2, n, 2, step, lanes), f32)
    level = pltpu.VMEM((n, per, lanes), f32)
    spread = pltpu.VMEM((nb, nl, per, lanes), f32)
    shapes = (2, depth, nb, 2, step, lanes), (depth, 2, step, lanes)
    results = pl.pallas_call(
        functools.partial(pieces, nb, nl),
        name="register",
        out_shape=tuple(pltpu.VMEM(shape, f32) for shape in shapes),
        in_specs=[anywhere] * 4,
        out_specs=(vmem, vmem),
        scratch_shapes=[
            pltpu.VMEM(phase_angles.shape, f32),
            pltpu.VMEM(mix_angles.shape, f32),
            pltpu.VMEM((2, depth, rows, lanes), f32),
            spread,
            pltpu.VMEM((nl, nb, per, lanes), f32),
            state,
            spread,
            state,
            pltpu.VMEM((n, 2, step, lanes), f32),
            pltpu.VMEM((2, n, 2, half, lanes), f32),
            pltpu.VMEM((n, 2, step, lanes), f32),
            pltpu.VMEM((2, n, 2, half, lanes), f32),
            level,
            level,
            pltpu.VMEM((2, 2, n, half, lanes), f32),
            pltpu.VMEM((2, nb, depth, 2, half, lanes), f32),
            pltpu.VMEM((2, nb, depth, 2, half, lanes), f32),
            pltpu.SemaphoreType.DMA((4,)),
            pltpu.SemaphoreType.DMA((9,)),
            pltpu.SemaphoreType.DMA((9,)),
            pltpu.SemaphoreType.REGULAR,
            pltpu.SemaphoreType.REGULAR,
            pltpu.SemaphoreType.REGULAR,
        ],
        compiler_params=pltpu.CompilerParams(collective_id=0, has_side_effects=True),
    )(amplitudes, energies.reshape(nb, nl, per, lanes), phase_angles, mix_angles)
    final, marginal = pl.pallas_call(
        keep,
        name="keep",
        out_shape=tuple(jax.ShapeDtypeStruct(shape, f32) for shape in shapes),
        in_specs=[vmem, vmem],
        out_specs=(anywhere, anywhere),
        scratch_shapes=[pltpu.SemaphoreType.DMA((2,))],
    )(*[pltpu.with_memory_space_constraint(x, pltpu.VMEM) for x in results])
    return final.reshape(amplitudes.shape), marginal.reshape(depth, rows // nb, lanes)


def on_device(nb, nl, amplitudes, energies, phase_angles, mix_angles):
    _, depth, rows, lanes = amplitudes.shape
    n = nb * nl
    per = depth * rows // n
    halves = 2 if per % 16 == 0 else 1
    piece = rows // nb
    if per == 2 * 8 and piece == per and rows // per % nl == 0 and n * 8 % lanes == 0:
        return in_pieces(nb, nl, amplitudes, energies, phase_angles, mix_angles)
    f32 = jnp.float32
    state = pltpu.VMEM((halves, n, 2, per // halves, lanes), f32)
    level = pltpu.VMEM((n, per, lanes), f32)
    spread = pltpu.VMEM((nb, nl, per, lanes), f32)
    vmem = pl.BlockSpec(memory_space=pltpu.VMEM)
    anywhere = pl.BlockSpec(memory_space=pl.ANY)
    whole = pltpu.VMEM((2, depth, rows, lanes), f32)
    return pl.pallas_call(
        functools.partial(kernel, nb, nl, halves),
        name="register",
        out_shape=(pltpu.VMEM(amplitudes.shape, f32), pltpu.VMEM((depth, piece, lanes), f32)),
        in_specs=[anywhere] * 4,
        out_specs=(vmem, vmem),
        scratch_shapes=[
            pltpu.VMEM(phase_angles.shape, f32),
            pltpu.VMEM(mix_angles.shape, f32),
            whole,
            spread,
            pltpu.VMEM((nl, nb, per, lanes), f32),
            whole if per % 8 else pltpu.VMEM((1, 1, 8, 128), f32),
            state,
            spread,
            state,
            state,
            state,
            level,
            level,
            pltpu.VMEM((2, depth, rows // halves, lanes), f32),
            pltpu.VMEM((depth, nb, piece, lanes), f32),
            pltpu.VMEM((nb, depth, piece, lanes), f32),
            pltpu.SemaphoreType.DMA((4,)),
            pltpu.SemaphoreType.DMA((2 * halves + 3,)),
            pltpu.SemaphoreType.DMA((2 * halves + 3,)),
            pltpu.SemaphoreType.REGULAR,
            pltpu.SemaphoreType.REGULAR,
            pltpu.SemaphoreType.REGULAR,
        ],
        compiler_params=pltpu.CompilerParams(collective_id=0, has_side_effects=True),
    )(amplitudes, energies.reshape(nb, nl, per, lanes), phase_angles, mix_angles)


def solution(mesh):
    placed = (P(None, ("bank", "lane"), None, None), P(("bank", "lane"), None, None), P(), P())
    return jax.shard_map(
        functools.partial(on_device, mesh.shape["bank"], mesh.shape["lane"]),
        mesh=mesh,
        in_specs=placed,
        out_specs=(P(None, ("bank", "lane"), None, None), P("lane", "bank", None)),
        check_vma=False,
    )
```

```python
import functools

import jax
import jax.numpy as jnp
from jax import lax
from jax.experimental import pallas as pl
from jax.experimental.pallas import tpu as pltpu
from jax.sharding import PartitionSpec as P

MESH = pl.DeviceIdType.MESH
SIN = (1.0, -1 / 6, 1 / 120, -1 / 5040, 1 / 362880, -1 / 39916800, 1 / 6227020800, -1 / 1307674368000)
COS = (1.0, -1 / 2, 1 / 24, -1 / 720, 1 / 40320, -1 / 3628800, 1 / 479001600, -1 / 87178291200, 1 / 20922789888000)


def series(square, terms):
    total = jnp.full_like(square, terms[-1])
    for term in terms[-2::-1]:
        total = total * square + term
    return total


def sin_cos(turn):
    square = turn * turn
    return turn * series(square, SIN), series(square, COS)


def split(x):
    high = x.astype(jnp.bfloat16)
    return high, (x - high.astype(jnp.float32)).astype(jnp.bfloat16)


def dot3(a, b):
    def one(x, y):
        return lax.dot_general(x, y, (((1,), (0,)), ((), ())), preferred_element_type=jnp.float32)

    return one(a[0], b[0]) + (one(a[1], b[0]) + one(a[0], b[1]))


def turn_table(count, cosine, sine, places=None):
    places = count.bit_length() - 1 if places is None else places
    row = lax.broadcasted_iota(jnp.int32, (count, count), 0)
    col = lax.broadcasted_iota(jnp.int32, (count, count), 1)
    apart = row ^ col
    size = jnp.ones((count, count), jnp.float32)
    ones = jnp.zeros((count, count), jnp.int32)
    for place in range(places):
        bit = (apart >> place) & 1
        size = size * jnp.where(bit == 1, sine, cosine)
        ones = ones + bit
    size = jnp.where(apart >> places == 0, size, 0.0)
    phase = ones & 3
    real = jnp.where(phase == 0, size, jnp.where(phase == 2, -size, 0.0))
    imag = jnp.where(phase == 1, -size, jnp.where(phase == 3, size, 0.0))
    return real, imag


def butterfly(re, im, stride, cosine, sine):
    count, rest = re.shape[0], re.shape[1:]
    parts = (count // (2 * stride), 2, stride) + rest
    re, im = re.reshape(parts), im.reshape(parts)
    ur, vr, ui, vi = re[:, 0], re[:, 1], im[:, 0], im[:, 1]
    new_re = jnp.stack([cosine * ur + sine * vi, cosine * vr + sine * ui], axis=1)
    new_im = jnp.stack([cosine * ui - sine * vr, cosine * vi - sine * ur], axis=1)
    return new_re.reshape((count,) + rest), new_im.reshape((count,) + rest)


def kernel(
    nb, nl, halves, amp_hbm, en_hbm, ph_hbm, mix_hbm, out, marg,
    ph, mix, amp, en, e_l, tmp, s_a, e_b, b_b, o_b, r_a, cs_b, sn_b, part_done, ch, m_in, load, send, recv, line_in, lines_in, all_in,
):
    n = nb * nl
    depth, rows, lanes = amp.shape[1:]
    per = en.shape[2]
    step = per // halves
    tiled = per % 8 == 0
    units = rows // per
    piece = rows // nb
    last = 2 * halves + 2
    hub = nl // 2 - 1
    bank, lane = lax.axis_index("bank"), lax.axis_index("lane")
    me = bank * nl + lane

    load_en = pltpu.make_async_copy(en_hbm, en, load.at[0])
    load_amp = pltpu.make_async_copy(amp_hbm, amp, load.at[1])
    load_ph = pltpu.make_async_copy(ph_hbm, ph, load.at[2])
    load_mix = pltpu.make_async_copy(mix_hbm, mix, load.at[3])
    barrier = pltpu.get_barrier_semaphore()

    def partner(k):
        return lax.rem(bank + nb - lax.rem(k, nb), nb), lax.rem(lane + k // nb, nl)

    def greet_line(k, carry):
        to = lax.rem(lane + k, nl)

        @pl.when(to != hub)
        def _():
            pl.semaphore_signal(barrier, 1, device_id=(bank, to), device_id_type=MESH)

        return carry

    def signal_hubs(sem):
        def one(k, carry):
            pl.semaphore_signal(sem, 1, device_id=(lax.rem(bank + k, nb), hub), device_id_type=MESH)
            return carry

        lax.fori_loop(1, nb, one, 0)

    @pl.when(lane == hub)
    def _():
        signal_hubs(barrier)

    lax.fori_loop(1, nl, greet_line, 0)
    load_en.start()
    load_mix.start()
    load_amp.start()
    load_ph.start()

    def exchange(src, dst, which):
        def one(k, carry):
            to_bank, to_lane = partner(k)
            pltpu.make_async_remote_copy(
                src_ref=src.at[to_bank * nl + to_lane],
                dst_ref=dst.at[me],
                send_sem=send.at[which],
                recv_sem=recv.at[which],
                device_id=(to_bank, to_lane),
                device_id_type=MESH,
            ).start()
            return carry

        lax.fori_loop(1, n, one, 0)
        dst[me] = src[me]

    def arrived(dst, count, sems, which):
        most = dst.at[pl.ds(0, count - 1)]
        pltpu.make_async_copy(most, most, sems.at[which]).wait()

    load_en.wait()
    pl.semaphore_wait(barrier, jnp.where(lane == hub, nb - 1, nl - 1))

    @pl.when(lane == hub + 1)
    def _():
        pl.semaphore_signal(line_in, 1, device_id=(bank, hub), device_id_type=MESH)

    @pl.when(lane == hub)
    def _():
        pl.semaphore_wait(line_in, 1)
        signal_hubs(lines_in)

    def along_line(k, carry):
        to = lax.rem(lane + k, nl)
        pltpu.make_async_remote_copy(
            src_ref=en.at[:, to],
            dst_ref=e_l.at[lane],
            send_sem=send.at[0],
            recv_sem=recv.at[0],
            device_id=(bank, to),
            device_id_type=MESH,
        ).start()
        return carry

    lax.fori_loop(1, nl, along_line, 0)
    e_l[lane] = en[:, lane]
    load_mix.wait()
    cosines, sines = jnp.cos(mix[...]), jnp.sin(mix[...])

    def angle(layer, group):
        return cosines[layer : layer + 1, group : group + 1], sines[layer : layer + 1, group : group + 1]

    def tables(layer, count):
        real, imag = turn_table(lanes, *angle(layer, 0))
        by_lane = split(jnp.concatenate([jnp.concatenate([real, imag], 1), jnp.concatenate([-imag, real], 1)], 0))
        real, imag = turn_table(count, *angle(layer, 1))
        by_row = split(jnp.concatenate([jnp.concatenate([real, -imag], 1), jnp.concatenate([imag, real], 1)], 0))
        return by_lane, by_row

    def local_mix(layer, by_lane, by_row, count, read, write):
        pairs = [read(d) for d in range(depth)]
        stride = 1
        cosine, sine = (jnp.broadcast_to(x, (8, lanes))[None] for x in angle(layer, 2))
        re = jnp.stack([p[0] for p in pairs]).reshape(depth, count // 8, 8, lanes)
        im = jnp.stack([p[1] for p in pairs]).reshape(depth, count // 8, 8, lanes)
        while stride < depth:
            re, im = butterfly(re, im, stride, cosine, sine)
            stride *= 2
        re, im = re.reshape(depth, count, lanes), im.reshape(depth, count, lanes)
        for d in range(depth):
            both = dot3(split(jnp.concatenate([re[d], im[d]], 1)), by_lane)
            both = dot3(by_row, split(jnp.concatenate([both[:, :lanes], both[:, lanes:]], 0)))
            write(d, both[:count], both[count:])

    first_tables = tables(0, rows)
    second_tables = tables(1, rows // halves)

    load_amp.wait()
    load_ph.wait()

    def first(d):
        if tiled:
            e = en[pl.ds(d * units // nl, units // nl)].reshape(rows, lanes)
        else:
            e = tmp[0, d]
        sine, cosine = sin_cos(ph[0:1] * e)
        return amp[0, d] * cosine + amp[1, d] * sine, amp[1, d] * cosine - amp[0, d] * sine

    def to_units(d, re, im):
        if tiled:
            for part, x in enumerate((re, im)):
                x = x.reshape(units, halves, step, lanes)
                for h in range(halves):
                    s_a[h, pl.ds(d * units, units), part] = x[:, h]
        else:
            tmp[0, d] = re
            tmp[1, d] = im

    if not tiled:
        for d in range(depth):

            def spread(u, carry):
                tmp[0, d, pl.ds(u * per, per)] = en[(d * units + u) // nl, lax.rem(d * units + u, nl)]
                return carry

            lax.fori_loop(0, units, spread, 0)
    local_mix(0, *first_tables, rows, first, to_units)
    if not tiled:
        for d in range(depth):

            def gather(u, carry):
                for part in range(2):
                    s_a[0, d * units + u, part] = tmp[part, d, pl.ds(u * per, per)]
                return carry

            lax.fori_loop(0, units, gather, 0)

    @pl.when(lane == hub)
    def _():
        pl.semaphore_wait(lines_in, nb - 1)

        def tell(k, carry):
            pl.semaphore_signal(all_in, 1, device_id=(bank, lax.rem(lane + k, nl)), device_id_type=MESH)
            return carry

        lax.fori_loop(1, nl, tell, 0)

    @pl.when(lane != hub)
    def _():
        pl.semaphore_wait(all_in, 1)

    exchange(s_a.at[0], b_b.at[0], 1)
    arrived(e_l, nl, recv, 0)

    def across(k, carry):
        to = lax.rem(bank + k, nb)
        pltpu.make_async_remote_copy(
            src_ref=e_l.at[:, to],
            dst_ref=e_b.at[bank],
            send_sem=send.at[last - 1],
            recv_sem=recv.at[last - 1],
            device_id=(to, lane),
            device_id_type=MESH,
        ).start()
        return carry

    lax.fori_loop(1, nb, across, 0)
    e_b[bank] = e_l[:, bank]
    for h in range(1, halves):
        exchange(s_a.at[h], b_b.at[h], 1 + h)
    arrived(e_b, nb, recv, last - 1)
    sine, cosine = sin_cos(ph[1:2][None] * e_b[...].reshape(n, per, lanes))
    sn_b[...] = sine
    cs_b[...] = cosine

    for h in range(halves):
        arrived(b_b.at[h], n, recv, 1 + h)
        span = pl.ds(h * step, step)
        re, im = b_b[h, :, 0], b_b[h, :, 1]
        for layer in range(2):
            stride = 1
            while stride < n:
                cosine, sine = (
                    jnp.broadcast_to(x, (step, lanes))[None, None] for x in angle(layer, 3 if stride < nl else 2)
                )
                re, im = butterfly(re, im, stride, cosine, sine)
                stride *= 2
            if layer == 0:
                cosine, sine = cs_b[:, span], sn_b[:, span]
                re, im = re * cosine + im * sine, im * cosine - re * sine
        o_b[h, :, 0] = re
        o_b[h, :, 1] = im
        exchange(o_b.at[h], r_a.at[h], 1 + halves + h)

    def second(h, d):
        if tiled:
            return tuple(
                r_a[h, pl.ds(d * units, units), part].reshape(rows // halves, lanes) for part in range(2)
            )
        return tmp[0, d], tmp[1, d]

    def keep(d, re, im):
        part_done[0, d] = re
        part_done[1, d] = im

    def pass_on(d):
        def one(k, carry):
            to_bank = lax.rem(bank + k, nb)
            pltpu.make_async_remote_copy(
                src_ref=ch.at[d, to_bank],
                dst_ref=m_in.at[bank, d],
                send_sem=send.at[last],
                recv_sem=recv.at[last],
                device_id=(to_bank, lane),
                device_id_type=MESH,
            ).start()
            return carry

        lax.fori_loop(1, nb, one, 0)
        m_in[bank, d] = ch[d, bank]

    def finish(d, re, im):
        if halves == 2:
            cosine, sine = angle(1, 1)
            ur, ui, vr, vi = part_done[0, d], part_done[1, d], re, im
            shape = (units, 1, step, lanes)
            re = [cosine * ur + sine * vi, cosine * vr + sine * ui]
            im = [cosine * ui - sine * vr, cosine * vi - sine * ur]
            re = jnp.concatenate([x.reshape(shape) for x in re], 1).reshape(rows, lanes)
            im = jnp.concatenate([x.reshape(shape) for x in im], 1).reshape(rows, lanes)
        chance = re * re + im * im
        for g in range(nb):
            ch[d, g] = chance[g * piece : (g + 1) * piece]
        out[0, d] = re
        out[1, d] = im
        pass_on(d)

    for h in range(halves):
        arrived(r_a.at[h], n, recv, 1 + halves + h)
        if not tiled:
            for d in range(depth):

                def place(u, carry):
                    for part in range(2):
                        tmp[part, d, pl.ds(u * per, per)] = r_a[h, d * units + u, part]
                    return carry

                lax.fori_loop(0, units, place, 0)
        write = finish if h == halves - 1 else keep
        local_mix(1, *second_tables, rows // halves, functools.partial(second, h), write)

    arrived(m_in, nb, recv, last)
    total = m_in[0]
    for g in range(1, nb):
        total = total + m_in[g]
    marg[...] = total * (1.0 / nb)
    arrived(e_l, nl, send, 0)
    arrived(e_b, nb, send, last - 1)
    for h in range(halves):
        arrived(b_b.at[h], n, send, 1 + h)
        arrived(r_a.at[h], n, send, 1 + halves + h)
    arrived(m_in, nb, send, last)


def contact(nb, nl, bank, lane, line_in, last_in, lines_in, all_in):
    barrier = pltpu.get_barrier_semaphore()
    last = nl - 1
    is_hub, is_last = lane == 0, lane == last
    between = jnp.logical_not(jnp.logical_or(is_hub, is_last))

    def signal(sem, to_bank, to_lane):
        pl.semaphore_signal(sem, 1, device_id=(to_bank, to_lane), device_id_type=MESH)

    def signal_hubs(sem):
        def one(k, carry):
            signal(sem, lax.rem(bank + k, nb), 0)
            return carry

        lax.fori_loop(1, nb, one, 0)

    def greet():
        @pl.when(is_last)
        def _():
            signal(barrier, bank, 0)

        @pl.when(jnp.logical_not(is_last))
        def _():
            for to in range(last, 0, -1):

                @pl.when(lane != to)
                def _():
                    signal(barrier, bank, to)

        @pl.when(is_hub)
        def _():
            signal_hubs(barrier)

    def line():
        pl.semaphore_wait(barrier, jnp.where(is_hub, nb, jnp.where(is_last, last, last - 1)))

        @pl.when(lane == 1)
        def _():
            signal(line_in, bank, 0)

        @pl.when(is_hub)
        def _():
            pl.semaphore_wait(line_in, 1)
            for to in range(1, last):
                signal(last_in, bank, to)
            signal_hubs(lines_in)

    def all_of_line():
        @pl.when(between)
        def _():
            pl.semaphore_wait(last_in, 1)

    def everyone():
        @pl.when(is_hub)
        def _():
            pl.semaphore_wait(lines_in, nb - 1)
            for to in range(last, 0, -1):
                signal(all_in, bank, to)

        @pl.when(jnp.logical_not(is_hub))
        def _():
            pl.semaphore_wait(all_in, 1)

    def known(to):
        return jnp.logical_not(jnp.logical_and(between, to == last))

    return greet, line, all_of_line, everyone, known


def pieces(
    nb, nl, amp_hbm, en_hbm, ph_hbm, mix_hbm, out, marg,
    ph, mix, amp, en, e_l, s_a, e_b, b_b, o_a, o_b, r_a, r_b, cs_b, sn_b, part, ch, m_in,
    load, send, recv, *met,
):
    n = nb * nl
    depth, rows, lanes = amp.shape[1:]
    step = s_a.shape[3]
    half = step // 2
    units = rows // (2 * step)
    bank, lane = lax.axis_index("bank"), lax.axis_index("lane")
    me = bank * nl + lane
    greet, line, all_of_line, everyone, known = contact(nb, nl, bank, lane, *met)
    loads = [
        pltpu.make_async_copy(x, y, load.at[i])
        for i, (x, y) in enumerate([(en_hbm, en), (mix_hbm, mix), (amp_hbm, amp), (ph_hbm, ph)])
    ]
    greet()
    for copy in loads:
        copy.start()

    def remote(src, dst, which, to):
        pltpu.make_async_remote_copy(
            src_ref=src,
            dst_ref=dst,
            send_sem=send.at[which],
            recv_sem=recv.at[which],
            device_id=to,
            device_id_type=MESH,
        ).start()

    def send_lane(to_lane, src, dst, which):
        def one(k, carry):
            to_bank = lax.rem(bank + k, nb)

            @pl.when(to_bank * nl + to_lane != me)
            def _():
                remote(src.at[to_bank * nl + to_lane], dst.at[me], which, (to_bank, to_lane))

            return carry

        lax.fori_loop(0, nb, one, 0)

    def now(to):
        return jnp.logical_or(lane != 2, to != 1)

    def exchange(src, dst, which):
        def one(to_lane, carry):
            send_lane(to_lane, src, dst, which)
            return carry

        lax.fori_loop(0, nl, one, 0)
        dst[me] = src[me]

    def along_line(k, start):
        to = lane ^ (nl - k)
        copy = pltpu.make_async_remote_copy(
            src_ref=en.at[:, to],
            dst_ref=e_l.at[lane if start else to],
            send_sem=send.at[8 + k],
            recv_sem=recv.at[8 + k],
            device_id=(bank, to),
            device_id_type=MESH,
        )
        if start:
            copy.start()
            return None
        copy.wait_recv()
        return to

    def across(pick, dst, which):
        def one(to, carry):
            @pl.when(to != bank)
            def _():
                remote(pick(to), dst.at[bank], which, (to, lane))

            return carry

        lax.fori_loop(0, nb, one, 0)

    def arrived(dst, count, sems, which):
        most = dst.at[pl.ds(0, count - 1)]
        pltpu.make_async_copy(most, most, sems.at[which]).wait()

    def angle(layer, group):
        return cosines[layer : layer + 1, group : group + 1], sines[layer : layer + 1, group : group + 1]

    def mixed(layer, re, im, stride, stop, group):
        cosine, sine = (jnp.broadcast_to(x, re.shape[1:])[None, None] for x in angle(layer, group))
        while stride < stop:
            re, im = butterfly(re, im, stride, cosine, sine)
            stride *= 2
        return re, im

    def lane_table(layer):
        real, imag = turn_table(lanes, *angle(layer, 0))
        return split(jnp.concatenate([jnp.concatenate([real, imag], 1), jnp.concatenate([-imag, real], 1)], 0))

    def row_table(layer, count, places=None):
        real, imag = turn_table(count, *angle(layer, 1), places)
        return split(jnp.concatenate([jnp.concatenate([real, -imag], 1), jnp.concatenate([imag, real], 1)], 0))

    loads[0].wait()
    line()
    for k in range(1, nl):
        pl.when(known(lane ^ (nl - k)))(functools.partial(along_line, k, True))
    loads[1].wait()
    cosines, sines = jnp.cos(mix[...]), jnp.sin(mix[...])
    lane_first, row_first = lane_table(0), row_table(0, rows)
    lane_second, row_second = lane_table(1), row_table(1, lanes, step.bit_length() - 1)
    loads[2].wait()
    loads[3].wait()

    pairs = []
    for d in range(depth):
        e = en[pl.ds(d * units // nl, units // nl)].reshape(rows, lanes)
        sine, cosine = sin_cos(ph[0:1] * e)
        pairs.append((amp[0, d] * cosine + amp[1, d] * sine, amp[1, d] * cosine - amp[0, d] * sine))
    re = jnp.stack([p[0] for p in pairs]).reshape(depth, rows // 8, 8, lanes)
    im = jnp.stack([p[1] for p in pairs]).reshape(depth, rows // 8, 8, lanes)
    cosine, sine = (jnp.broadcast_to(x, (8, lanes))[None] for x in angle(0, 2))
    stride = 1
    while stride < depth:
        re, im = butterfly(re, im, stride, cosine, sine)
        stride *= 2
    re, im = re.reshape(depth, rows, lanes), im.reshape(depth, rows, lanes)
    for d in range(depth):
        both = dot3(split(jnp.concatenate([re[d], im[d]], 1)), lane_first)
        both = dot3(row_first, split(jnp.concatenate([both[:, :lanes], both[:, lanes:]], 0)))
        for i in range(2):
            x = both[i * rows : (i + 1) * rows].reshape(units, 2, step, lanes)
            for h in range(2):
                s_a[h, pl.ds(d * units, units), i] = x[:, h]

    all_of_line()
    for k in range(1, nl):
        pl.when(jnp.logical_not(known(lane ^ (nl - k))))(functools.partial(along_line, k, True))
    everyone()
    across(lambda to: en.at[to, lane], e_b.at[:, lane], 1)
    e_b[bank, lane] = en[bank, lane]
    exchange(s_a.at[0], b_b.at[0], 2)
    for k in range(1, nl):
        source = along_line(k, False)
        across(lambda to: e_l.at[source, to], e_b.at[:, source], 1)
        e_b[bank, source] = e_l[source, bank]
    exchange(s_a.at[1], b_b.at[1], 3)
    arrived(e_b, nb, recv, 1)
    sine, cosine = sin_cos(ph[1:2][None] * e_b[...].reshape(n, 2 * step, lanes))
    sn_b[...] = sine
    cs_b[...] = cosine

    for h in range(2):
        arrived(b_b.at[h], n, recv, 2 + h)
        span = pl.ds(h * step, step)
        re, im = b_b[h, :, 0], b_b[h, :, 1]
        re, im = mixed(0, re, im, 1, nl, 3)
        re, im = mixed(0, re, im, nl, n, 2)
        cosine, sine = cs_b[:, span], sn_b[:, span]
        re, im = re * cosine + im * sine, im * cosine - re * sine
        re, im = mixed(1, re, im, 1, nl, 3)
        re, im = mixed(1, re, im, nl, n, 2)
        re, im = re.reshape(n * step, lanes), im.reshape(n * step, lanes)
        both = dot3(split(jnp.concatenate([re, im], 1)), lane_second)
        groups = range(0, n * step, lanes)
        wide = [jnp.concatenate([both[g : g + lanes, i * lanes : (i + 1) * lanes] for g in groups], 1) for i in range(2)]
        both = dot3(row_second, split(jnp.concatenate(wide, 0)))
        for i in range(2):
            x = [both[i * lanes : (i + 1) * lanes, g : g + lanes] for g in groups]
            x = jnp.concatenate(x, 0).reshape(n, step, lanes)
            if h == 0:
                o_a[:, i] = x
            else:
                for s in range(2):
                    o_b[s, :, i] = x[:, s * half : (s + 1) * half]
        if h == 0:
            for to in [0, 3, 1, 2]:
                pl.when(now(to))(functools.partial(send_lane, to, o_a, r_a, 4))
            r_a[me] = o_a[me]
        else:
            for to, s in [(0, 0), (3, 0), (0, 1), (3, 1), (1, -1), (1, 0), (2, 0), (1, 1), (2, 1)]:
                if s < 0:
                    pl.when(jnp.logical_not(now(to)))(functools.partial(send_lane, to, o_a, r_a, 4))
                else:
                    send_lane(to, o_b.at[s], r_b.at[s], 5 + s)
            for s in range(2):
                r_b[s, me] = o_b[s, me]

    arrived(r_a, n, recv, 4)
    re, im = mixed(1, r_a[:, 0], r_a[:, 1], 1, units, 1)
    re, im = mixed(1, re, im, units, n, 2)
    for s in range(2):
        part[s, 0] = re[:, s * half : (s + 1) * half]
        part[s, 1] = im[:, s * half : (s + 1) * half]

    for s in range(2):
        arrived(r_b.at[s], n, recv, 5 + s)
        vr, vi = mixed(1, r_b[s, :, 0], r_b[s, :, 1], 1, units, 1)
        vr, vi = mixed(1, vr, vi, units, n, 2)
        ur, ui = part[s, 0], part[s, 1]
        cosine, sine = (jnp.broadcast_to(x, (half, lanes))[None] for x in angle(1, 1))
        re = (cosine * ur + sine * vi, cosine * vr + sine * ui)
        im = (cosine * ui - sine * vr, cosine * vi - sine * ur)
        for h in range(2):
            chance = re[h] * re[h] + im[h] * im[h]
            for d in range(depth):
                ch[s, :, d, h] = chance[d * units : (d + 1) * units]
        across(lambda to: ch.at[s, to], m_in.at[s], 7 * s)
        m_in[s, bank] = ch[s, bank]
        for h in range(2):
            for i, x in enumerate((re[h], im[h])):
                out[i, :, :, h, s * half : (s + 1) * half] = x.reshape(depth, units, half, lanes)

    for s in range(2):
        arrived(m_in.at[s], nb, recv, 7 * s)
        total = m_in[s, 0]
        for g in range(1, nb):
            total = total + m_in[s, g]
        marg[:, :, s * half : (s + 1) * half] = total * (1.0 / nb)
    for k in range(1, nl):
        pltpu.make_async_copy(en.at[:, 0], e_l.at[0], send.at[8 + k]).wait()
    arrived(e_b, nb, send, 1)
    for h in range(2):
        arrived(b_b.at[h], n, send, 2 + h)
        arrived(r_b.at[h], n, send, 5 + h)
        arrived(m_in.at[h], nb, send, 7 * h)
    arrived(r_a, n, send, 4)


def keep(a, b, a_hbm, b_hbm, sems):
    copies = [pltpu.make_async_copy(a, a_hbm, sems.at[0]), pltpu.make_async_copy(b, b_hbm, sems.at[1])]
    for copy in copies:
        copy.start()
    for copy in copies:
        copy.wait()


def in_pieces(nb, nl, amplitudes, energies, phase_angles, mix_angles):
    _, depth, rows, lanes = amplitudes.shape
    n = nb * nl
    per = depth * rows // n
    step, half = per // 2, per // 4
    f32 = jnp.float32
    vmem = pl.BlockSpec(memory_space=pltpu.VMEM)
    anywhere = pl.BlockSpec(memory_space=pl.ANY)
    state = pltpu.VMEM((2, n, 2, step, lanes), f32)
    level = pltpu.VMEM((n, per, lanes), f32)
    spread = pltpu.VMEM((nb, nl, per, lanes), f32)
    shapes = (2, depth, nb, 2, step, lanes), (depth, 2, step, lanes)
    results = pl.pallas_call(
        functools.partial(pieces, nb, nl),
        name="register",
        out_shape=tuple(pltpu.VMEM(shape, f32) for shape in shapes),
        in_specs=[anywhere] * 4,
        out_specs=(vmem, vmem),
        scratch_shapes=[
            pltpu.VMEM(phase_angles.shape, f32),
            pltpu.VMEM(mix_angles.shape, f32),
            pltpu.VMEM((2, depth, rows, lanes), f32),
            spread,
            pltpu.VMEM((nl, nb, per, lanes), f32),
            state,
            spread,
            state,
            pltpu.VMEM((n, 2, step, lanes), f32),
            pltpu.VMEM((2, n, 2, half, lanes), f32),
            pltpu.VMEM((n, 2, step, lanes), f32),
            pltpu.VMEM((2, n, 2, half, lanes), f32),
            level,
            level,
            pltpu.VMEM((2, 2, n, half, lanes), f32),
            pltpu.VMEM((2, nb, depth, 2, half, lanes), f32),
            pltpu.VMEM((2, nb, depth, 2, half, lanes), f32),
            pltpu.SemaphoreType.DMA((4,)),
            pltpu.SemaphoreType.DMA((8 + nl,)),
            pltpu.SemaphoreType.DMA((8 + nl,)),
            *[pltpu.SemaphoreType.REGULAR] * 4,
        ],
        compiler_params=pltpu.CompilerParams(collective_id=0, has_side_effects=True),
    )(amplitudes, energies.reshape(nb, nl, per, lanes), phase_angles, mix_angles)
    final, marginal = pl.pallas_call(
        keep,
        name="keep",
        out_shape=tuple(jax.ShapeDtypeStruct(shape, f32) for shape in shapes),
        in_specs=[vmem, vmem],
        out_specs=(anywhere, anywhere),
        scratch_shapes=[pltpu.SemaphoreType.DMA((2,))],
    )(*[pltpu.with_memory_space_constraint(x, pltpu.VMEM) for x in results])
    return final.reshape(amplitudes.shape), marginal.reshape(depth, rows // nb, lanes)


def on_device(nb, nl, amplitudes, energies, phase_angles, mix_angles):
    _, depth, rows, lanes = amplitudes.shape
    n = nb * nl
    per = depth * rows // n
    halves = 2 if per % 16 == 0 else 1
    piece = rows // nb
    if per == 2 * 8 and piece == per and rows // per % nl == 0 and n * 8 % lanes == 0:
        return in_pieces(nb, nl, amplitudes, energies, phase_angles, mix_angles)
    f32 = jnp.float32
    state = pltpu.VMEM((halves, n, 2, per // halves, lanes), f32)
    level = pltpu.VMEM((n, per, lanes), f32)
    spread = pltpu.VMEM((nb, nl, per, lanes), f32)
    vmem = pl.BlockSpec(memory_space=pltpu.VMEM)
    anywhere = pl.BlockSpec(memory_space=pl.ANY)
    whole = pltpu.VMEM((2, depth, rows, lanes), f32)
    return pl.pallas_call(
        functools.partial(kernel, nb, nl, halves),
        name="register",
        out_shape=(pltpu.VMEM(amplitudes.shape, f32), pltpu.VMEM((depth, piece, lanes), f32)),
        in_specs=[anywhere] * 4,
        out_specs=(vmem, vmem),
        scratch_shapes=[
            pltpu.VMEM(phase_angles.shape, f32),
            pltpu.VMEM(mix_angles.shape, f32),
            whole,
            spread,
            pltpu.VMEM((nl, nb, per, lanes), f32),
            whole if per % 8 else pltpu.VMEM((1, 1, 8, 128), f32),
            state,
            spread,
            state,
            state,
            state,
            level,
            level,
            pltpu.VMEM((2, depth, rows // halves, lanes), f32),
            pltpu.VMEM((depth, nb, piece, lanes), f32),
            pltpu.VMEM((nb, depth, piece, lanes), f32),
            pltpu.SemaphoreType.DMA((4,)),
            pltpu.SemaphoreType.DMA((2 * halves + 3,)),
            pltpu.SemaphoreType.DMA((2 * halves + 3,)),
            pltpu.SemaphoreType.REGULAR,
            pltpu.SemaphoreType.REGULAR,
            pltpu.SemaphoreType.REGULAR,
        ],
        compiler_params=pltpu.CompilerParams(collective_id=0, has_side_effects=True),
    )(amplitudes, energies.reshape(nb, nl, per, lanes), phase_angles, mix_angles)


def solution(mesh):
    placed = (P(None, ("bank", "lane"), None, None), P(("bank", "lane"), None, None), P(), P())
    return jax.shard_map(
        functools.partial(on_device, mesh.shape["bank"], mesh.shape["lane"]),
        mesh=mesh,
        in_specs=placed,
        out_specs=(P(None, ("bank", "lane"), None, None), P("lane", "bank", None)),
        check_vma=False,
    )
```

```python
import functools

import jax
import jax.numpy as jnp
from jax import lax
from jax.experimental import pallas as pl
from jax.experimental.pallas import tpu as pltpu
from jax.sharding import PartitionSpec as P

MESH = pl.DeviceIdType.MESH
SIN = (1.0, -1 / 6, 1 / 120, -1 / 5040, 1 / 362880, -1 / 39916800, 1 / 6227020800, -1 / 1307674368000)
COS = (1.0, -1 / 2, 1 / 24, -1 / 720, 1 / 40320, -1 / 3628800, 1 / 479001600, -1 / 87178291200, 1 / 20922789888000)


def series(square, terms):
    total = jnp.full_like(square, terms[-1])
    for term in terms[-2::-1]:
        total = total * square + term
    return total


def sin_cos(turn):
    square = turn * turn
    return turn * series(square, SIN), series(square, COS)


def split(x):
    high = x.astype(jnp.bfloat16)
    return high, (x - high.astype(jnp.float32)).astype(jnp.bfloat16)


def dot3(a, b):
    def one(x, y):
        return lax.dot_general(x, y, (((1,), (0,)), ((), ())), preferred_element_type=jnp.float32)

    return one(a[0], b[0]) + (one(a[1], b[0]) + one(a[0], b[1]))


def turn_table(count, cosine, sine, places=None):
    places = count.bit_length() - 1 if places is None else places
    row = lax.broadcasted_iota(jnp.int32, (count, count), 0)
    col = lax.broadcasted_iota(jnp.int32, (count, count), 1)
    apart = row ^ col
    size = jnp.ones((count, count), jnp.float32)
    ones = jnp.zeros((count, count), jnp.int32)
    for place in range(places):
        bit = (apart >> place) & 1
        size = size * jnp.where(bit == 1, sine, cosine)
        ones = ones + bit
    size = jnp.where(apart >> places == 0, size, 0.0)
    phase = ones & 3
    real = jnp.where(phase == 0, size, jnp.where(phase == 2, -size, 0.0))
    imag = jnp.where(phase == 1, -size, jnp.where(phase == 3, size, 0.0))
    return real, imag


def butterfly(re, im, stride, cosine, sine):
    count, rest = re.shape[0], re.shape[1:]
    parts = (count // (2 * stride), 2, stride) + rest
    re, im = re.reshape(parts), im.reshape(parts)
    ur, vr, ui, vi = re[:, 0], re[:, 1], im[:, 0], im[:, 1]
    new_re = jnp.stack([cosine * ur + sine * vi, cosine * vr + sine * ui], axis=1)
    new_im = jnp.stack([cosine * ui - sine * vr, cosine * vi - sine * ur], axis=1)
    return new_re.reshape((count,) + rest), new_im.reshape((count,) + rest)


def kernel(
    nb, nl, halves, amp_hbm, en_hbm, ph_hbm, mix_hbm, out, marg,
    ph, mix, amp, en, e_l, tmp, s_a, e_b, b_b, o_b, r_a, cs_b, sn_b, part_done, ch, m_in, load, send, recv, line_in, lines_in, all_in,
):
    n = nb * nl
    depth, rows, lanes = amp.shape[1:]
    per = en.shape[2]
    step = per // halves
    tiled = per % 8 == 0
    units = rows // per
    piece = rows // nb
    last = 2 * halves + 2
    hub = nl // 2 - 1
    bank, lane = lax.axis_index("bank"), lax.axis_index("lane")
    me = bank * nl + lane

    load_en = pltpu.make_async_copy(en_hbm, en, load.at[0])
    load_amp = pltpu.make_async_copy(amp_hbm, amp, load.at[1])
    load_ph = pltpu.make_async_copy(ph_hbm, ph, load.at[2])
    load_mix = pltpu.make_async_copy(mix_hbm, mix, load.at[3])
    barrier = pltpu.get_barrier_semaphore()

    def partner(k):
        return lax.rem(bank + nb - lax.rem(k, nb), nb), lax.rem(lane + k // nb, nl)

    def greet_line(k, carry):
        to = lax.rem(lane + k, nl)

        @pl.when(to != hub)
        def _():
            pl.semaphore_signal(barrier, 1, device_id=(bank, to), device_id_type=MESH)

        return carry

    def signal_hubs(sem):
        def one(k, carry):
            pl.semaphore_signal(sem, 1, device_id=(lax.rem(bank + k, nb), hub), device_id_type=MESH)
            return carry

        lax.fori_loop(1, nb, one, 0)

    @pl.when(lane == hub)
    def _():
        signal_hubs(barrier)

    lax.fori_loop(1, nl, greet_line, 0)
    load_en.start()
    load_mix.start()
    load_amp.start()
    load_ph.start()

    def exchange(src, dst, which):
        def one(k, carry):
            to_bank, to_lane = partner(k)
            pltpu.make_async_remote_copy(
                src_ref=src.at[to_bank * nl + to_lane],
                dst_ref=dst.at[me],
                send_sem=send.at[which],
                recv_sem=recv.at[which],
                device_id=(to_bank, to_lane),
                device_id_type=MESH,
            ).start()
            return carry

        lax.fori_loop(1, n, one, 0)
        dst[me] = src[me]

    def arrived(dst, count, sems, which):
        most = dst.at[pl.ds(0, count - 1)]
        pltpu.make_async_copy(most, most, sems.at[which]).wait()

    load_en.wait()
    pl.semaphore_wait(barrier, jnp.where(lane == hub, nb - 1, nl - 1))

    @pl.when(lane == hub + 1)
    def _():
        pl.semaphore_signal(line_in, 1, device_id=(bank, hub), device_id_type=MESH)

    @pl.when(lane == hub)
    def _():
        pl.semaphore_wait(line_in, 1)
        signal_hubs(lines_in)

    def along_line(k, carry):
        to = lax.rem(lane + k, nl)
        pltpu.make_async_remote_copy(
            src_ref=en.at[:, to],
            dst_ref=e_l.at[lane],
            send_sem=send.at[0],
            recv_sem=recv.at[0],
            device_id=(bank, to),
            device_id_type=MESH,
        ).start()
        return carry

    lax.fori_loop(1, nl, along_line, 0)
    e_l[lane] = en[:, lane]
    load_mix.wait()
    cosines, sines = jnp.cos(mix[...]), jnp.sin(mix[...])

    def angle(layer, group):
        return cosines[layer : layer + 1, group : group + 1], sines[layer : layer + 1, group : group + 1]

    def tables(layer, count):
        real, imag = turn_table(lanes, *angle(layer, 0))
        by_lane = split(jnp.concatenate([jnp.concatenate([real, imag], 1), jnp.concatenate([-imag, real], 1)], 0))
        real, imag = turn_table(count, *angle(layer, 1))
        by_row = split(jnp.concatenate([jnp.concatenate([real, -imag], 1), jnp.concatenate([imag, real], 1)], 0))
        return by_lane, by_row

    def local_mix(layer, by_lane, by_row, count, read, write):
        pairs = [read(d) for d in range(depth)]
        stride = 1
        cosine, sine = (jnp.broadcast_to(x, (8, lanes))[None] for x in angle(layer, 2))
        re = jnp.stack([p[0] for p in pairs]).reshape(depth, count // 8, 8, lanes)
        im = jnp.stack([p[1] for p in pairs]).reshape(depth, count // 8, 8, lanes)
        while stride < depth:
            re, im = butterfly(re, im, stride, cosine, sine)
            stride *= 2
        re, im = re.reshape(depth, count, lanes), im.reshape(depth, count, lanes)
        for d in range(depth):
            both = dot3(split(jnp.concatenate([re[d], im[d]], 1)), by_lane)
            both = dot3(by_row, split(jnp.concatenate([both[:, :lanes], both[:, lanes:]], 0)))
            write(d, both[:count], both[count:])

    first_tables = tables(0, rows)
    second_tables = tables(1, rows // halves)

    load_amp.wait()
    load_ph.wait()

    def first(d):
        if tiled:
            e = en[pl.ds(d * units // nl, units // nl)].reshape(rows, lanes)
        else:
            e = tmp[0, d]
        sine, cosine = sin_cos(ph[0:1] * e)
        return amp[0, d] * cosine + amp[1, d] * sine, amp[1, d] * cosine - amp[0, d] * sine

    def to_units(d, re, im):
        if tiled:
            for part, x in enumerate((re, im)):
                x = x.reshape(units, halves, step, lanes)
                for h in range(halves):
                    s_a[h, pl.ds(d * units, units), part] = x[:, h]
        else:
            tmp[0, d] = re
            tmp[1, d] = im

    if not tiled:
        for d in range(depth):

            def spread(u, carry):
                tmp[0, d, pl.ds(u * per, per)] = en[(d * units + u) // nl, lax.rem(d * units + u, nl)]
                return carry

            lax.fori_loop(0, units, spread, 0)
    local_mix(0, *first_tables, rows, first, to_units)
    if not tiled:
        for d in range(depth):

            def gather(u, carry):
                for part in range(2):
                    s_a[0, d * units + u, part] = tmp[part, d, pl.ds(u * per, per)]
                return carry

            lax.fori_loop(0, units, gather, 0)

    @pl.when(lane == hub)
    def _():
        pl.semaphore_wait(lines_in, nb - 1)

        def tell(k, carry):
            pl.semaphore_signal(all_in, 1, device_id=(bank, lax.rem(lane + k, nl)), device_id_type=MESH)
            return carry

        lax.fori_loop(1, nl, tell, 0)

    @pl.when(lane != hub)
    def _():
        pl.semaphore_wait(all_in, 1)

    exchange(s_a.at[0], b_b.at[0], 1)
    arrived(e_l, nl, recv, 0)

    def across(k, carry):
        to = lax.rem(bank + k, nb)
        pltpu.make_async_remote_copy(
            src_ref=e_l.at[:, to],
            dst_ref=e_b.at[bank],
            send_sem=send.at[last - 1],
            recv_sem=recv.at[last - 1],
            device_id=(to, lane),
            device_id_type=MESH,
        ).start()
        return carry

    lax.fori_loop(1, nb, across, 0)
    e_b[bank] = e_l[:, bank]
    for h in range(1, halves):
        exchange(s_a.at[h], b_b.at[h], 1 + h)
    arrived(e_b, nb, recv, last - 1)
    sine, cosine = sin_cos(ph[1:2][None] * e_b[...].reshape(n, per, lanes))
    sn_b[...] = sine
    cs_b[...] = cosine

    for h in range(halves):
        arrived(b_b.at[h], n, recv, 1 + h)
        span = pl.ds(h * step, step)
        re, im = b_b[h, :, 0], b_b[h, :, 1]
        for layer in range(2):
            stride = 1
            while stride < n:
                cosine, sine = (
                    jnp.broadcast_to(x, (step, lanes))[None, None] for x in angle(layer, 3 if stride < nl else 2)
                )
                re, im = butterfly(re, im, stride, cosine, sine)
                stride *= 2
            if layer == 0:
                cosine, sine = cs_b[:, span], sn_b[:, span]
                re, im = re * cosine + im * sine, im * cosine - re * sine
        o_b[h, :, 0] = re
        o_b[h, :, 1] = im
        exchange(o_b.at[h], r_a.at[h], 1 + halves + h)

    def second(h, d):
        if tiled:
            return tuple(
                r_a[h, pl.ds(d * units, units), part].reshape(rows // halves, lanes) for part in range(2)
            )
        return tmp[0, d], tmp[1, d]

    def keep(d, re, im):
        part_done[0, d] = re
        part_done[1, d] = im

    def pass_on(d):
        def one(k, carry):
            to_bank = lax.rem(bank + k, nb)
            pltpu.make_async_remote_copy(
                src_ref=ch.at[d, to_bank],
                dst_ref=m_in.at[bank, d],
                send_sem=send.at[last],
                recv_sem=recv.at[last],
                device_id=(to_bank, lane),
                device_id_type=MESH,
            ).start()
            return carry

        lax.fori_loop(1, nb, one, 0)
        m_in[bank, d] = ch[d, bank]

    def finish(d, re, im):
        if halves == 2:
            cosine, sine = angle(1, 1)
            ur, ui, vr, vi = part_done[0, d], part_done[1, d], re, im
            shape = (units, 1, step, lanes)
            re = [cosine * ur + sine * vi, cosine * vr + sine * ui]
            im = [cosine * ui - sine * vr, cosine * vi - sine * ur]
            re = jnp.concatenate([x.reshape(shape) for x in re], 1).reshape(rows, lanes)
            im = jnp.concatenate([x.reshape(shape) for x in im], 1).reshape(rows, lanes)
        chance = re * re + im * im
        for g in range(nb):
            ch[d, g] = chance[g * piece : (g + 1) * piece]
        out[0, d] = re
        out[1, d] = im
        pass_on(d)

    for h in range(halves):
        arrived(r_a.at[h], n, recv, 1 + halves + h)
        if not tiled:
            for d in range(depth):

                def place(u, carry):
                    for part in range(2):
                        tmp[part, d, pl.ds(u * per, per)] = r_a[h, d * units + u, part]
                    return carry

                lax.fori_loop(0, units, place, 0)
        write = finish if h == halves - 1 else keep
        local_mix(1, *second_tables, rows // halves, functools.partial(second, h), write)

    arrived(m_in, nb, recv, last)
    total = m_in[0]
    for g in range(1, nb):
        total = total + m_in[g]
    marg[...] = total * (1.0 / nb)
    arrived(e_l, nl, send, 0)
    arrived(e_b, nb, send, last - 1)
    for h in range(halves):
        arrived(b_b.at[h], n, send, 1 + h)
        arrived(r_a.at[h], n, send, 1 + halves + h)
    arrived(m_in, nb, send, last)


def contact(nb, nl, bank, lane, line_in, last_in, lines_in, all_in):
    barrier = pltpu.get_barrier_semaphore()
    last = nl - 1
    is_hub, is_last = lane == 0, lane == last
    between = jnp.logical_not(jnp.logical_or(is_hub, is_last))

    def signal(sem, to_bank, to_lane):
        pl.semaphore_signal(sem, 1, device_id=(to_bank, to_lane), device_id_type=MESH)

    def signal_hubs(sem):
        def one(k, carry):
            signal(sem, lax.rem(bank + k, nb), 0)
            return carry

        lax.fori_loop(1, nb, one, 0)

    def greet():
        @pl.when(is_last)
        def _():
            signal(barrier, bank, 0)

        @pl.when(jnp.logical_not(is_last))
        def _():
            for to in range(last, 0, -1):

                @pl.when(lane != to)
                def _():
                    signal(barrier, bank, to)

        @pl.when(is_hub)
        def _():
            signal_hubs(barrier)

    def line():
        pl.semaphore_wait(barrier, jnp.where(is_hub, nb, jnp.where(is_last, last, last - 1)))

        @pl.when(lane == 1)
        def _():
            signal(line_in, bank, 0)

        @pl.when(is_hub)
        def _():
            pl.semaphore_wait(line_in, 1)
            for to in range(1, last):
                signal(last_in, bank, to)
            signal_hubs(lines_in)

    def all_of_line():
        @pl.when(between)
        def _():
            pl.semaphore_wait(last_in, 1)

    def everyone():
        @pl.when(is_hub)
        def _():
            pl.semaphore_wait(lines_in, nb - 1)
            for to in range(last, 0, -1):
                signal(all_in, bank, to)

        @pl.when(jnp.logical_not(is_hub))
        def _():
            pl.semaphore_wait(all_in, 1)

    def known(to):
        return jnp.logical_not(jnp.logical_and(between, to == last))

    return greet, line, all_of_line, everyone, known


def pieces(
    nb, nl, amp_hbm, en_hbm, ph_hbm, mix_hbm, out, marg,
    ph, mix, amp, en, e_l, s_a, e_b, b_b, o_a, o_b, r_a, r_b, cs_b, sn_b, part, ch, near, pair, m_in,
    load, send, recv, *met,
):
    n = nb * nl
    depth, rows, lanes = amp.shape[1:]
    step = s_a.shape[3]
    half = step // 2
    units = rows // (2 * step)
    bank, lane = lax.axis_index("bank"), lax.axis_index("lane")
    me = bank * nl + lane
    side, pairs_at = lax.rem(bank, 2), bank // 2
    greet, line, all_of_line, everyone, known = contact(nb, nl, bank, lane, *met)
    loads = [
        pltpu.make_async_copy(x, y, load.at[i])
        for i, (x, y) in enumerate([(en_hbm, en), (mix_hbm, mix), (amp_hbm, amp), (ph_hbm, ph)])
    ]
    greet()
    for copy in loads:
        copy.start()

    def remote(src, dst, which, to):
        pltpu.make_async_remote_copy(
            src_ref=src,
            dst_ref=dst,
            send_sem=send.at[which],
            recv_sem=recv.at[which],
            device_id=to,
            device_id_type=MESH,
        ).start()

    def send_lane(to_lane, src, dst, which):
        def one(k, carry):
            to_bank = lax.rem(bank + k, nb)

            @pl.when(to_bank * nl + to_lane != me)
            def _():
                remote(src.at[to_bank * nl + to_lane], dst.at[me], which, (to_bank, to_lane))

            return carry

        lax.fori_loop(0, nb, one, 0)

    def now(to):
        return jnp.logical_or(lane != 2, to != 1)

    def exchange(src, dst, which, order):
        for to in order:
            send_lane(to, src, dst, which)
        dst[me] = src[me]

    def along_line(k, start):
        to = lane ^ (nl - k)
        copy = pltpu.make_async_remote_copy(
            src_ref=en.at[:, to],
            dst_ref=e_l.at[lane if start else to],
            send_sem=send.at[8 + k],
            recv_sem=recv.at[8 + k],
            device_id=(bank, to),
            device_id_type=MESH,
        )
        if start:
            copy.start()
            return None
        copy.wait_recv()
        return to

    def across(pick, dst, which):
        def one(to, carry):
            @pl.when(to != bank)
            def _():
                remote(pick(to), dst.at[bank], which, (to, lane))

            return carry

        lax.fori_loop(0, nb, one, 0)

    def arrived(dst, count, sems, which):
        most = dst.at[pl.ds(0, count - 1)]
        pltpu.make_async_copy(most, most, sems.at[which]).wait()

    def angle(layer, group):
        return cosines[layer : layer + 1, group : group + 1], sines[layer : layer + 1, group : group + 1]

    def mixed(layer, re, im, stride, stop, group):
        cosine, sine = (jnp.broadcast_to(x, re.shape[1:])[None, None] for x in angle(layer, group))
        while stride < stop:
            re, im = butterfly(re, im, stride, cosine, sine)
            stride *= 2
        return re, im

    def lane_table(layer):
        real, imag = turn_table(lanes, *angle(layer, 0))
        return split(jnp.concatenate([jnp.concatenate([real, imag], 1), jnp.concatenate([-imag, real], 1)], 0))

    def row_table(layer, count, places=None):
        real, imag = turn_table(count, *angle(layer, 1), places)
        return split(jnp.concatenate([jnp.concatenate([real, -imag], 1), jnp.concatenate([imag, real], 1)], 0))

    loads[0].wait()
    line()
    for k in range(1, nl):
        pl.when(known(lane ^ (nl - k)))(functools.partial(along_line, k, True))
    loads[1].wait()
    cosines, sines = jnp.cos(mix[...]), jnp.sin(mix[...])
    lane_first, row_first = lane_table(0), row_table(0, rows)
    lane_second, row_second = lane_table(1), row_table(1, lanes, step.bit_length() - 1)
    loads[2].wait()
    loads[3].wait()

    pairs = []
    for d in range(depth):
        e = en[pl.ds(d * units // nl, units // nl)].reshape(rows, lanes)
        sine, cosine = sin_cos(ph[0:1] * e)
        pairs.append((amp[0, d] * cosine + amp[1, d] * sine, amp[1, d] * cosine - amp[0, d] * sine))
    re = jnp.stack([p[0] for p in pairs]).reshape(depth, rows // 8, 8, lanes)
    im = jnp.stack([p[1] for p in pairs]).reshape(depth, rows // 8, 8, lanes)
    cosine, sine = (jnp.broadcast_to(x, (8, lanes))[None] for x in angle(0, 2))
    stride = 1
    while stride < depth:
        re, im = butterfly(re, im, stride, cosine, sine)
        stride *= 2
    re, im = re.reshape(depth, rows, lanes), im.reshape(depth, rows, lanes)
    for d in range(depth):
        both = dot3(split(jnp.concatenate([re[d], im[d]], 1)), lane_first)
        both = dot3(row_first, split(jnp.concatenate([both[:, :lanes], both[:, lanes:]], 0)))
        for i in range(2):
            x = both[i * rows : (i + 1) * rows].reshape(units, 2, step, lanes)
            for h in range(2):
                s_a[h, pl.ds(d * units, units), i] = x[:, h]

    all_of_line()
    for k in range(1, nl):
        pl.when(jnp.logical_not(known(lane ^ (nl - k))))(functools.partial(along_line, k, True))
    everyone()
    across(lambda to: en.at[to, lane], e_b.at[:, lane], 1)
    e_b[bank, lane] = en[bank, lane]
    exchange(s_a.at[0], b_b.at[0], 2, (1, 2, 0, 3))
    for k in range(1, nl):
        source = along_line(k, False)
        across(lambda to: e_l.at[source, to], e_b.at[:, source], 1)
        e_b[bank, source] = e_l[source, bank]
    exchange(s_a.at[1], b_b.at[1], 3, (1, 2, 0, 3))
    arrived(e_b, nb, recv, 1)
    sine, cosine = sin_cos(ph[1:2][None] * e_b[...].reshape(n, 2 * step, lanes))
    sn_b[...] = sine
    cs_b[...] = cosine

    for h in range(2):
        arrived(b_b.at[h], n, recv, 2 + h)
        span = pl.ds(h * step, step)
        re, im = b_b[h, :, 0], b_b[h, :, 1]
        re, im = mixed(0, re, im, 1, nl, 3)
        re, im = mixed(0, re, im, nl, n, 2)
        cosine, sine = cs_b[:, span], sn_b[:, span]
        re, im = re * cosine + im * sine, im * cosine - re * sine
        re, im = mixed(1, re, im, 1, nl, 3)
        re, im = mixed(1, re, im, nl, n, 2)
        re, im = re.reshape(n * step, lanes), im.reshape(n * step, lanes)
        both = dot3(split(jnp.concatenate([re, im], 1)), lane_second)
        groups = range(0, n * step, lanes)
        wide = [jnp.concatenate([both[g : g + lanes, i * lanes : (i + 1) * lanes] for g in groups], 1) for i in range(2)]
        both = dot3(row_second, split(jnp.concatenate(wide, 0)))
        for i in range(2):
            x = [both[i * lanes : (i + 1) * lanes, g : g + lanes] for g in groups]
            x = jnp.concatenate(x, 0).reshape(n, step, lanes)
            if h == 0:
                o_a[:, i] = x
            else:
                for s in range(2):
                    o_b[s, :, i] = x[:, s * half : (s + 1) * half]
        if h == 0:
            for to in [0,2,1,3]:
                pl.when(now(to))(functools.partial(send_lane, to, o_a, r_a, 4))
            r_a[me] = o_a[me]
        else:
            for to, s in [(0,0),(2,0),(0,1),(2,1),(1,-1),(1,0),(3,0),(1,1),(3,1)]:
                if s < 0:
                    pl.when(jnp.logical_not(now(to)))(functools.partial(send_lane, to, o_a, r_a, 4))
                else:
                    send_lane(to, o_b.at[s], r_b.at[s], 5 + s)
            for s in range(2):
                r_b[s, me] = o_b[s, me]

    arrived(r_a, n, recv, 4)
    re, im = mixed(1, r_a[:, 0], r_a[:, 1], 1, units, 1)
    re, im = mixed(1, re, im, units, n, 2)
    for s in range(2):
        part[s, 0] = re[:, s * half : (s + 1) * half]
        part[s, 1] = im[:, s * half : (s + 1) * half]

    for s in range(2):
        arrived(r_b.at[s], n, recv, 5 + s)
        vr, vi = mixed(1, r_b[s, :, 0], r_b[s, :, 1], 1, units, 1)
        vr, vi = mixed(1, vr, vi, units, n, 2)
        ur, ui = part[s, 0], part[s, 1]
        cosine, sine = (jnp.broadcast_to(x, (half, lanes))[None] for x in angle(1, 1))
        re = (cosine * ur + sine * vi, cosine * vr + sine * ui)
        im = (cosine * ui - sine * vr, cosine * vi - sine * ur)
        for h in range(2):
            chance = re[h] * re[h] + im[h] * im[h]
            for d in range(depth):
                ch[s, :, :, d, h] = chance[d * units : (d + 1) * units].reshape(nb // 2, 2, half, lanes)
        remote(ch.at[s, :, 1 - side], near.at[s], 8 + nl * s, (bank ^ 1, lane))
        for h in range(2):
            for i, x in enumerate((re[h], im[h])):
                out[i, :, :, h, s * half : (s + 1) * half] = x.reshape(depth, units, half, lanes)

    for s in range(2):
        pltpu.make_async_copy(near.at[s], near.at[s], recv.at[8 + nl * s]).wait()
        pair[s] = ch[s, :, side] + near[s]

        def one(to, carry):
            @pl.when(to != pairs_at)
            def _():
                remote(pair.at[s, to], m_in.at[s, pairs_at], 7 * s, (2 * to + side, lane))

            return carry

        lax.fori_loop(0, nb // 2, one, 0)
        m_in[s, pairs_at] = pair[s, pairs_at]
    for s in range(2):
        arrived(m_in.at[s], nb // 2, recv, 7 * s)
        total = m_in[s, 0]
        for g in range(1, nb // 2):
            total = total + m_in[s, g]
        marg[:, :, s * half : (s + 1) * half] = total * (1.0 / nb)
    for k in range(1, nl):
        pltpu.make_async_copy(en.at[:, 0], e_l.at[0], send.at[8 + k]).wait()
    arrived(e_b, nb, send, 1)
    for h in range(2):
        arrived(b_b.at[h], n, send, 2 + h)
        arrived(r_b.at[h], n, send, 5 + h)
        arrived(m_in.at[h], nb // 2, send, 7 * h)
        pltpu.make_async_copy(near.at[h], near.at[h], send.at[8 + nl * h]).wait()
    arrived(r_a, n, send, 4)


def keep(a, b, a_hbm, b_hbm, sems):
    copies = [pltpu.make_async_copy(a, a_hbm, sems.at[0]), pltpu.make_async_copy(b, b_hbm, sems.at[1])]
    for copy in copies:
        copy.start()
    for copy in copies:
        copy.wait()


def in_pieces(nb, nl, amplitudes, energies, phase_angles, mix_angles):
    _, depth, rows, lanes = amplitudes.shape
    n = nb * nl
    per = depth * rows // n
    step, half = per // 2, per // 4
    f32 = jnp.float32
    vmem = pl.BlockSpec(memory_space=pltpu.VMEM)
    anywhere = pl.BlockSpec(memory_space=pl.ANY)
    state = pltpu.VMEM((2, n, 2, step, lanes), f32)
    level = pltpu.VMEM((n, per, lanes), f32)
    spread = pltpu.VMEM((nb, nl, per, lanes), f32)
    shapes = (2, depth, nb, 2, step, lanes), (depth, 2, step, lanes)
    results = pl.pallas_call(
        functools.partial(pieces, nb, nl),
        name="register",
        out_shape=tuple(pltpu.VMEM(shape, f32) for shape in shapes),
        in_specs=[anywhere] * 4,
        out_specs=(vmem, vmem),
        scratch_shapes=[
            pltpu.VMEM(phase_angles.shape, f32),
            pltpu.VMEM(mix_angles.shape, f32),
            pltpu.VMEM((2, depth, rows, lanes), f32),
            spread,
            pltpu.VMEM((nl, nb, per, lanes), f32),
            state,
            spread,
            state,
            pltpu.VMEM((n, 2, step, lanes), f32),
            pltpu.VMEM((2, n, 2, half, lanes), f32),
            pltpu.VMEM((n, 2, step, lanes), f32),
            pltpu.VMEM((2, n, 2, half, lanes), f32),
            level,
            level,
            pltpu.VMEM((2, 2, n, half, lanes), f32),
            pltpu.VMEM((2, nb // 2, 2, depth, 2, half, lanes), f32),
            pltpu.VMEM((2, nb // 2, depth, 2, half, lanes), f32),
            pltpu.VMEM((2, nb // 2, depth, 2, half, lanes), f32),
            pltpu.VMEM((2, nb // 2, depth, 2, half, lanes), f32),
            pltpu.SemaphoreType.DMA((4,)),
            pltpu.SemaphoreType.DMA((9 + nl,)),
            pltpu.SemaphoreType.DMA((9 + nl,)),
            *[pltpu.SemaphoreType.REGULAR] * 4,
        ],
        compiler_params=pltpu.CompilerParams(collective_id=0, has_side_effects=True),
    )(amplitudes, energies.reshape(nb, nl, per, lanes), phase_angles, mix_angles)
    final, marginal = pl.pallas_call(
        keep,
        name="keep",
        out_shape=tuple(jax.ShapeDtypeStruct(shape, f32) for shape in shapes),
        in_specs=[vmem, vmem],
        out_specs=(anywhere, anywhere),
        scratch_shapes=[pltpu.SemaphoreType.DMA((2,))],
    )(*[pltpu.with_memory_space_constraint(x, pltpu.VMEM) for x in results])
    return final.reshape(amplitudes.shape), marginal.reshape(depth, rows // nb, lanes)


def on_device(nb, nl, amplitudes, energies, phase_angles, mix_angles):
    _, depth, rows, lanes = amplitudes.shape
    n = nb * nl
    per = depth * rows // n
    halves = 2 if per % 16 == 0 else 1
    piece = rows // nb
    if per == 2 * 8 and piece == per and rows // per % nl == 0 and n * 8 % lanes == 0:
        return in_pieces(nb, nl, amplitudes, energies, phase_angles, mix_angles)
    f32 = jnp.float32
    state = pltpu.VMEM((halves, n, 2, per // halves, lanes), f32)
    level = pltpu.VMEM((n, per, lanes), f32)
    spread = pltpu.VMEM((nb, nl, per, lanes), f32)
    vmem = pl.BlockSpec(memory_space=pltpu.VMEM)
    anywhere = pl.BlockSpec(memory_space=pl.ANY)
    whole = pltpu.VMEM((2, depth, rows, lanes), f32)
    return pl.pallas_call(
        functools.partial(kernel, nb, nl, halves),
        name="register",
        out_shape=(pltpu.VMEM(amplitudes.shape, f32), pltpu.VMEM((depth, piece, lanes), f32)),
        in_specs=[anywhere] * 4,
        out_specs=(vmem, vmem),
        scratch_shapes=[
            pltpu.VMEM(phase_angles.shape, f32),
            pltpu.VMEM(mix_angles.shape, f32),
            whole,
            spread,
            pltpu.VMEM((nl, nb, per, lanes), f32),
            whole if per % 8 else pltpu.VMEM((1, 1, 8, 128), f32),
            state,
            spread,
            state,
            state,
            state,
            level,
            level,
            pltpu.VMEM((2, depth, rows // halves, lanes), f32),
            pltpu.VMEM((depth, nb, piece, lanes), f32),
            pltpu.VMEM((nb, depth, piece, lanes), f32),
            pltpu.SemaphoreType.DMA((4,)),
            pltpu.SemaphoreType.DMA((2 * halves + 3,)),
            pltpu.SemaphoreType.DMA((2 * halves + 3,)),
            pltpu.SemaphoreType.REGULAR,
            pltpu.SemaphoreType.REGULAR,
            pltpu.SemaphoreType.REGULAR,
        ],
        compiler_params=pltpu.CompilerParams(collective_id=0, has_side_effects=True),
    )(amplitudes, energies.reshape(nb, nl, per, lanes), phase_angles, mix_angles)


def solution(mesh):
    placed = (P(None, ("bank", "lane"), None, None), P(("bank", "lane"), None, None), P(), P())
    return jax.shard_map(
        functools.partial(on_device, mesh.shape["bank"], mesh.shape["lane"]),
        mesh=mesh,
        in_specs=placed,
        out_specs=(P(None, ("bank", "lane"), None, None), P("lane", "bank", None)),
        check_vma=False,
    )
```

```python
import functools

import jax
import jax.numpy as jnp
from jax import lax
from jax.experimental import pallas as pl
from jax.experimental.pallas import tpu as pltpu
from jax.sharding import PartitionSpec as P

MESH = pl.DeviceIdType.MESH
SIN = (1.0, -1 / 6, 1 / 120, -1 / 5040, 1 / 362880, -1 / 39916800, 1 / 6227020800, -1 / 1307674368000)
COS = (1.0, -1 / 2, 1 / 24, -1 / 720, 1 / 40320, -1 / 3628800, 1 / 479001600, -1 / 87178291200, 1 / 20922789888000)


def series(square, terms):
    total = jnp.full_like(square, terms[-1])
    for term in terms[-2::-1]:
        total = total * square + term
    return total


def sin_cos(turn):
    square = turn * turn
    return turn * series(square, SIN), series(square, COS)


def split(x):
    high = x.astype(jnp.bfloat16)
    return high, (x - high.astype(jnp.float32)).astype(jnp.bfloat16)


def dot3(a, b):
    def one(x, y):
        return lax.dot_general(x, y, (((1,), (0,)), ((), ())), preferred_element_type=jnp.float32)

    return one(a[0], b[0]) + (one(a[1], b[0]) + one(a[0], b[1]))


def turn_table(count, cosine, sine, places=None):
    places = count.bit_length() - 1 if places is None else places
    row = lax.broadcasted_iota(jnp.int32, (count, count), 0)
    col = lax.broadcasted_iota(jnp.int32, (count, count), 1)
    apart = row ^ col
    size = jnp.ones((count, count), jnp.float32)
    ones = jnp.zeros((count, count), jnp.int32)
    for place in range(places):
        bit = (apart >> place) & 1
        size = size * jnp.where(bit == 1, sine, cosine)
        ones = ones + bit
    size = jnp.where(apart >> places == 0, size, 0.0)
    phase = ones & 3
    real = jnp.where(phase == 0, size, jnp.where(phase == 2, -size, 0.0))
    imag = jnp.where(phase == 1, -size, jnp.where(phase == 3, size, 0.0))
    return real, imag


def butterfly(re, im, stride, cosine, sine):
    count, rest = re.shape[0], re.shape[1:]
    parts = (count // (2 * stride), 2, stride) + rest
    re, im = re.reshape(parts), im.reshape(parts)
    ur, vr, ui, vi = re[:, 0], re[:, 1], im[:, 0], im[:, 1]
    new_re = jnp.stack([cosine * ur + sine * vi, cosine * vr + sine * ui], axis=1)
    new_im = jnp.stack([cosine * ui - sine * vr, cosine * vi - sine * ur], axis=1)
    return new_re.reshape((count,) + rest), new_im.reshape((count,) + rest)


def kernel(
    nb, nl, halves, amp_hbm, en_hbm, ph_hbm, mix_hbm, out, marg,
    ph, mix, amp, en, e_l, tmp, s_a, e_b, b_b, o_b, r_a, cs_b, sn_b, part_done, ch, m_in, load, send, recv, line_in, lines_in, all_in,
):
    n = nb * nl
    depth, rows, lanes = amp.shape[1:]
    per = en.shape[2]
    step = per // halves
    tiled = per % 8 == 0
    units = rows // per
    piece = rows // nb
    last = 2 * halves + 2
    hub = nl // 2 - 1
    bank, lane = lax.axis_index("bank"), lax.axis_index("lane")
    me = bank * nl + lane

    load_en = pltpu.make_async_copy(en_hbm, en, load.at[0])
    load_amp = pltpu.make_async_copy(amp_hbm, amp, load.at[1])
    load_ph = pltpu.make_async_copy(ph_hbm, ph, load.at[2])
    load_mix = pltpu.make_async_copy(mix_hbm, mix, load.at[3])
    barrier = pltpu.get_barrier_semaphore()

    def partner(k):
        return lax.rem(bank + nb - lax.rem(k, nb), nb), lax.rem(lane + k // nb, nl)

    def greet_line(k, carry):
        to = lax.rem(lane + k, nl)

        @pl.when(to != hub)
        def _():
            pl.semaphore_signal(barrier, 1, device_id=(bank, to), device_id_type=MESH)

        return carry

    def signal_hubs(sem):
        def one(k, carry):
            pl.semaphore_signal(sem, 1, device_id=(lax.rem(bank + k, nb), hub), device_id_type=MESH)
            return carry

        lax.fori_loop(1, nb, one, 0)

    @pl.when(lane == hub)
    def _():
        signal_hubs(barrier)

    lax.fori_loop(1, nl, greet_line, 0)
    load_en.start()
    load_mix.start()
    load_amp.start()
    load_ph.start()

    def exchange(src, dst, which):
        def one(k, carry):
            to_bank, to_lane = partner(k)
            pltpu.make_async_remote_copy(
                src_ref=src.at[to_bank * nl + to_lane],
                dst_ref=dst.at[me],
                send_sem=send.at[which],
                recv_sem=recv.at[which],
                device_id=(to_bank, to_lane),
                device_id_type=MESH,
            ).start()
            return carry

        lax.fori_loop(1, n, one, 0)
        dst[me] = src[me]

    def arrived(dst, count, sems, which):
        most = dst.at[pl.ds(0, count - 1)]
        pltpu.make_async_copy(most, most, sems.at[which]).wait()

    load_en.wait()
    pl.semaphore_wait(barrier, jnp.where(lane == hub, nb - 1, nl - 1))

    @pl.when(lane == hub + 1)
    def _():
        pl.semaphore_signal(line_in, 1, device_id=(bank, hub), device_id_type=MESH)

    @pl.when(lane == hub)
    def _():
        pl.semaphore_wait(line_in, 1)
        signal_hubs(lines_in)

    def along_line(k, carry):
        to = lax.rem(lane + k, nl)
        pltpu.make_async_remote_copy(
            src_ref=en.at[:, to],
            dst_ref=e_l.at[lane],
            send_sem=send.at[0],
            recv_sem=recv.at[0],
            device_id=(bank, to),
            device_id_type=MESH,
        ).start()
        return carry

    lax.fori_loop(1, nl, along_line, 0)
    e_l[lane] = en[:, lane]
    load_mix.wait()
    cosines, sines = jnp.cos(mix[...]), jnp.sin(mix[...])

    def angle(layer, group):
        return cosines[layer : layer + 1, group : group + 1], sines[layer : layer + 1, group : group + 1]

    def tables(layer, count):
        real, imag = turn_table(lanes, *angle(layer, 0))
        by_lane = split(jnp.concatenate([jnp.concatenate([real, imag], 1), jnp.concatenate([-imag, real], 1)], 0))
        real, imag = turn_table(count, *angle(layer, 1))
        by_row = split(jnp.concatenate([jnp.concatenate([real, -imag], 1), jnp.concatenate([imag, real], 1)], 0))
        return by_lane, by_row

    def local_mix(layer, by_lane, by_row, count, read, write):
        pairs = [read(d) for d in range(depth)]
        stride = 1
        cosine, sine = (jnp.broadcast_to(x, (8, lanes))[None] for x in angle(layer, 2))
        re = jnp.stack([p[0] for p in pairs]).reshape(depth, count // 8, 8, lanes)
        im = jnp.stack([p[1] for p in pairs]).reshape(depth, count // 8, 8, lanes)
        while stride < depth:
            re, im = butterfly(re, im, stride, cosine, sine)
            stride *= 2
        re, im = re.reshape(depth, count, lanes), im.reshape(depth, count, lanes)
        for d in range(depth):
            both = dot3(split(jnp.concatenate([re[d], im[d]], 1)), by_lane)
            both = dot3(by_row, split(jnp.concatenate([both[:, :lanes], both[:, lanes:]], 0)))
            write(d, both[:count], both[count:])

    first_tables = tables(0, rows)
    second_tables = tables(1, rows // halves)

    load_amp.wait()
    load_ph.wait()

    def first(d):
        if tiled:
            e = en[pl.ds(d * units // nl, units // nl)].reshape(rows, lanes)
        else:
            e = tmp[0, d]
        sine, cosine = sin_cos(ph[0:1] * e)
        return amp[0, d] * cosine + amp[1, d] * sine, amp[1, d] * cosine - amp[0, d] * sine

    def to_units(d, re, im):
        if tiled:
            for part, x in enumerate((re, im)):
                x = x.reshape(units, halves, step, lanes)
                for h in range(halves):
                    s_a[h, pl.ds(d * units, units), part] = x[:, h]
        else:
            tmp[0, d] = re
            tmp[1, d] = im

    if not tiled:
        for d in range(depth):

            def spread(u, carry):
                tmp[0, d, pl.ds(u * per, per)] = en[(d * units + u) // nl, lax.rem(d * units + u, nl)]
                return carry

            lax.fori_loop(0, units, spread, 0)
    local_mix(0, *first_tables, rows, first, to_units)
    if not tiled:
        for d in range(depth):

            def gather(u, carry):
                for part in range(2):
                    s_a[0, d * units + u, part] = tmp[part, d, pl.ds(u * per, per)]
                return carry

            lax.fori_loop(0, units, gather, 0)

    @pl.when(lane == hub)
    def _():
        pl.semaphore_wait(lines_in, nb - 1)

        def tell(k, carry):
            pl.semaphore_signal(all_in, 1, device_id=(bank, lax.rem(lane + k, nl)), device_id_type=MESH)
            return carry

        lax.fori_loop(1, nl, tell, 0)

    @pl.when(lane != hub)
    def _():
        pl.semaphore_wait(all_in, 1)

    exchange(s_a.at[0], b_b.at[0], 1)
    arrived(e_l, nl, recv, 0)

    def across(k, carry):
        to = lax.rem(bank + k, nb)
        pltpu.make_async_remote_copy(
            src_ref=e_l.at[:, to],
            dst_ref=e_b.at[bank],
            send_sem=send.at[last - 1],
            recv_sem=recv.at[last - 1],
            device_id=(to, lane),
            device_id_type=MESH,
        ).start()
        return carry

    lax.fori_loop(1, nb, across, 0)
    e_b[bank] = e_l[:, bank]
    for h in range(1, halves):
        exchange(s_a.at[h], b_b.at[h], 1 + h)
    arrived(e_b, nb, recv, last - 1)
    sine, cosine = sin_cos(ph[1:2][None] * e_b[...].reshape(n, per, lanes))
    sn_b[...] = sine
    cs_b[...] = cosine

    for h in range(halves):
        arrived(b_b.at[h], n, recv, 1 + h)
        span = pl.ds(h * step, step)
        re, im = b_b[h, :, 0], b_b[h, :, 1]
        for layer in range(2):
            stride = 1
            while stride < n:
                cosine, sine = (
                    jnp.broadcast_to(x, (step, lanes))[None, None] for x in angle(layer, 3 if stride < nl else 2)
                )
                re, im = butterfly(re, im, stride, cosine, sine)
                stride *= 2
            if layer == 0:
                cosine, sine = cs_b[:, span], sn_b[:, span]
                re, im = re * cosine + im * sine, im * cosine - re * sine
        o_b[h, :, 0] = re
        o_b[h, :, 1] = im
        exchange(o_b.at[h], r_a.at[h], 1 + halves + h)

    def second(h, d):
        if tiled:
            return tuple(
                r_a[h, pl.ds(d * units, units), part].reshape(rows // halves, lanes) for part in range(2)
            )
        return tmp[0, d], tmp[1, d]

    def keep(d, re, im):
        part_done[0, d] = re
        part_done[1, d] = im

    def pass_on(d):
        def one(k, carry):
            to_bank = lax.rem(bank + k, nb)
            pltpu.make_async_remote_copy(
                src_ref=ch.at[d, to_bank],
                dst_ref=m_in.at[bank, d],
                send_sem=send.at[last],
                recv_sem=recv.at[last],
                device_id=(to_bank, lane),
                device_id_type=MESH,
            ).start()
            return carry

        lax.fori_loop(1, nb, one, 0)
        m_in[bank, d] = ch[d, bank]

    def finish(d, re, im):
        if halves == 2:
            cosine, sine = angle(1, 1)
            ur, ui, vr, vi = part_done[0, d], part_done[1, d], re, im
            shape = (units, 1, step, lanes)
            re = [cosine * ur + sine * vi, cosine * vr + sine * ui]
            im = [cosine * ui - sine * vr, cosine * vi - sine * ur]
            re = jnp.concatenate([x.reshape(shape) for x in re], 1).reshape(rows, lanes)
            im = jnp.concatenate([x.reshape(shape) for x in im], 1).reshape(rows, lanes)
        chance = re * re + im * im
        for g in range(nb):
            ch[d, g] = chance[g * piece : (g + 1) * piece]
        out[0, d] = re
        out[1, d] = im
        pass_on(d)

    for h in range(halves):
        arrived(r_a.at[h], n, recv, 1 + halves + h)
        if not tiled:
            for d in range(depth):

                def place(u, carry):
                    for part in range(2):
                        tmp[part, d, pl.ds(u * per, per)] = r_a[h, d * units + u, part]
                    return carry

                lax.fori_loop(0, units, place, 0)
        write = finish if h == halves - 1 else keep
        local_mix(1, *second_tables, rows // halves, functools.partial(second, h), write)

    arrived(m_in, nb, recv, last)
    total = m_in[0]
    for g in range(1, nb):
        total = total + m_in[g]
    marg[...] = total * (1.0 / nb)
    arrived(e_l, nl, send, 0)
    arrived(e_b, nb, send, last - 1)
    for h in range(halves):
        arrived(b_b.at[h], n, send, 1 + h)
        arrived(r_a.at[h], n, send, 1 + halves + h)
    arrived(m_in, nb, send, last)


def contact(nb, nl, bank, lane, line_in, last_in, lines_in, all_in):
    barrier = pltpu.get_barrier_semaphore()
    last = nl - 1
    is_hub, is_last = lane == 0, lane == last
    between = jnp.logical_not(jnp.logical_or(is_hub, is_last))

    def signal(sem, to_bank, to_lane):
        pl.semaphore_signal(sem, 1, device_id=(to_bank, to_lane), device_id_type=MESH)

    def signal_hubs(sem):
        def one(k, carry):
            signal(sem, lax.rem(bank + k, nb), 0)
            return carry

        lax.fori_loop(1, nb, one, 0)

    def greet():
        @pl.when(is_last)
        def _():
            signal(barrier, bank, 0)

        @pl.when(jnp.logical_not(is_last))
        def _():
            for to in range(last, 0, -1):

                @pl.when(lane != to)
                def _():
                    signal(barrier, bank, to)

        @pl.when(is_hub)
        def _():
            signal_hubs(barrier)

    def line():
        pl.semaphore_wait(barrier, jnp.where(is_hub, nb, jnp.where(is_last, last, last - 1)))

        @pl.when(lane == 1)
        def _():
            signal(line_in, bank, 0)

        @pl.when(is_hub)
        def _():
            pl.semaphore_wait(line_in, 1)
            for to in range(1, last):
                signal(last_in, bank, to)
            signal_hubs(lines_in)

    def all_of_line():
        @pl.when(between)
        def _():
            pl.semaphore_wait(last_in, 1)

    def everyone():
        @pl.when(is_hub)
        def _():
            pl.semaphore_wait(lines_in, nb - 1)
            for to in range(last, 0, -1):
                signal(all_in, bank, to)

        @pl.when(jnp.logical_not(is_hub))
        def _():
            pl.semaphore_wait(all_in, 1)

    def known(to):
        return jnp.logical_not(jnp.logical_and(between, to == last))

    return greet, line, all_of_line, everyone, known


def pieces(
    nb, nl, amp_hbm, en_hbm, ph_hbm, mix_hbm, out, marg,
    ph, mix, turns, amp, en, e_l, s_a, e_b, b_b, o_a, o_b, r_a, r_b, cs_b, sn_b, part, ch, near, pair, m_in,
    load, send, recv, *met,
):
    n = nb * nl
    depth, rows, lanes = amp.shape[1:]
    step = s_a.shape[3]
    half = step // 2
    units = rows // (2 * step)
    bank, lane = lax.axis_index("bank"), lax.axis_index("lane")
    me = bank * nl + lane
    side, pairs_at = lax.rem(bank, 2), bank // 2
    greet, line, all_of_line, everyone, known = contact(nb, nl, bank, lane, *met)
    loads = [
        pltpu.make_async_copy(x, y, load.at[i])
        for i, (x, y) in enumerate([(en_hbm, en), (mix_hbm, mix), (amp_hbm, amp), (ph_hbm, ph)])
    ]
    greet()
    for copy in loads:
        copy.start()

    def remote(src, dst, which, to):
        pltpu.make_async_remote_copy(
            src_ref=src,
            dst_ref=dst,
            send_sem=send.at[which],
            recv_sem=recv.at[which],
            device_id=to,
            device_id_type=MESH,
        ).start()

    def send_lane(to_lane, src, dst, which):
        def one(k, carry):
            to_bank = lax.rem(bank + k, nb)

            @pl.when(to_bank * nl + to_lane != me)
            def _():
                remote(src.at[to_bank * nl + to_lane], dst.at[me], which, (to_bank, to_lane))

            return carry

        lax.fori_loop(0, nb, one, 0)

    def now(to):
        return jnp.logical_or(lane != 2, to != 1)

    other = jnp.where(lane < nl // 2, nl // 2, 0)
    role = {"a": other, "b": other + 1, "t": lane ^ 1, "p": lane}

    def exchange(src, dst, which, order):
        for to in order:
            send_lane(role.get(to, to), src, dst, which)
        dst[me] = src[me]

    def along_line(k, start):
        to = lane ^ (nl - k)
        copy = pltpu.make_async_remote_copy(
            src_ref=en_hbm.at[:, to],
            dst_ref=e_l.at[lane if start else to],
            send_sem=send.at[8 + k],
            recv_sem=recv.at[8 + k],
            device_id=(bank, to),
            device_id_type=MESH,
        )
        if start:
            copy.start()
            return None
        copy.wait_recv()
        return to

    def across(pick, dst, which):
        def one(to, carry):
            @pl.when(to != bank)
            def _():
                remote(pick(to), dst.at[bank], which, (to, lane))

            return carry

        lax.fori_loop(0, nb, one, 0)

    def arrived(dst, count, sems, which):
        most = dst.at[pl.ds(0, count - 1)]
        pltpu.make_async_copy(most, most, sems.at[which]).wait()

    def angle(layer, group):
        return tuple(turns[i, layer : layer + 1, group : group + 1] for i in range(2))

    def mixed(layer, re, im, stride, stop, group):
        cosine, sine = (jnp.broadcast_to(x, re.shape[1:])[None, None] for x in angle(layer, group))
        while stride < stop:
            re, im = butterfly(re, im, stride, cosine, sine)
            stride *= 2
        return re, im

    def lane_table(layer):
        real, imag = turn_table(lanes, *angle(layer, 0))
        return split(jnp.concatenate([jnp.concatenate([real, imag], 1), jnp.concatenate([-imag, real], 1)], 0))

    def row_table(layer, count, places=None):
        real, imag = turn_table(count, *angle(layer, 1), places)
        return split(jnp.concatenate([jnp.concatenate([real, -imag], 1), jnp.concatenate([imag, real], 1)], 0))

    def prepare():
        loads[0].wait()
        loads[1].wait()
        turns[0] = jnp.cos(mix[...])
        turns[1] = jnp.sin(mix[...])
        lane_first, row_first = lane_table(0), row_table(0, rows)
        loads[2].wait()
        loads[3].wait()

        pairs = []
        for d in range(depth):
            e = en[pl.ds(d * units // nl, units // nl)].reshape(rows, lanes)
            sine, cosine = sin_cos(ph[0:1] * e)
            pairs.append((amp[0, d] * cosine + amp[1, d] * sine, amp[1, d] * cosine - amp[0, d] * sine))
        re = jnp.stack([p[0] for p in pairs]).reshape(depth, rows // 8, 8, lanes)
        im = jnp.stack([p[1] for p in pairs]).reshape(depth, rows // 8, 8, lanes)
        cosine, sine = (jnp.broadcast_to(x, (8, lanes))[None] for x in angle(0, 2))
        stride = 1
        while stride < depth:
            re, im = butterfly(re, im, stride, cosine, sine)
            stride *= 2
        re, im = re.reshape(depth, rows, lanes), im.reshape(depth, rows, lanes)
        for d in range(depth):
            both = dot3(split(jnp.concatenate([re[d], im[d]], 1)), lane_first)
            both = dot3(row_first, split(jnp.concatenate([both[:, :lanes], both[:, lanes:]], 0)))
            for i in range(2):
                x = both[i * rows : (i + 1) * rows].reshape(units, 2, step, lanes)
                for h in range(2):
                    s_a[h, pl.ds(d * units, units), i] = x[:, h]

    pl.when(lane == 0)(prepare)
    line()
    for k in range(1, nl):
        pl.when(known(lane ^ (nl - k)))(functools.partial(along_line, k, True))
    pl.when(lane != 0)(prepare)
    all_of_line()
    for k in range(1, nl):
        pl.when(jnp.logical_not(known(lane ^ (nl - k))))(functools.partial(along_line, k, True))
    everyone()
    across(lambda to: en.at[to, lane], e_b.at[:, lane], 1)
    e_b[bank, lane] = en[bank, lane]
    exchange(s_a.at[0], b_b.at[0], 2, (1, 2, 0, 3))
    lane_second, row_second = lane_table(1), row_table(1, lanes, step.bit_length() - 1)
    for k in range(1, nl):
        source = along_line(k, False)
        across(lambda to: e_l.at[source, to], e_b.at[:, source], 1)
        e_b[bank, source] = e_l[source, bank]
    exchange(s_a.at[1], b_b.at[1], 3, (1, 2, 0, 3))
    arrived(e_b, nb, recv, 1)
    sine, cosine = sin_cos(ph[1:2][None] * e_b[...].reshape(n, 2 * step, lanes))
    sn_b[...] = sine
    cs_b[...] = cosine

    for h in range(2):
        arrived(b_b.at[h], n, recv, 2 + h)
        span = pl.ds(h * step, step)
        re, im = b_b[h, :, 0], b_b[h, :, 1]
        re, im = mixed(0, re, im, 1, nl, 3)
        re, im = mixed(0, re, im, nl, n, 2)
        cosine, sine = cs_b[:, span], sn_b[:, span]
        re, im = re * cosine + im * sine, im * cosine - re * sine
        re, im = mixed(1, re, im, 1, nl, 3)
        re, im = mixed(1, re, im, nl, n, 2)
        re, im = re.reshape(n * step, lanes), im.reshape(n * step, lanes)
        both = dot3(split(jnp.concatenate([re, im], 1)), lane_second)
        groups = range(0, n * step, lanes)
        wide = [jnp.concatenate([both[g : g + lanes, i * lanes : (i + 1) * lanes] for g in groups], 1) for i in range(2)]
        both = dot3(row_second, split(jnp.concatenate(wide, 0)))
        for i in range(2):
            x = [both[i * lanes : (i + 1) * lanes, g : g + lanes] for g in groups]
            x = jnp.concatenate(x, 0).reshape(n, step, lanes)
            if h == 0:
                o_a[:, i] = x
            else:
                for s in range(2):
                    o_b[s, :, i] = x[:, s * half : (s + 1) * half]
        if h == 0:
            for to in [role.get(x, x) for x in 'abtp']:
                pl.when(now(to))(functools.partial(send_lane, to, o_a, r_a, 4))
            r_a[me] = o_a[me]
        else:
            for to, s in [(role.get(x, x), s) for x, s in [('a', 0), ('p', 0), ('a', 1), ('b', -1), ('p', 1), ('b', 0), ('t', 0), ('b', 1), ('t', 1)]]:
                if s < 0:
                    pl.when(jnp.logical_not(now(to)))(functools.partial(send_lane, to, o_a, r_a, 4))
                else:
                    send_lane(to, o_b.at[s], r_b.at[s], 5 + s)
            for s in range(2):
                r_b[s, me] = o_b[s, me]

    arrived(r_a, n, recv, 4)
    re, im = mixed(1, r_a[:, 0], r_a[:, 1], 1, units, 1)
    re, im = mixed(1, re, im, units, n, 2)
    for s in range(2):
        part[s, 0] = re[:, s * half : (s + 1) * half]
        part[s, 1] = im[:, s * half : (s + 1) * half]

    for s in range(2):
        arrived(r_b.at[s], n, recv, 5 + s)
        vr, vi = mixed(1, r_b[s, :, 0], r_b[s, :, 1], 1, units, 1)
        vr, vi = mixed(1, vr, vi, units, n, 2)
        ur, ui = part[s, 0], part[s, 1]
        cosine, sine = (jnp.broadcast_to(x, (half, lanes))[None] for x in angle(1, 1))
        re = (cosine * ur + sine * vi, cosine * vr + sine * ui)
        im = (cosine * ui - sine * vr, cosine * vi - sine * ur)
        for h in range(2):
            chance = re[h] * re[h] + im[h] * im[h]
            for d in range(depth):
                ch[s, :, :, d, h] = chance[d * units : (d + 1) * units].reshape(nb // 2, 2, half, lanes)
        remote(ch.at[s, :, 1 - side], near.at[s], 8 + nl * s, (bank ^ 1, lane))
        for h in range(2):
            for i, x in enumerate((re[h], im[h])):
                out[i, :, :, h, s * half : (s + 1) * half] = x.reshape(depth, units, half, lanes)

    for s in range(2):
        pltpu.make_async_copy(near.at[s], near.at[s], recv.at[8 + nl * s]).wait()
        pair[s] = ch[s, :, side] + near[s]

        def one(to, carry):
            @pl.when(to != pairs_at)
            def _():
                remote(pair.at[s, to], m_in.at[s, pairs_at], 7 * s, (2 * to + side, lane))

            return carry

        lax.fori_loop(0, nb // 2, one, 0)
        m_in[s, pairs_at] = pair[s, pairs_at]
    for s in range(2):
        arrived(m_in.at[s], nb // 2, recv, 7 * s)
        total = m_in[s, 0]
        for g in range(1, nb // 2):
            total = total + m_in[s, g]
        marg[:, :, s * half : (s + 1) * half] = total * (1.0 / nb)
    for k in range(1, nl):
        pltpu.make_async_copy(en.at[:, 0], e_l.at[0], send.at[8 + k]).wait()
    arrived(e_b, nb, send, 1)
    for h in range(2):
        arrived(b_b.at[h], n, send, 2 + h)
        arrived(r_b.at[h], n, send, 5 + h)
        arrived(m_in.at[h], nb // 2, send, 7 * h)
        pltpu.make_async_copy(near.at[h], near.at[h], send.at[8 + nl * h]).wait()
    arrived(r_a, n, send, 4)


def keep(a, b, a_hbm, b_hbm, sems):
    copies = [pltpu.make_async_copy(a, a_hbm, sems.at[0]), pltpu.make_async_copy(b, b_hbm, sems.at[1])]
    for copy in copies:
        copy.start()
    for copy in copies:
        copy.wait()


def in_pieces(nb, nl, amplitudes, energies, phase_angles, mix_angles):
    _, depth, rows, lanes = amplitudes.shape
    n = nb * nl
    per = depth * rows // n
    step, half = per // 2, per // 4
    f32 = jnp.float32
    vmem = pl.BlockSpec(memory_space=pltpu.VMEM)
    anywhere = pl.BlockSpec(memory_space=pl.ANY)
    state = pltpu.VMEM((2, n, 2, step, lanes), f32)
    level = pltpu.VMEM((n, per, lanes), f32)
    spread = pltpu.VMEM((nb, nl, per, lanes), f32)
    shapes = (2, depth, nb, 2, step, lanes), (depth, 2, step, lanes)
    results = pl.pallas_call(
        functools.partial(pieces, nb, nl),
        name="register",
        out_shape=tuple(pltpu.VMEM(shape, f32) for shape in shapes),
        in_specs=[anywhere] * 4,
        out_specs=(vmem, vmem),
        scratch_shapes=[
            pltpu.VMEM(phase_angles.shape, f32),
            pltpu.VMEM(mix_angles.shape, f32),
            pltpu.VMEM((2, *mix_angles.shape), f32),
            pltpu.VMEM((2, depth, rows, lanes), f32),
            spread,
            pltpu.VMEM((nl, nb, per, lanes), f32),
            state,
            spread,
            state,
            pltpu.VMEM((n, 2, step, lanes), f32),
            pltpu.VMEM((2, n, 2, half, lanes), f32),
            pltpu.VMEM((n, 2, step, lanes), f32),
            pltpu.VMEM((2, n, 2, half, lanes), f32),
            level,
            level,
            pltpu.VMEM((2, 2, n, half, lanes), f32),
            pltpu.VMEM((2, nb // 2, 2, depth, 2, half, lanes), f32),
            pltpu.VMEM((2, nb // 2, depth, 2, half, lanes), f32),
            pltpu.VMEM((2, nb // 2, depth, 2, half, lanes), f32),
            pltpu.VMEM((2, nb // 2, depth, 2, half, lanes), f32),
            pltpu.SemaphoreType.DMA((4,)),
            pltpu.SemaphoreType.DMA((9 + nl,)),
            pltpu.SemaphoreType.DMA((9 + nl,)),
            *[pltpu.SemaphoreType.REGULAR] * 4,
        ],
        compiler_params=pltpu.CompilerParams(collective_id=0, has_side_effects=True),
    )(amplitudes, energies.reshape(nb, nl, per, lanes), phase_angles, mix_angles)
    final, marginal = pl.pallas_call(
        keep,
        name="keep",
        out_shape=tuple(jax.ShapeDtypeStruct(shape, f32) for shape in shapes),
        in_specs=[vmem, vmem],
        out_specs=(anywhere, anywhere),
        scratch_shapes=[pltpu.SemaphoreType.DMA((2,))],
    )(*[pltpu.with_memory_space_constraint(x, pltpu.VMEM) for x in results])
    return final.reshape(amplitudes.shape), marginal.reshape(depth, rows // nb, lanes)


def on_device(nb, nl, amplitudes, energies, phase_angles, mix_angles):
    _, depth, rows, lanes = amplitudes.shape
    n = nb * nl
    per = depth * rows // n
    halves = 2 if per % 16 == 0 else 1
    piece = rows // nb
    if per == 2 * 8 and piece == per and rows // per % nl == 0 and n * 8 % lanes == 0:
        return in_pieces(nb, nl, amplitudes, energies, phase_angles, mix_angles)
    f32 = jnp.float32
    state = pltpu.VMEM((halves, n, 2, per // halves, lanes), f32)
    level = pltpu.VMEM((n, per, lanes), f32)
    spread = pltpu.VMEM((nb, nl, per, lanes), f32)
    vmem = pl.BlockSpec(memory_space=pltpu.VMEM)
    anywhere = pl.BlockSpec(memory_space=pl.ANY)
    whole = pltpu.VMEM((2, depth, rows, lanes), f32)
    return pl.pallas_call(
        functools.partial(kernel, nb, nl, halves),
        name="register",
        out_shape=(pltpu.VMEM(amplitudes.shape, f32), pltpu.VMEM((depth, piece, lanes), f32)),
        in_specs=[anywhere] * 4,
        out_specs=(vmem, vmem),
        scratch_shapes=[
            pltpu.VMEM(phase_angles.shape, f32),
            pltpu.VMEM(mix_angles.shape, f32),
            whole,
            spread,
            pltpu.VMEM((nl, nb, per, lanes), f32),
            whole if per % 8 else pltpu.VMEM((1, 1, 8, 128), f32),
            state,
            spread,
            state,
            state,
            state,
            level,
            level,
            pltpu.VMEM((2, depth, rows // halves, lanes), f32),
            pltpu.VMEM((depth, nb, piece, lanes), f32),
            pltpu.VMEM((nb, depth, piece, lanes), f32),
            pltpu.SemaphoreType.DMA((4,)),
            pltpu.SemaphoreType.DMA((2 * halves + 3,)),
            pltpu.SemaphoreType.DMA((2 * halves + 3,)),
            pltpu.SemaphoreType.REGULAR,
            pltpu.SemaphoreType.REGULAR,
            pltpu.SemaphoreType.REGULAR,
        ],
        compiler_params=pltpu.CompilerParams(collective_id=0, has_side_effects=True),
    )(amplitudes, energies.reshape(nb, nl, per, lanes), phase_angles, mix_angles)


def solution(mesh):
    placed = (P(None, ("bank", "lane"), None, None), P(("bank", "lane"), None, None), P(), P())
    return jax.shard_map(
        functools.partial(on_device, mesh.shape["bank"], mesh.shape["lane"]),
        mesh=mesh,
        in_specs=placed,
        out_specs=(P(None, ("bank", "lane"), None, None), P("lane", "bank", None)),
        check_vma=False,
    )
```

```python
import functools

import jax
import jax.numpy as jnp
from jax import lax
from jax.experimental import pallas as pl
from jax.experimental.pallas import tpu as pltpu
from jax.sharding import PartitionSpec as P

MESH = pl.DeviceIdType.MESH
SIN = (1.0, -1 / 6, 1 / 120, -1 / 5040, 1 / 362880, -1 / 39916800, 1 / 6227020800, -1 / 1307674368000)
COS = (1.0, -1 / 2, 1 / 24, -1 / 720, 1 / 40320, -1 / 3628800, 1 / 479001600, -1 / 87178291200, 1 / 20922789888000)


def series(square, terms):
    total = jnp.full_like(square, terms[-1])
    for term in terms[-2::-1]:
        total = total * square + term
    return total


def sin_cos(turn):
    square = turn * turn
    return turn * series(square, SIN), series(square, COS)


def split(x):
    high = x.astype(jnp.bfloat16)
    return high, (x - high.astype(jnp.float32)).astype(jnp.bfloat16)


def dot3(a, b):
    def one(x, y):
        return lax.dot_general(x, y, (((1,), (0,)), ((), ())), preferred_element_type=jnp.float32)

    return one(a[0], b[0]) + (one(a[1], b[0]) + one(a[0], b[1]))


def turn_table(count, cosine, sine, places=None):
    places = count.bit_length() - 1 if places is None else places
    row = lax.broadcasted_iota(jnp.int32, (count, count), 0)
    col = lax.broadcasted_iota(jnp.int32, (count, count), 1)
    apart = row ^ col
    size = jnp.ones((count, count), jnp.float32)
    ones = jnp.zeros((count, count), jnp.int32)
    for place in range(places):
        bit = (apart >> place) & 1
        size = size * jnp.where(bit == 1, sine, cosine)
        ones = ones + bit
    size = jnp.where(apart >> places == 0, size, 0.0)
    phase = ones & 3
    real = jnp.where(phase == 0, size, jnp.where(phase == 2, -size, 0.0))
    imag = jnp.where(phase == 1, -size, jnp.where(phase == 3, size, 0.0))
    return real, imag


def butterfly(re, im, stride, cosine, sine):
    count, rest = re.shape[0], re.shape[1:]
    parts = (count // (2 * stride), 2, stride) + rest
    re, im = re.reshape(parts), im.reshape(parts)
    ur, vr, ui, vi = re[:, 0], re[:, 1], im[:, 0], im[:, 1]
    new_re = jnp.stack([cosine * ur + sine * vi, cosine * vr + sine * ui], axis=1)
    new_im = jnp.stack([cosine * ui - sine * vr, cosine * vi - sine * ur], axis=1)
    return new_re.reshape((count,) + rest), new_im.reshape((count,) + rest)


def kernel(
    nb, nl, halves, amp_hbm, en_hbm, ph_hbm, mix_hbm, out, marg,
    ph, mix, amp, en, e_l, tmp, s_a, e_b, b_b, o_b, r_a, cs_b, sn_b, part_done, ch, m_in, load, send, recv, line_in, lines_in, all_in,
):
    n = nb * nl
    depth, rows, lanes = amp.shape[1:]
    per = en.shape[2]
    step = per // halves
    tiled = per % 8 == 0
    units = rows // per
    piece = rows // nb
    last = 2 * halves + 2
    hub = nl // 2 - 1
    bank, lane = lax.axis_index("bank"), lax.axis_index("lane")
    me = bank * nl + lane

    load_en = pltpu.make_async_copy(en_hbm, en, load.at[0])
    load_amp = pltpu.make_async_copy(amp_hbm, amp, load.at[1])
    load_ph = pltpu.make_async_copy(ph_hbm, ph, load.at[2])
    load_mix = pltpu.make_async_copy(mix_hbm, mix, load.at[3])
    barrier = pltpu.get_barrier_semaphore()

    def partner(k):
        return lax.rem(bank + nb - lax.rem(k, nb), nb), lax.rem(lane + k // nb, nl)

    def greet_line(k, carry):
        to = lax.rem(lane + k, nl)

        @pl.when(to != hub)
        def _():
            pl.semaphore_signal(barrier, 1, device_id=(bank, to), device_id_type=MESH)

        return carry

    def signal_hubs(sem):
        def one(k, carry):
            pl.semaphore_signal(sem, 1, device_id=(lax.rem(bank + k, nb), hub), device_id_type=MESH)
            return carry

        lax.fori_loop(1, nb, one, 0)

    @pl.when(lane == hub)
    def _():
        signal_hubs(barrier)

    lax.fori_loop(1, nl, greet_line, 0)
    load_en.start()
    load_mix.start()
    load_amp.start()
    load_ph.start()

    def exchange(src, dst, which):
        def one(k, carry):
            to_bank, to_lane = partner(k)
            pltpu.make_async_remote_copy(
                src_ref=src.at[to_bank * nl + to_lane],
                dst_ref=dst.at[me],
                send_sem=send.at[which],
                recv_sem=recv.at[which],
                device_id=(to_bank, to_lane),
                device_id_type=MESH,
            ).start()
            return carry

        lax.fori_loop(1, n, one, 0)
        dst[me] = src[me]

    def arrived(dst, count, sems, which):
        most = dst.at[pl.ds(0, count - 1)]
        pltpu.make_async_copy(most, most, sems.at[which]).wait()

    load_en.wait()
    pl.semaphore_wait(barrier, jnp.where(lane == hub, nb - 1, nl - 1))

    @pl.when(lane == hub + 1)
    def _():
        pl.semaphore_signal(line_in, 1, device_id=(bank, hub), device_id_type=MESH)

    @pl.when(lane == hub)
    def _():
        pl.semaphore_wait(line_in, 1)
        signal_hubs(lines_in)

    def along_line(k, carry):
        to = lax.rem(lane + k, nl)
        pltpu.make_async_remote_copy(
            src_ref=en.at[:, to],
            dst_ref=e_l.at[lane],
            send_sem=send.at[0],
            recv_sem=recv.at[0],
            device_id=(bank, to),
            device_id_type=MESH,
        ).start()
        return carry

    lax.fori_loop(1, nl, along_line, 0)
    e_l[lane] = en[:, lane]
    load_mix.wait()
    cosines, sines = jnp.cos(mix[...]), jnp.sin(mix[...])

    def angle(layer, group):
        return cosines[layer : layer + 1, group : group + 1], sines[layer : layer + 1, group : group + 1]

    def tables(layer, count):
        real, imag = turn_table(lanes, *angle(layer, 0))
        by_lane = split(jnp.concatenate([jnp.concatenate([real, imag], 1), jnp.concatenate([-imag, real], 1)], 0))
        real, imag = turn_table(count, *angle(layer, 1))
        by_row = split(jnp.concatenate([jnp.concatenate([real, -imag], 1), jnp.concatenate([imag, real], 1)], 0))
        return by_lane, by_row

    def local_mix(layer, by_lane, by_row, count, read, write):
        pairs = [read(d) for d in range(depth)]
        stride = 1
        cosine, sine = (jnp.broadcast_to(x, (8, lanes))[None] for x in angle(layer, 2))
        re = jnp.stack([p[0] for p in pairs]).reshape(depth, count // 8, 8, lanes)
        im = jnp.stack([p[1] for p in pairs]).reshape(depth, count // 8, 8, lanes)
        while stride < depth:
            re, im = butterfly(re, im, stride, cosine, sine)
            stride *= 2
        re, im = re.reshape(depth, count, lanes), im.reshape(depth, count, lanes)
        for d in range(depth):
            both = dot3(split(jnp.concatenate([re[d], im[d]], 1)), by_lane)
            both = dot3(by_row, split(jnp.concatenate([both[:, :lanes], both[:, lanes:]], 0)))
            write(d, both[:count], both[count:])

    first_tables = tables(0, rows)
    second_tables = tables(1, rows // halves)

    load_amp.wait()
    load_ph.wait()

    def first(d):
        if tiled:
            e = en[pl.ds(d * units // nl, units // nl)].reshape(rows, lanes)
        else:
            e = tmp[0, d]
        sine, cosine = sin_cos(ph[0:1] * e)
        return amp[0, d] * cosine + amp[1, d] * sine, amp[1, d] * cosine - amp[0, d] * sine

    def to_units(d, re, im):
        if tiled:
            for part, x in enumerate((re, im)):
                x = x.reshape(units, halves, step, lanes)
                for h in range(halves):
                    s_a[h, pl.ds(d * units, units), part] = x[:, h]
        else:
            tmp[0, d] = re
            tmp[1, d] = im

    if not tiled:
        for d in range(depth):

            def spread(u, carry):
                tmp[0, d, pl.ds(u * per, per)] = en[(d * units + u) // nl, lax.rem(d * units + u, nl)]
                return carry

            lax.fori_loop(0, units, spread, 0)
    local_mix(0, *first_tables, rows, first, to_units)
    if not tiled:
        for d in range(depth):

            def gather(u, carry):
                for part in range(2):
                    s_a[0, d * units + u, part] = tmp[part, d, pl.ds(u * per, per)]
                return carry

            lax.fori_loop(0, units, gather, 0)

    @pl.when(lane == hub)
    def _():
        pl.semaphore_wait(lines_in, nb - 1)

        def tell(k, carry):
            pl.semaphore_signal(all_in, 1, device_id=(bank, lax.rem(lane + k, nl)), device_id_type=MESH)
            return carry

        lax.fori_loop(1, nl, tell, 0)

    @pl.when(lane != hub)
    def _():
        pl.semaphore_wait(all_in, 1)

    exchange(s_a.at[0], b_b.at[0], 1)
    arrived(e_l, nl, recv, 0)

    def across(k, carry):
        to = lax.rem(bank + k, nb)
        pltpu.make_async_remote_copy(
            src_ref=e_l.at[:, to],
            dst_ref=e_b.at[bank],
            send_sem=send.at[last - 1],
            recv_sem=recv.at[last - 1],
            device_id=(to, lane),
            device_id_type=MESH,
        ).start()
        return carry

    lax.fori_loop(1, nb, across, 0)
    e_b[bank] = e_l[:, bank]
    for h in range(1, halves):
        exchange(s_a.at[h], b_b.at[h], 1 + h)
    arrived(e_b, nb, recv, last - 1)
    sine, cosine = sin_cos(ph[1:2][None] * e_b[...].reshape(n, per, lanes))
    sn_b[...] = sine
    cs_b[...] = cosine

    for h in range(halves):
        arrived(b_b.at[h], n, recv, 1 + h)
        span = pl.ds(h * step, step)
        re, im = b_b[h, :, 0], b_b[h, :, 1]
        for layer in range(2):
            stride = 1
            while stride < n:
                cosine, sine = (
                    jnp.broadcast_to(x, (step, lanes))[None, None] for x in angle(layer, 3 if stride < nl else 2)
                )
                re, im = butterfly(re, im, stride, cosine, sine)
                stride *= 2
            if layer == 0:
                cosine, sine = cs_b[:, span], sn_b[:, span]
                re, im = re * cosine + im * sine, im * cosine - re * sine
        o_b[h, :, 0] = re
        o_b[h, :, 1] = im
        exchange(o_b.at[h], r_a.at[h], 1 + halves + h)

    def second(h, d):
        if tiled:
            return tuple(
                r_a[h, pl.ds(d * units, units), part].reshape(rows // halves, lanes) for part in range(2)
            )
        return tmp[0, d], tmp[1, d]

    def keep(d, re, im):
        part_done[0, d] = re
        part_done[1, d] = im

    def pass_on(d):
        def one(k, carry):
            to_bank = lax.rem(bank + k, nb)
            pltpu.make_async_remote_copy(
                src_ref=ch.at[d, to_bank],
                dst_ref=m_in.at[bank, d],
                send_sem=send.at[last],
                recv_sem=recv.at[last],
                device_id=(to_bank, lane),
                device_id_type=MESH,
            ).start()
            return carry

        lax.fori_loop(1, nb, one, 0)
        m_in[bank, d] = ch[d, bank]

    def finish(d, re, im):
        if halves == 2:
            cosine, sine = angle(1, 1)
            ur, ui, vr, vi = part_done[0, d], part_done[1, d], re, im
            shape = (units, 1, step, lanes)
            re = [cosine * ur + sine * vi, cosine * vr + sine * ui]
            im = [cosine * ui - sine * vr, cosine * vi - sine * ur]
            re = jnp.concatenate([x.reshape(shape) for x in re], 1).reshape(rows, lanes)
            im = jnp.concatenate([x.reshape(shape) for x in im], 1).reshape(rows, lanes)
        chance = re * re + im * im
        for g in range(nb):
            ch[d, g] = chance[g * piece : (g + 1) * piece]
        out[0, d] = re
        out[1, d] = im
        pass_on(d)

    for h in range(halves):
        arrived(r_a.at[h], n, recv, 1 + halves + h)
        if not tiled:
            for d in range(depth):

                def place(u, carry):
                    for part in range(2):
                        tmp[part, d, pl.ds(u * per, per)] = r_a[h, d * units + u, part]
                    return carry

                lax.fori_loop(0, units, place, 0)
        write = finish if h == halves - 1 else keep
        local_mix(1, *second_tables, rows // halves, functools.partial(second, h), write)

    arrived(m_in, nb, recv, last)
    total = m_in[0]
    for g in range(1, nb):
        total = total + m_in[g]
    marg[...] = total * (1.0 / nb)
    arrived(e_l, nl, send, 0)
    arrived(e_b, nb, send, last - 1)
    for h in range(halves):
        arrived(b_b.at[h], n, send, 1 + h)
        arrived(r_a.at[h], n, send, 1 + halves + h)
    arrived(m_in, nb, send, last)


def contact(nb, nl, bank, lane, line_in, last_in, lines_in, all_in):
    barrier = pltpu.get_barrier_semaphore()
    last = nl - 1
    is_hub, is_last = lane == 0, lane == last
    between = jnp.logical_not(jnp.logical_or(is_hub, is_last))

    def signal(sem, to_bank, to_lane):
        pl.semaphore_signal(sem, 1, device_id=(to_bank, to_lane), device_id_type=MESH)

    def signal_hubs(sem):
        def one(k, carry):
            signal(sem, lax.rem(bank + k, nb), 0)
            return carry

        lax.fori_loop(1, nb, one, 0)

    def greet():
        @pl.when(is_last)
        def _():
            signal(barrier, bank, 0)

        @pl.when(jnp.logical_not(is_last))
        def _():
            for to in range(last, 0, -1):

                @pl.when(lane != to)
                def _():
                    signal(barrier, bank, to)

        @pl.when(is_hub)
        def _():
            signal_hubs(barrier)

    def line():
        pl.semaphore_wait(barrier, jnp.where(is_hub, nb, jnp.where(is_last, last, last - 1)))

        @pl.when(lane == 1)
        def _():
            signal(line_in, bank, 0)

        @pl.when(is_hub)
        def _():
            pl.semaphore_wait(line_in, 1)
            for to in range(1, last):
                signal(last_in, bank, to)
            signal_hubs(lines_in)

    def all_of_line():
        @pl.when(between)
        def _():
            pl.semaphore_wait(last_in, 1)

    def everyone():
        @pl.when(is_hub)
        def _():
            pl.semaphore_wait(lines_in, nb - 1)
            for to in range(last, 0, -1):
                signal(all_in, bank, to)

        @pl.when(jnp.logical_not(is_hub))
        def _():
            pl.semaphore_wait(all_in, 1)

    def known(to):
        return jnp.logical_not(jnp.logical_and(between, to == last))

    return greet, line, all_of_line, everyone, known


def pieces(
    nb, nl, amp_hbm, en_hbm, ph_hbm, mix_hbm, out, marg,
    ph, mix, turns, amp, en, e_l, s_a, e_b, b_b, o_a, o_b, r_a, r_b, cs_b, sn_b, part, ch, near, pair, m_in,
    load, send, recv, *met,
):
    n = nb * nl
    depth, rows, lanes = amp.shape[1:]
    step = s_a.shape[3]
    half = step // 2
    units = rows // (2 * step)
    bank, lane = lax.axis_index("bank"), lax.axis_index("lane")
    me = bank * nl + lane
    side, pairs_at = lax.rem(bank, 2), bank // 2
    greet, line, all_of_line, everyone, known = contact(nb, nl, bank, lane, *met)
    loads = [
        pltpu.make_async_copy(x, y, load.at[i])
        for i, (x, y) in enumerate([(en_hbm, en), (mix_hbm, mix), (amp_hbm, amp), (ph_hbm, ph)])
    ]
    greet()
    for copy in loads:
        copy.start()

    def remote(src, dst, which, to):
        pltpu.make_async_remote_copy(
            src_ref=src,
            dst_ref=dst,
            send_sem=send.at[which],
            recv_sem=recv.at[which],
            device_id=to,
            device_id_type=MESH,
        ).start()

    def send_lane(to_lane, src, dst, which):
        def one(k, carry):
            to_bank = lax.rem(bank + k, nb)

            @pl.when(to_bank * nl + to_lane != me)
            def _():
                remote(src.at[to_bank * nl + to_lane], dst.at[me], which, (to_bank, to_lane))

            return carry

        lax.fori_loop(0, nb, one, 0)

    def now(to):
        return jnp.logical_or(lane != 2, to != 1)

    other = jnp.where(lane < nl // 2, nl // 2, 0)
    early = jnp.where(lane == 1, 0, 1)
    role = {"g": other + 1 - early, "h": other + early, "a": other, "b": other + 1, "t": lane ^ 1, "p": lane}

    def exchange(src, dst, which, order):
        for to in order:
            send_lane(role.get(to, to), src, dst, which)
        dst[me] = src[me]

    def along_line(k, start):
        to = lane ^ (nl - k)
        copy = pltpu.make_async_remote_copy(
            src_ref=en_hbm.at[:, to],
            dst_ref=e_l.at[lane if start else to],
            send_sem=send.at[8 + k],
            recv_sem=recv.at[8 + k],
            device_id=(bank, to),
            device_id_type=MESH,
        )
        if start:
            copy.start()
            return None
        copy.wait_recv()
        return to

    def across(pick, dst, which):
        def one(to, carry):
            @pl.when(to != bank)
            def _():
                remote(pick(to), dst.at[bank], which, (to, lane))

            return carry

        lax.fori_loop(0, nb, one, 0)

    def arrived(dst, count, sems, which):
        most = dst.at[pl.ds(0, count - 1)]
        pltpu.make_async_copy(most, most, sems.at[which]).wait()

    def angle(layer, group):
        return tuple(turns[i, layer : layer + 1, group : group + 1] for i in range(2))

    def mixed(layer, re, im, stride, stop, group):
        cosine, sine = (jnp.broadcast_to(x, re.shape[1:])[None, None] for x in angle(layer, group))
        while stride < stop:
            re, im = butterfly(re, im, stride, cosine, sine)
            stride *= 2
        return re, im

    def lane_table(layer):
        real, imag = turn_table(lanes, *angle(layer, 0))
        return split(jnp.concatenate([jnp.concatenate([real, imag], 1), jnp.concatenate([-imag, real], 1)], 0))

    def row_table(layer, count, places=None):
        real, imag = turn_table(count, *angle(layer, 1), places)
        return split(jnp.concatenate([jnp.concatenate([real, -imag], 1), jnp.concatenate([imag, real], 1)], 0))

    def prepare():
        loads[0].wait()
        loads[1].wait()
        turns[0] = jnp.cos(mix[...])
        turns[1] = jnp.sin(mix[...])
        lane_first, row_first = lane_table(0), row_table(0, rows)
        loads[2].wait()
        loads[3].wait()

        pairs = []
        for d in range(depth):
            e = en[pl.ds(d * units // nl, units // nl)].reshape(rows, lanes)
            sine, cosine = sin_cos(ph[0:1] * e)
            pairs.append((amp[0, d] * cosine + amp[1, d] * sine, amp[1, d] * cosine - amp[0, d] * sine))
        re = jnp.stack([p[0] for p in pairs]).reshape(depth, rows // 8, 8, lanes)
        im = jnp.stack([p[1] for p in pairs]).reshape(depth, rows // 8, 8, lanes)
        cosine, sine = (jnp.broadcast_to(x, (8, lanes))[None] for x in angle(0, 2))
        stride = 1
        while stride < depth:
            re, im = butterfly(re, im, stride, cosine, sine)
            stride *= 2
        re, im = re.reshape(depth, rows, lanes), im.reshape(depth, rows, lanes)
        for d in range(depth):
            both = dot3(split(jnp.concatenate([re[d], im[d]], 1)), lane_first)
            both = dot3(row_first, split(jnp.concatenate([both[:, :lanes], both[:, lanes:]], 0)))
            for i in range(2):
                x = both[i * rows : (i + 1) * rows].reshape(units, 2, step, lanes)
                for h in range(2):
                    s_a[h, pl.ds(d * units, units), i] = x[:, h]

    pl.when(lane == 0)(prepare)
    line()
    for k in range(1, nl):
        pl.when(known(lane ^ (nl - k)))(functools.partial(along_line, k, True))
    pl.when(lane != 0)(prepare)
    all_of_line()
    for k in range(1, nl):
        pl.when(jnp.logical_not(known(lane ^ (nl - k))))(functools.partial(along_line, k, True))
    everyone()
    across(lambda to: en.at[to, lane], e_b.at[:, lane], 1)
    e_b[bank, lane] = en[bank, lane]
    exchange(s_a.at[0], b_b.at[0], 2, (1, 2, 0, 3))
    lane_second, row_second = lane_table(1), row_table(1, lanes, step.bit_length() - 1)
    for k in range(1, nl):
        source = along_line(k, False)
        across(lambda to: e_l.at[source, to], e_b.at[:, source], 1)
        e_b[bank, source] = e_l[source, bank]
    exchange(s_a.at[1], b_b.at[1], 3, (1, 2, 0, 3))
    arrived(e_b, nb, recv, 1)
    sine, cosine = sin_cos(ph[1:2][None] * e_b[...].reshape(n, 2 * step, lanes))
    sn_b[...] = sine
    cs_b[...] = cosine

    for h in range(2):
        arrived(b_b.at[h], n, recv, 2 + h)
        span = pl.ds(h * step, step)
        re, im = b_b[h, :, 0], b_b[h, :, 1]
        re, im = mixed(0, re, im, 1, nl, 3)
        re, im = mixed(0, re, im, nl, n, 2)
        cosine, sine = cs_b[:, span], sn_b[:, span]
        re, im = re * cosine + im * sine, im * cosine - re * sine
        re, im = mixed(1, re, im, 1, nl, 3)
        re, im = mixed(1, re, im, nl, n, 2)
        re, im = re.reshape(n * step, lanes), im.reshape(n * step, lanes)
        both = dot3(split(jnp.concatenate([re, im], 1)), lane_second)
        groups = range(0, n * step, lanes)
        wide = [jnp.concatenate([both[g : g + lanes, i * lanes : (i + 1) * lanes] for g in groups], 1) for i in range(2)]
        both = dot3(row_second, split(jnp.concatenate(wide, 0)))
        for i in range(2):
            x = [both[i * lanes : (i + 1) * lanes, g : g + lanes] for g in groups]
            x = jnp.concatenate(x, 0).reshape(n, step, lanes)
            if h == 0:
                o_a[:, i] = x
            else:
                for s in range(2):
                    o_b[s, :, i] = x[:, s * half : (s + 1) * half]
        if h == 0:
            for to in [role.get(x, x) for x in 'abtp']:
                pl.when(now(to))(functools.partial(send_lane, to, o_a, r_a, 4))
            r_a[me] = o_a[me]
        else:
            for to, s in [(role.get(x, x), s) for x, s in [('a', 0), ('p', 0), ('g', early), ('b', -1), ('p', 1), ('h', 1 - early), ('t', 0), ('b', 1), ('t', 1)]]:
                if isinstance(s, int) and s < 0:
                    pl.when(jnp.logical_not(now(to)))(functools.partial(send_lane, to, o_a, r_a, 4))
                else:
                    send_lane(to, o_b.at[s], r_b.at[s], 5 + s)
            for s in range(2):
                r_b[s, me] = o_b[s, me]

    arrived(r_a, n, recv, 4)
    re, im = mixed(1, r_a[:, 0], r_a[:, 1], 1, units, 1)
    re, im = mixed(1, re, im, units, n, 2)
    for s in range(2):
        part[s, 0] = re[:, s * half : (s + 1) * half]
        part[s, 1] = im[:, s * half : (s + 1) * half]

    for s in range(2):
        arrived(r_b.at[s], n, recv, 5 + s)
        vr, vi = mixed(1, r_b[s, :, 0], r_b[s, :, 1], 1, units, 1)
        vr, vi = mixed(1, vr, vi, units, n, 2)
        ur, ui = part[s, 0], part[s, 1]
        cosine, sine = (jnp.broadcast_to(x, (half, lanes))[None] for x in angle(1, 1))
        re = (cosine * ur + sine * vi, cosine * vr + sine * ui)
        im = (cosine * ui - sine * vr, cosine * vi - sine * ur)
        for h in range(2):
            chance = re[h] * re[h] + im[h] * im[h]
            for d in range(depth):
                ch[s, :, :, d, h] = chance[d * units : (d + 1) * units].reshape(nb // 2, 2, half, lanes)
        remote(ch.at[s, :, 1 - side], near.at[s], 8 + nl * s, (bank ^ 1, lane))
        for h in range(2):
            for i, x in enumerate((re[h], im[h])):
                out[i, :, :, h, s * half : (s + 1) * half] = x.reshape(depth, units, half, lanes)

    for s in range(2):
        pltpu.make_async_copy(near.at[s], near.at[s], recv.at[8 + nl * s]).wait()
        pair[s] = ch[s, :, side] + near[s]

        for apart in range(nb // 2 - 1, 0, -1):
            to = pairs_at ^ apart
            remote(pair.at[s, to], m_in.at[s, pairs_at], 7 * s, (2 * to + side, lane))
        m_in[s, pairs_at] = pair[s, pairs_at]
    for s in range(2):
        arrived(m_in.at[s], nb // 2, recv, 7 * s)
        total = m_in[s, 0]
        for g in range(1, nb // 2):
            total = total + m_in[s, g]
        marg[:, :, s * half : (s + 1) * half] = total * (1.0 / nb)
    for k in range(1, nl):
        pltpu.make_async_copy(en.at[:, 0], e_l.at[0], send.at[8 + k]).wait()
    arrived(e_b, nb, send, 1)
    for h in range(2):
        arrived(b_b.at[h], n, send, 2 + h)
        arrived(r_b.at[h], n, send, 5 + h)
        arrived(m_in.at[h], nb // 2, send, 7 * h)
        pltpu.make_async_copy(near.at[h], near.at[h], send.at[8 + nl * h]).wait()
    arrived(r_a, n, send, 4)


def keep(a, b, a_hbm, b_hbm, sems):
    copies = [pltpu.make_async_copy(a, a_hbm, sems.at[0]), pltpu.make_async_copy(b, b_hbm, sems.at[1])]
    for copy in copies:
        copy.start()
    for copy in copies:
        copy.wait()


def in_pieces(nb, nl, amplitudes, energies, phase_angles, mix_angles):
    _, depth, rows, lanes = amplitudes.shape
    n = nb * nl
    per = depth * rows // n
    step, half = per // 2, per // 4
    f32 = jnp.float32
    vmem = pl.BlockSpec(memory_space=pltpu.VMEM)
    anywhere = pl.BlockSpec(memory_space=pl.ANY)
    state = pltpu.VMEM((2, n, 2, step, lanes), f32)
    level = pltpu.VMEM((n, per, lanes), f32)
    spread = pltpu.VMEM((nb, nl, per, lanes), f32)
    shapes = (2, depth, nb, 2, step, lanes), (depth, 2, step, lanes)
    results = pl.pallas_call(
        functools.partial(pieces, nb, nl),
        name="register",
        out_shape=tuple(pltpu.VMEM(shape, f32) for shape in shapes),
        in_specs=[anywhere] * 4,
        out_specs=(vmem, vmem),
        scratch_shapes=[
            pltpu.VMEM(phase_angles.shape, f32),
            pltpu.VMEM(mix_angles.shape, f32),
            pltpu.VMEM((2, *mix_angles.shape), f32),
            pltpu.VMEM((2, depth, rows, lanes), f32),
            spread,
            pltpu.VMEM((nl, nb, per, lanes), f32),
            state,
            spread,
            state,
            pltpu.VMEM((n, 2, step, lanes), f32),
            pltpu.VMEM((2, n, 2, half, lanes), f32),
            pltpu.VMEM((n, 2, step, lanes), f32),
            pltpu.VMEM((2, n, 2, half, lanes), f32),
            level,
            level,
            pltpu.VMEM((2, 2, n, half, lanes), f32),
            pltpu.VMEM((2, nb // 2, 2, depth, 2, half, lanes), f32),
            pltpu.VMEM((2, nb // 2, depth, 2, half, lanes), f32),
            pltpu.VMEM((2, nb // 2, depth, 2, half, lanes), f32),
            pltpu.VMEM((2, nb // 2, depth, 2, half, lanes), f32),
            pltpu.SemaphoreType.DMA((4,)),
            pltpu.SemaphoreType.DMA((9 + nl,)),
            pltpu.SemaphoreType.DMA((9 + nl,)),
            *[pltpu.SemaphoreType.REGULAR] * 4,
        ],
        compiler_params=pltpu.CompilerParams(collective_id=0, has_side_effects=True),
    )(amplitudes, energies.reshape(nb, nl, per, lanes), phase_angles, mix_angles)
    final, marginal = pl.pallas_call(
        keep,
        name="keep",
        out_shape=tuple(jax.ShapeDtypeStruct(shape, f32) for shape in shapes),
        in_specs=[vmem, vmem],
        out_specs=(anywhere, anywhere),
        scratch_shapes=[pltpu.SemaphoreType.DMA((2,))],
    )(*[pltpu.with_memory_space_constraint(x, pltpu.VMEM) for x in results])
    return final.reshape(amplitudes.shape), marginal.reshape(depth, rows // nb, lanes)


def on_device(nb, nl, amplitudes, energies, phase_angles, mix_angles):
    _, depth, rows, lanes = amplitudes.shape
    n = nb * nl
    per = depth * rows // n
    halves = 2 if per % 16 == 0 else 1
    piece = rows // nb
    if per == 2 * 8 and piece == per and rows // per % nl == 0 and n * 8 % lanes == 0:
        return in_pieces(nb, nl, amplitudes, energies, phase_angles, mix_angles)
    f32 = jnp.float32
    state = pltpu.VMEM((halves, n, 2, per // halves, lanes), f32)
    level = pltpu.VMEM((n, per, lanes), f32)
    spread = pltpu.VMEM((nb, nl, per, lanes), f32)
    vmem = pl.BlockSpec(memory_space=pltpu.VMEM)
    anywhere = pl.BlockSpec(memory_space=pl.ANY)
    whole = pltpu.VMEM((2, depth, rows, lanes), f32)
    return pl.pallas_call(
        functools.partial(kernel, nb, nl, halves),
        name="register",
        out_shape=(pltpu.VMEM(amplitudes.shape, f32), pltpu.VMEM((depth, piece, lanes), f32)),
        in_specs=[anywhere] * 4,
        out_specs=(vmem, vmem),
        scratch_shapes=[
            pltpu.VMEM(phase_angles.shape, f32),
            pltpu.VMEM(mix_angles.shape, f32),
            whole,
            spread,
            pltpu.VMEM((nl, nb, per, lanes), f32),
            whole if per % 8 else pltpu.VMEM((1, 1, 8, 128), f32),
            state,
            spread,
            state,
            state,
            state,
            level,
            level,
            pltpu.VMEM((2, depth, rows // halves, lanes), f32),
            pltpu.VMEM((depth, nb, piece, lanes), f32),
            pltpu.VMEM((nb, depth, piece, lanes), f32),
            pltpu.SemaphoreType.DMA((4,)),
            pltpu.SemaphoreType.DMA((2 * halves + 3,)),
            pltpu.SemaphoreType.DMA((2 * halves + 3,)),
            pltpu.SemaphoreType.REGULAR,
            pltpu.SemaphoreType.REGULAR,
            pltpu.SemaphoreType.REGULAR,
        ],
        compiler_params=pltpu.CompilerParams(collective_id=0, has_side_effects=True),
    )(amplitudes, energies.reshape(nb, nl, per, lanes), phase_angles, mix_angles)


def solution(mesh):
    placed = (P(None, ("bank", "lane"), None, None), P(("bank", "lane"), None, None), P(), P())
    return jax.shard_map(
        functools.partial(on_device, mesh.shape["bank"], mesh.shape["lane"]),
        mesh=mesh,
        in_specs=placed,
        out_specs=(P(None, ("bank", "lane"), None, None), P("lane", "bank", None)),
        check_vma=False,
    )
```

```python
import functools

import jax
import jax.numpy as jnp
from jax import lax
from jax.experimental import pallas as pl
from jax.experimental.pallas import tpu as pltpu
from jax.sharding import PartitionSpec as P

MESH = pl.DeviceIdType.MESH
SIN = (1.0, -1 / 6, 1 / 120, -1 / 5040, 1 / 362880, -1 / 39916800, 1 / 6227020800, -1 / 1307674368000)
COS = (1.0, -1 / 2, 1 / 24, -1 / 720, 1 / 40320, -1 / 3628800, 1 / 479001600, -1 / 87178291200, 1 / 20922789888000)


def series(square, terms):
    total = jnp.full_like(square, terms[-1])
    for term in terms[-2::-1]:
        total = total * square + term
    return total


def sin_cos(turn):
    square = turn * turn
    return turn * series(square, SIN), series(square, COS)


def split(x):
    high = x.astype(jnp.bfloat16)
    return high, (x - high.astype(jnp.float32)).astype(jnp.bfloat16)


def dot3(a, b):
    def one(x, y):
        return lax.dot_general(x, y, (((1,), (0,)), ((), ())), preferred_element_type=jnp.float32)

    return one(a[0], b[0]) + (one(a[1], b[0]) + one(a[0], b[1]))


def turn_table(count, cosine, sine, places=None):
    places = count.bit_length() - 1 if places is None else places
    row = lax.broadcasted_iota(jnp.int32, (count, count), 0)
    col = lax.broadcasted_iota(jnp.int32, (count, count), 1)
    apart = row ^ col
    size = jnp.ones((count, count), jnp.float32)
    ones = jnp.zeros((count, count), jnp.int32)
    for place in range(places):
        bit = (apart >> place) & 1
        size = size * jnp.where(bit == 1, sine, cosine)
        ones = ones + bit
    size = jnp.where(apart >> places == 0, size, 0.0)
    phase = ones & 3
    real = jnp.where(phase == 0, size, jnp.where(phase == 2, -size, 0.0))
    imag = jnp.where(phase == 1, -size, jnp.where(phase == 3, size, 0.0))
    return real, imag


def butterfly(re, im, stride, cosine, sine):
    count, rest = re.shape[0], re.shape[1:]
    parts = (count // (2 * stride), 2, stride) + rest
    re, im = re.reshape(parts), im.reshape(parts)
    ur, vr, ui, vi = re[:, 0], re[:, 1], im[:, 0], im[:, 1]
    new_re = jnp.stack([cosine * ur + sine * vi, cosine * vr + sine * ui], axis=1)
    new_im = jnp.stack([cosine * ui - sine * vr, cosine * vi - sine * ur], axis=1)
    return new_re.reshape((count,) + rest), new_im.reshape((count,) + rest)


def kernel(
    nb, nl, halves, amp_hbm, en_hbm, ph_hbm, mix_hbm, out, marg,
    ph, mix, amp, en, e_l, tmp, s_a, e_b, b_b, o_b, r_a, cs_b, sn_b, part_done, ch, m_in, load, send, recv, line_in, lines_in, all_in,
):
    n = nb * nl
    depth, rows, lanes = amp.shape[1:]
    per = en.shape[2]
    step = per // halves
    tiled = per % 8 == 0
    units = rows // per
    piece = rows // nb
    last = 2 * halves + 2
    hub = nl // 2 - 1
    bank, lane = lax.axis_index("bank"), lax.axis_index("lane")
    me = bank * nl + lane

    load_en = pltpu.make_async_copy(en_hbm, en, load.at[0])
    load_amp = pltpu.make_async_copy(amp_hbm, amp, load.at[1])
    load_ph = pltpu.make_async_copy(ph_hbm, ph, load.at[2])
    load_mix = pltpu.make_async_copy(mix_hbm, mix, load.at[3])
    barrier = pltpu.get_barrier_semaphore()

    def partner(k):
        return lax.rem(bank + nb - lax.rem(k, nb), nb), lax.rem(lane + k // nb, nl)

    def greet_line(k, carry):
        to = lax.rem(lane + k, nl)

        @pl.when(to != hub)
        def _():
            pl.semaphore_signal(barrier, 1, device_id=(bank, to), device_id_type=MESH)

        return carry

    def signal_hubs(sem):
        def one(k, carry):
            pl.semaphore_signal(sem, 1, device_id=(lax.rem(bank + k, nb), hub), device_id_type=MESH)
            return carry

        lax.fori_loop(1, nb, one, 0)

    @pl.when(lane == hub)
    def _():
        signal_hubs(barrier)

    lax.fori_loop(1, nl, greet_line, 0)
    load_en.start()
    load_mix.start()
    load_amp.start()
    load_ph.start()

    def exchange(src, dst, which):
        def one(k, carry):
            to_bank, to_lane = partner(k)
            pltpu.make_async_remote_copy(
                src_ref=src.at[to_bank * nl + to_lane],
                dst_ref=dst.at[me],
                send_sem=send.at[which],
                recv_sem=recv.at[which],
                device_id=(to_bank, to_lane),
                device_id_type=MESH,
            ).start()
            return carry

        lax.fori_loop(1, n, one, 0)
        dst[me] = src[me]

    def arrived(dst, count, sems, which):
        most = dst.at[pl.ds(0, count - 1)]
        pltpu.make_async_copy(most, most, sems.at[which]).wait()

    load_en.wait()
    pl.semaphore_wait(barrier, jnp.where(lane == hub, nb - 1, nl - 1))

    @pl.when(lane == hub + 1)
    def _():
        pl.semaphore_signal(line_in, 1, device_id=(bank, hub), device_id_type=MESH)

    @pl.when(lane == hub)
    def _():
        pl.semaphore_wait(line_in, 1)
        signal_hubs(lines_in)

    def along_line(k, carry):
        to = lax.rem(lane + k, nl)
        pltpu.make_async_remote_copy(
            src_ref=en.at[:, to],
            dst_ref=e_l.at[lane],
            send_sem=send.at[0],
            recv_sem=recv.at[0],
            device_id=(bank, to),
            device_id_type=MESH,
        ).start()
        return carry

    lax.fori_loop(1, nl, along_line, 0)
    e_l[lane] = en[:, lane]
    load_mix.wait()
    cosines, sines = jnp.cos(mix[...]), jnp.sin(mix[...])

    def angle(layer, group):
        return cosines[layer : layer + 1, group : group + 1], sines[layer : layer + 1, group : group + 1]

    def tables(layer, count):
        real, imag = turn_table(lanes, *angle(layer, 0))
        by_lane = split(jnp.concatenate([jnp.concatenate([real, imag], 1), jnp.concatenate([-imag, real], 1)], 0))
        real, imag = turn_table(count, *angle(layer, 1))
        by_row = split(jnp.concatenate([jnp.concatenate([real, -imag], 1), jnp.concatenate([imag, real], 1)], 0))
        return by_lane, by_row

    def local_mix(layer, by_lane, by_row, count, read, write):
        pairs = [read(d) for d in range(depth)]
        stride = 1
        cosine, sine = (jnp.broadcast_to(x, (8, lanes))[None] for x in angle(layer, 2))
        re = jnp.stack([p[0] for p in pairs]).reshape(depth, count // 8, 8, lanes)
        im = jnp.stack([p[1] for p in pairs]).reshape(depth, count // 8, 8, lanes)
        while stride < depth:
            re, im = butterfly(re, im, stride, cosine, sine)
            stride *= 2
        re, im = re.reshape(depth, count, lanes), im.reshape(depth, count, lanes)
        for d in range(depth):
            both = dot3(split(jnp.concatenate([re[d], im[d]], 1)), by_lane)
            both = dot3(by_row, split(jnp.concatenate([both[:, :lanes], both[:, lanes:]], 0)))
            write(d, both[:count], both[count:])

    first_tables = tables(0, rows)
    second_tables = tables(1, rows // halves)

    load_amp.wait()
    load_ph.wait()

    def first(d):
        if tiled:
            e = en[pl.ds(d * units // nl, units // nl)].reshape(rows, lanes)
        else:
            e = tmp[0, d]
        sine, cosine = sin_cos(ph[0:1] * e)
        return amp[0, d] * cosine + amp[1, d] * sine, amp[1, d] * cosine - amp[0, d] * sine

    def to_units(d, re, im):
        if tiled:
            for part, x in enumerate((re, im)):
                x = x.reshape(units, halves, step, lanes)
                for h in range(halves):
                    s_a[h, pl.ds(d * units, units), part] = x[:, h]
        else:
            tmp[0, d] = re
            tmp[1, d] = im

    if not tiled:
        for d in range(depth):

            def spread(u, carry):
                tmp[0, d, pl.ds(u * per, per)] = en[(d * units + u) // nl, lax.rem(d * units + u, nl)]
                return carry

            lax.fori_loop(0, units, spread, 0)
    local_mix(0, *first_tables, rows, first, to_units)
    if not tiled:
        for d in range(depth):

            def gather(u, carry):
                for part in range(2):
                    s_a[0, d * units + u, part] = tmp[part, d, pl.ds(u * per, per)]
                return carry

            lax.fori_loop(0, units, gather, 0)

    @pl.when(lane == hub)
    def _():
        pl.semaphore_wait(lines_in, nb - 1)

        def tell(k, carry):
            pl.semaphore_signal(all_in, 1, device_id=(bank, lax.rem(lane + k, nl)), device_id_type=MESH)
            return carry

        lax.fori_loop(1, nl, tell, 0)

    @pl.when(lane != hub)
    def _():
        pl.semaphore_wait(all_in, 1)

    exchange(s_a.at[0], b_b.at[0], 1)
    arrived(e_l, nl, recv, 0)

    def across(k, carry):
        to = lax.rem(bank + k, nb)
        pltpu.make_async_remote_copy(
            src_ref=e_l.at[:, to],
            dst_ref=e_b.at[bank],
            send_sem=send.at[last - 1],
            recv_sem=recv.at[last - 1],
            device_id=(to, lane),
            device_id_type=MESH,
        ).start()
        return carry

    lax.fori_loop(1, nb, across, 0)
    e_b[bank] = e_l[:, bank]
    for h in range(1, halves):
        exchange(s_a.at[h], b_b.at[h], 1 + h)
    arrived(e_b, nb, recv, last - 1)
    sine, cosine = sin_cos(ph[1:2][None] * e_b[...].reshape(n, per, lanes))
    sn_b[...] = sine
    cs_b[...] = cosine

    for h in range(halves):
        arrived(b_b.at[h], n, recv, 1 + h)
        span = pl.ds(h * step, step)
        re, im = b_b[h, :, 0], b_b[h, :, 1]
        for layer in range(2):
            stride = 1
            while stride < n:
                cosine, sine = (
                    jnp.broadcast_to(x, (step, lanes))[None, None] for x in angle(layer, 3 if stride < nl else 2)
                )
                re, im = butterfly(re, im, stride, cosine, sine)
                stride *= 2
            if layer == 0:
                cosine, sine = cs_b[:, span], sn_b[:, span]
                re, im = re * cosine + im * sine, im * cosine - re * sine
        o_b[h, :, 0] = re
        o_b[h, :, 1] = im
        exchange(o_b.at[h], r_a.at[h], 1 + halves + h)

    def second(h, d):
        if tiled:
            return tuple(
                r_a[h, pl.ds(d * units, units), part].reshape(rows // halves, lanes) for part in range(2)
            )
        return tmp[0, d], tmp[1, d]

    def keep(d, re, im):
        part_done[0, d] = re
        part_done[1, d] = im

    def pass_on(d):
        def one(k, carry):
            to_bank = lax.rem(bank + k, nb)
            pltpu.make_async_remote_copy(
                src_ref=ch.at[d, to_bank],
                dst_ref=m_in.at[bank, d],
                send_sem=send.at[last],
                recv_sem=recv.at[last],
                device_id=(to_bank, lane),
                device_id_type=MESH,
            ).start()
            return carry

        lax.fori_loop(1, nb, one, 0)
        m_in[bank, d] = ch[d, bank]

    def finish(d, re, im):
        if halves == 2:
            cosine, sine = angle(1, 1)
            ur, ui, vr, vi = part_done[0, d], part_done[1, d], re, im
            shape = (units, 1, step, lanes)
            re = [cosine * ur + sine * vi, cosine * vr + sine * ui]
            im = [cosine * ui - sine * vr, cosine * vi - sine * ur]
            re = jnp.concatenate([x.reshape(shape) for x in re], 1).reshape(rows, lanes)
            im = jnp.concatenate([x.reshape(shape) for x in im], 1).reshape(rows, lanes)
        chance = re * re + im * im
        for g in range(nb):
            ch[d, g] = chance[g * piece : (g + 1) * piece]
        out[0, d] = re
        out[1, d] = im
        pass_on(d)

    for h in range(halves):
        arrived(r_a.at[h], n, recv, 1 + halves + h)
        if not tiled:
            for d in range(depth):

                def place(u, carry):
                    for part in range(2):
                        tmp[part, d, pl.ds(u * per, per)] = r_a[h, d * units + u, part]
                    return carry

                lax.fori_loop(0, units, place, 0)
        write = finish if h == halves - 1 else keep
        local_mix(1, *second_tables, rows // halves, functools.partial(second, h), write)

    arrived(m_in, nb, recv, last)
    total = m_in[0]
    for g in range(1, nb):
        total = total + m_in[g]
    marg[...] = total * (1.0 / nb)
    arrived(e_l, nl, send, 0)
    arrived(e_b, nb, send, last - 1)
    for h in range(halves):
        arrived(b_b.at[h], n, send, 1 + h)
        arrived(r_a.at[h], n, send, 1 + halves + h)
    arrived(m_in, nb, send, last)


def contact(nb, nl, bank, lane, line_in, last_in, lines_in, all_in):
    barrier = pltpu.get_barrier_semaphore()
    last = nl - 1
    is_hub, is_last = lane == 0, lane == last
    between = jnp.logical_not(jnp.logical_or(is_hub, is_last))

    def signal(sem, to_bank, to_lane):
        pl.semaphore_signal(sem, 1, device_id=(to_bank, to_lane), device_id_type=MESH)

    def signal_hubs(sem):
        def one(k, carry):
            signal(sem, lax.rem(bank + k, nb), 0)
            return carry

        lax.fori_loop(1, nb, one, 0)

    def greet():
        @pl.when(is_last)
        def _():
            signal(barrier, bank, 0)

        @pl.when(jnp.logical_not(is_last))
        def _():
            for to in range(last, 0, -1):

                @pl.when(lane != to)
                def _():
                    signal(barrier, bank, to)

        @pl.when(is_hub)
        def _():
            signal_hubs(barrier)

    def line():
        pl.semaphore_wait(barrier, jnp.where(is_hub, nb, jnp.where(is_last, last, last - 1)))

        @pl.when(lane == 1)
        def _():
            signal(line_in, bank, 0)

        @pl.when(is_hub)
        def _():
            pl.semaphore_wait(line_in, 1)
            for to in range(1, last):
                signal(last_in, bank, to)
            signal_hubs(lines_in)

    def all_of_line():
        @pl.when(between)
        def _():
            pl.semaphore_wait(last_in, 1)

    def everyone():
        @pl.when(is_hub)
        def _():
            pl.semaphore_wait(lines_in, nb - 1)
            for to in range(last, 0, -1):
                signal(all_in, bank, to)

        @pl.when(jnp.logical_not(is_hub))
        def _():
            pl.semaphore_wait(all_in, 1)

    def known(to):
        return jnp.logical_not(jnp.logical_and(between, to == last))

    return greet, line, all_of_line, everyone, known


def pieces(
    nb, nl, amp_hbm, en_hbm, ph_hbm, mix_hbm, out, marg,
    ph, mix, turns, amp, en, e_l, s_a, e_b, b_b, o_a, o_b, r_a, r_b, cs_b, sn_b, part, ch, near, pair, m_in,
    load, send, recv, *met,
):
    n = nb * nl
    depth, rows, lanes = amp.shape[1:]
    step = s_a.shape[3]
    half = step // 2
    units = rows // (2 * step)
    bank, lane = lax.axis_index("bank"), lax.axis_index("lane")
    me = bank * nl + lane
    side, pairs_at = lax.rem(bank, 2), bank // 2
    greet, line, all_of_line, everyone, known = contact(nb, nl, bank, lane, *met)
    loads = [
        pltpu.make_async_copy(x, y, load.at[i])
        for i, (x, y) in enumerate([(en_hbm, en), (mix_hbm, mix), (amp_hbm, amp), (ph_hbm, ph)])
    ]
    greet()
    for copy in loads:
        copy.start()

    def remote(src, dst, which, to):
        pltpu.make_async_remote_copy(
            src_ref=src,
            dst_ref=dst,
            send_sem=send.at[which],
            recv_sem=recv.at[which],
            device_id=to,
            device_id_type=MESH,
        ).start()

    def send_lane(to_lane, src, dst, which):
        def one(k, carry):
            to_bank = lax.rem(bank + k, nb)

            @pl.when(to_bank * nl + to_lane != me)
            def _():
                remote(src.at[to_bank * nl + to_lane], dst.at[me], which, (to_bank, to_lane))

            return carry

        lax.fori_loop(0, nb, one, 0)

    def now(to):
        return jnp.logical_or(lane != 2, to != 1)

    other = jnp.where(lane < nl // 2, nl // 2, 0)
    role = {"a": other, "b": other + 1, "t": lane ^ 1, "p": lane}

    def exchange(src, dst, which, order):
        for to in order:
            send_lane(role.get(to, to), src, dst, which)
        dst[me] = src[me]

    def along_line(k, start):
        to = lane ^ (nl - k)
        copy = pltpu.make_async_remote_copy(
            src_ref=en_hbm.at[:, to],
            dst_ref=e_l.at[lane if start else to],
            send_sem=send.at[8 + k],
            recv_sem=recv.at[8 + k],
            device_id=(bank, to),
            device_id_type=MESH,
        )
        if start:
            copy.start()
            return None
        copy.wait_recv()
        return to

    def across(pick, dst, which):
        def one(to, carry):
            @pl.when(to != bank)
            def _():
                remote(pick(to), dst.at[bank], which, (to, lane))

            return carry

        lax.fori_loop(0, nb, one, 0)

    def arrived(dst, count, sems, which):
        most = dst.at[pl.ds(0, count - 1)]
        pltpu.make_async_copy(most, most, sems.at[which]).wait()

    def angle(layer, group):
        return tuple(turns[i, layer : layer + 1, group : group + 1] for i in range(2))

    def mixed(layer, re, im, stride, stop, group):
        cosine, sine = (jnp.broadcast_to(x, re.shape[1:])[None, None] for x in angle(layer, group))
        while stride < stop:
            re, im = butterfly(re, im, stride, cosine, sine)
            stride *= 2
        return re, im

    def lane_table(layer):
        real, imag = turn_table(lanes, *angle(layer, 0))
        return split(jnp.concatenate([jnp.concatenate([real, imag], 1), jnp.concatenate([-imag, real], 1)], 0))

    def row_table(layer, count, places=None):
        real, imag = turn_table(count, *angle(layer, 1), places)
        return split(jnp.concatenate([jnp.concatenate([real, -imag], 1), jnp.concatenate([imag, real], 1)], 0))

    def prepare():
        loads[0].wait()
        loads[1].wait()
        turns[0] = jnp.cos(mix[...])
        turns[1] = jnp.sin(mix[...])
        lane_first, row_first = lane_table(0), row_table(0, rows)
        loads[2].wait()
        loads[3].wait()

        pairs = []
        for d in range(depth):
            e = en[pl.ds(d * units // nl, units // nl)].reshape(rows, lanes)
            sine, cosine = sin_cos(ph[0:1] * e)
            pairs.append((amp[0, d] * cosine + amp[1, d] * sine, amp[1, d] * cosine - amp[0, d] * sine))
        re = jnp.stack([p[0] for p in pairs]).reshape(depth, rows // 8, 8, lanes)
        im = jnp.stack([p[1] for p in pairs]).reshape(depth, rows // 8, 8, lanes)
        cosine, sine = (jnp.broadcast_to(x, (8, lanes))[None] for x in angle(0, 2))
        stride = 1
        while stride < depth:
            re, im = butterfly(re, im, stride, cosine, sine)
            stride *= 2
        re, im = re.reshape(depth, rows, lanes), im.reshape(depth, rows, lanes)
        for d in range(depth):
            both = dot3(split(jnp.concatenate([re[d], im[d]], 1)), lane_first)
            both = dot3(row_first, split(jnp.concatenate([both[:, :lanes], both[:, lanes:]], 0)))
            for i in range(2):
                x = both[i * rows : (i + 1) * rows].reshape(units, 2, step, lanes)
                for h in range(2):
                    s_a[h, pl.ds(d * units, units), i] = x[:, h]

    pl.when(lane == 0)(prepare)
    line()
    for k in range(1, nl):
        pl.when(known(lane ^ (nl - k)))(functools.partial(along_line, k, True))
    pl.when(lane != 0)(prepare)
    all_of_line()
    for k in range(1, nl):
        pl.when(jnp.logical_not(known(lane ^ (nl - k))))(functools.partial(along_line, k, True))
    everyone()
    across(lambda to: en.at[to, lane], e_b.at[:, lane], 1)
    e_b[bank, lane] = en[bank, lane]
    exchange(s_a.at[0], b_b.at[0], 2, (1, 2, 3, 0))
    lane_second, row_second = lane_table(1), row_table(1, lanes, step.bit_length() - 1)
    for k in range(1, nl):
        source = along_line(k, False)
        across(lambda to: e_l.at[source, to], e_b.at[:, source], 1)
        e_b[bank, source] = e_l[source, bank]
    exchange(s_a.at[1], b_b.at[1], 3, (1, 2, 3, 0))
    arrived(e_b, nb, recv, 1)
    sine, cosine = sin_cos(ph[1:2][None] * e_b[...].reshape(n, 2 * step, lanes))
    sn_b[...] = sine
    cs_b[...] = cosine

    for h in range(2):
        arrived(b_b.at[h], n, recv, 2 + h)
        span = pl.ds(h * step, step)
        re, im = b_b[h, :, 0], b_b[h, :, 1]
        re, im = mixed(0, re, im, 1, nl, 3)
        re, im = mixed(0, re, im, nl, n, 2)
        cosine, sine = cs_b[:, span], sn_b[:, span]
        re, im = re * cosine + im * sine, im * cosine - re * sine
        re, im = mixed(1, re, im, 1, nl, 3)
        re, im = mixed(1, re, im, nl, n, 2)
        re, im = re.reshape(n * step, lanes), im.reshape(n * step, lanes)
        both = dot3(split(jnp.concatenate([re, im], 1)), lane_second)
        groups = range(0, n * step, lanes)
        wide = [jnp.concatenate([both[g : g + lanes, i * lanes : (i + 1) * lanes] for g in groups], 1) for i in range(2)]
        both = dot3(row_second, split(jnp.concatenate(wide, 0)))
        for i in range(2):
            x = [both[i * lanes : (i + 1) * lanes, g : g + lanes] for g in groups]
            x = jnp.concatenate(x, 0).reshape(n, step, lanes)
            if h == 0:
                o_a[:, i] = x
            else:
                for s in range(2):
                    o_b[s, :, i] = x[:, s * half : (s + 1) * half]
        if h == 0:
            for to in [role.get(x, x) for x in 'abtp']:
                pl.when(now(to))(functools.partial(send_lane, to, o_a, r_a, 4))
            r_a[me] = o_a[me]
        else:
            for to, s in [(role.get(x, x), s) for x, s in [('a', 0), ('p', 0), ('a', 1), ('b', -1), ('p', 1), ('b', 0), ('t', 0), ('b', 1), ('t', 1)]]:
                if s < 0:
                    pl.when(jnp.logical_not(now(to)))(functools.partial(send_lane, to, o_a, r_a, 4))
                else:
                    send_lane(to, o_b.at[s], r_b.at[s], 5 + s)
            for s in range(2):
                r_b[s, me] = o_b[s, me]

    arrived(r_a, n, recv, 4)
    re, im = mixed(1, r_a[:, 0], r_a[:, 1], 1, units, 1)
    re, im = mixed(1, re, im, units, n, 2)
    for s in range(2):
        part[s, 0] = re[:, s * half : (s + 1) * half]
        part[s, 1] = im[:, s * half : (s + 1) * half]

    for s in range(2):
        arrived(r_b.at[s], n, recv, 5 + s)
        vr, vi = mixed(1, r_b[s, :, 0], r_b[s, :, 1], 1, units, 1)
        vr, vi = mixed(1, vr, vi, units, n, 2)
        ur, ui = part[s, 0], part[s, 1]
        cosine, sine = (jnp.broadcast_to(x, (half, lanes))[None] for x in angle(1, 1))
        re = (cosine * ur + sine * vi, cosine * vr + sine * ui)
        im = (cosine * ui - sine * vr, cosine * vi - sine * ur)
        for h in range(2):
            chance = re[h] * re[h] + im[h] * im[h]
            for d in range(depth):
                ch[s, :, :, d, h] = chance[d * units : (d + 1) * units].reshape(nb // 2, 2, half, lanes)
        remote(ch.at[s, :, 1 - side], near.at[s], 8 + nl * s, (bank ^ 1, lane))
        for h in range(2):
            for i, x in enumerate((re[h], im[h])):
                out[i, :, :, h, s * half : (s + 1) * half] = x.reshape(depth, units, half, lanes)

    for s in range(2):
        pltpu.make_async_copy(near.at[s], near.at[s], recv.at[8 + nl * s]).wait()
        pair[s] = ch[s, :, side] + near[s]

        def one(to, carry):
            @pl.when(to != pairs_at)
            def _():
                remote(pair.at[s, to], m_in.at[s, pairs_at], 7 * s, (2 * to + side, lane))

            return carry

        lax.fori_loop(0, nb // 2, one, 0)
        m_in[s, pairs_at] = pair[s, pairs_at]
    for s in range(2):
        arrived(m_in.at[s], nb // 2, recv, 7 * s)
        total = m_in[s, 0]
        for g in range(1, nb // 2):
            total = total + m_in[s, g]
        marg[:, :, s * half : (s + 1) * half] = total * (1.0 / nb)
    for k in range(1, nl):
        pltpu.make_async_copy(en.at[:, 0], e_l.at[0], send.at[8 + k]).wait()
    arrived(e_b, nb, send, 1)
    for h in range(2):
        arrived(b_b.at[h], n, send, 2 + h)
        arrived(r_b.at[h], n, send, 5 + h)
        arrived(m_in.at[h], nb // 2, send, 7 * h)
        pltpu.make_async_copy(near.at[h], near.at[h], send.at[8 + nl * h]).wait()
    arrived(r_a, n, send, 4)


def keep(a, b, a_hbm, b_hbm, sems):
    copies = [pltpu.make_async_copy(a, a_hbm, sems.at[0]), pltpu.make_async_copy(b, b_hbm, sems.at[1])]
    for copy in copies:
        copy.start()
    for copy in copies:
        copy.wait()


def in_pieces(nb, nl, amplitudes, energies, phase_angles, mix_angles):
    _, depth, rows, lanes = amplitudes.shape
    n = nb * nl
    per = depth * rows // n
    step, half = per // 2, per // 4
    f32 = jnp.float32
    vmem = pl.BlockSpec(memory_space=pltpu.VMEM)
    anywhere = pl.BlockSpec(memory_space=pl.ANY)
    state = pltpu.VMEM((2, n, 2, step, lanes), f32)
    level = pltpu.VMEM((n, per, lanes), f32)
    spread = pltpu.VMEM((nb, nl, per, lanes), f32)
    shapes = (2, depth, nb, 2, step, lanes), (depth, 2, step, lanes)
    results = pl.pallas_call(
        functools.partial(pieces, nb, nl),
        name="register",
        out_shape=tuple(pltpu.VMEM(shape, f32) for shape in shapes),
        in_specs=[anywhere] * 4,
        out_specs=(vmem, vmem),
        scratch_shapes=[
            pltpu.VMEM(phase_angles.shape, f32),
            pltpu.VMEM(mix_angles.shape, f32),
            pltpu.VMEM((2, *mix_angles.shape), f32),
            pltpu.VMEM((2, depth, rows, lanes), f32),
            spread,
            pltpu.VMEM((nl, nb, per, lanes), f32),
            state,
            spread,
            state,
            pltpu.VMEM((n, 2, step, lanes), f32),
            pltpu.VMEM((2, n, 2, half, lanes), f32),
            pltpu.VMEM((n, 2, step, lanes), f32),
            pltpu.VMEM((2, n, 2, half, lanes), f32),
            level,
            level,
            pltpu.VMEM((2, 2, n, half, lanes), f32),
            pltpu.VMEM((2, nb // 2, 2, depth, 2, half, lanes), f32),
            pltpu.VMEM((2, nb // 2, depth, 2, half, lanes), f32),
            pltpu.VMEM((2, nb // 2, depth, 2, half, lanes), f32),
            pltpu.VMEM((2, nb // 2, depth, 2, half, lanes), f32),
            pltpu.SemaphoreType.DMA((4,)),
            pltpu.SemaphoreType.DMA((9 + nl,)),
            pltpu.SemaphoreType.DMA((9 + nl,)),
            *[pltpu.SemaphoreType.REGULAR] * 4,
        ],
        compiler_params=pltpu.CompilerParams(collective_id=0, has_side_effects=True),
    )(amplitudes, energies.reshape(nb, nl, per, lanes), phase_angles, mix_angles)
    final, marginal = pl.pallas_call(
        keep,
        name="keep",
        out_shape=tuple(jax.ShapeDtypeStruct(shape, f32) for shape in shapes),
        in_specs=[vmem, vmem],
        out_specs=(anywhere, anywhere),
        scratch_shapes=[pltpu.SemaphoreType.DMA((2,))],
    )(*[pltpu.with_memory_space_constraint(x, pltpu.VMEM) for x in results])
    return final.reshape(amplitudes.shape), marginal.reshape(depth, rows // nb, lanes)


def on_device(nb, nl, amplitudes, energies, phase_angles, mix_angles):
    _, depth, rows, lanes = amplitudes.shape
    n = nb * nl
    per = depth * rows // n
    halves = 2 if per % 16 == 0 else 1
    piece = rows // nb
    if per == 2 * 8 and piece == per and rows // per % nl == 0 and n * 8 % lanes == 0:
        return in_pieces(nb, nl, amplitudes, energies, phase_angles, mix_angles)
    f32 = jnp.float32
    state = pltpu.VMEM((halves, n, 2, per // halves, lanes), f32)
    level = pltpu.VMEM((n, per, lanes), f32)
    spread = pltpu.VMEM((nb, nl, per, lanes), f32)
    vmem = pl.BlockSpec(memory_space=pltpu.VMEM)
    anywhere = pl.BlockSpec(memory_space=pl.ANY)
    whole = pltpu.VMEM((2, depth, rows, lanes), f32)
    return pl.pallas_call(
        functools.partial(kernel, nb, nl, halves),
        name="register",
        out_shape=(pltpu.VMEM(amplitudes.shape, f32), pltpu.VMEM((depth, piece, lanes), f32)),
        in_specs=[anywhere] * 4,
        out_specs=(vmem, vmem),
        scratch_shapes=[
            pltpu.VMEM(phase_angles.shape, f32),
            pltpu.VMEM(mix_angles.shape, f32),
            whole,
            spread,
            pltpu.VMEM((nl, nb, per, lanes), f32),
            whole if per % 8 else pltpu.VMEM((1, 1, 8, 128), f32),
            state,
            spread,
            state,
            state,
            state,
            level,
            level,
            pltpu.VMEM((2, depth, rows // halves, lanes), f32),
            pltpu.VMEM((depth, nb, piece, lanes), f32),
            pltpu.VMEM((nb, depth, piece, lanes), f32),
            pltpu.SemaphoreType.DMA((4,)),
            pltpu.SemaphoreType.DMA((2 * halves + 3,)),
            pltpu.SemaphoreType.DMA((2 * halves + 3,)),
            pltpu.SemaphoreType.REGULAR,
            pltpu.SemaphoreType.REGULAR,
            pltpu.SemaphoreType.REGULAR,
        ],
        compiler_params=pltpu.CompilerParams(collective_id=0, has_side_effects=True),
    )(amplitudes, energies.reshape(nb, nl, per, lanes), phase_angles, mix_angles)


def solution(mesh):
    placed = (P(None, ("bank", "lane"), None, None), P(("bank", "lane"), None, None), P(), P())
    return jax.shard_map(
        functools.partial(on_device, mesh.shape["bank"], mesh.shape["lane"]),
        mesh=mesh,
        in_specs=placed,
        out_specs=(P(None, ("bank", "lane"), None, None), P("lane", "bank", None)),
        check_vma=False,
    )
```
